256 devices in a mesh: tm: 8 (over y, core), space: 32 (over z, x).
Axes of the slice: x: 4, y: 4, z: 8, core: 2. Of those that a mesh axis runs over, the one named last changes fastest.
Arguments:
- state: bfloat16 [8, 16384, 137], P('tm', 'space'), may hold values from -6 to 6
- obs_start: int32 [131072], P(('tm', 'space')), may hold values from 0 to 16383, as said below
- foot_weight: bfloat16 [131072, 8], P(('tm', 'space')), may hold values from 0.019897461 to 0.29882812
- obs_slot: int32 [131072], P(('tm', 'space')), may hold values from 0 to 6
- obs_frac: float32 [131072], P(('tm', 'space')), may hold values from 0 to 1
- live_count: int32 [8, 32], P('tm', 'space'), may hold values from 64 to 512
- obs_values: float32 [131072, 128], P(('tm', 'space')), may hold values from -6 to 6
- jacobian: bfloat16 [137, 128], replicated, may hold values from -0.5 to 0.5
- inv_var: float32 [128], replicated, may hold values from 0.25 to 4
Outputs:
- departures: float32 [131072, 128], P(('tm', 'space'))
- adjoint: float32 [8, 16384, 137], P('tm', 'space')
The draws below stay inside these ranges and needn't reach their ends.
Inputs may be any that keep to these rules, and one draw needn't show every extreme that they name: `obs_start`: on the devices of space index s, every observation's footprint columns lie within 256 columns of tile s, that is within s * 512 - 256 .. (s + 1) * 512 + 255 taken modulo 16384. `live_count`: rows at or beyond a device's count are padding.
All inputs are finite; a program needn't handle non-finite values.
Results may differ from the reference program's by a relative error of at most 0.008.
Values may be sent and summed in bfloat16 or wider, within the bound.
A program may use at most 64 MiB of HBM per device.

```python
import math
import jax
import jax.numpy as jnp
from jax import lax

LEV = 137
CHAN = 128
FOOT = 8
COL_DEV = 512
OBS_DEV = 512
HALO = 256
SLOTS = 8
TILES = 32
COLS = 16384
OBS = 131072
N_TM = 8
N_SPACE = 32


def draw_obs_start(key, part):
    total_rows = OBS_DEV * N_TM * N_SPACE
    row_index = jnp.arange(total_rows, dtype=jnp.int32)
    tile_index = row_index // OBS_DEV % N_SPACE
    offset = jax.random.randint(key, (total_rows,), 0, COL_DEV + 2 * HALO - FOOT + 1, dtype=jnp.int32)
    return jnp.mod(tile_index * COL_DEV - HALO + offset, COLS).astype(jnp.int32)


def with_ends(drawn, key, low, top_value):
    longest = drawn.shape.index(max(drawn.shape))
    spots = []
    for shift in (0, 1):
        where = [jax.random.randint(jax.random.fold_in(key, axis), (), 0, length) for axis, length in enumerate(drawn.shape)]
        where[longest] = (where[longest] + shift) % drawn.shape[longest]
        spots.append(tuple(where))
    return drawn.at[spots[0]].set(low).at[spots[1]].set(top_value)


def block_scale(key, extent, split, smallest, largest):
    factor_of = 1.0
    for position, parts in split:
        steps = jax.random.uniform(jax.random.fold_in(jax.random.fold_in(key, 6), position), (parts,), jnp.float32, smallest / len(split), largest / len(split))
        factor_of = factor_of * jnp.repeat(jnp.exp(steps), extent[position] // parts).reshape((-1,) + (1,) * (len(extent) - 1 - position))
    return factor_of


def centred(rng, dims, scale, most, split=(), held_as=jnp.bfloat16):
    array = scale * jax.random.normal(rng, dims, jnp.float32)
    if split:
        array = array * block_scale(rng, dims, split, -0.22, 0.18)
    return jnp.clip(array, -most, most).astype(held_as)


def setup_inputs(seed: int = 0) -> dict:
    streams_of = jax.random.split(jax.random.key(seed), 10)
    state = centred(streams_of[0], (SLOTS, COLS, LEV), 1.0, 6.0, ((0, 8), (1, 32)))
    obs_start = draw_obs_start(jax.random.fold_in(streams_of[9], 71), 0)
    foot_weight = jnp.clip(jnp.exp(math.log(0.29882812) - 2.7092764 * jax.random.uniform(streams_of[2], (OBS, FOOT), jnp.float32) ** block_scale(streams_of[2], (OBS, FOOT), ((0, 256),), -0.2, 0.2)), 0.019897461, 0.29882812).astype(jnp.bfloat16)
    obs_slot = with_ends(jax.random.randint(streams_of[3], (OBS,), 0, SLOTS - 1), jax.random.fold_in(streams_of[3], 1), 0, (SLOTS - 1) - 1).astype(jnp.int32)
    obs_frac = jnp.clip(1.0 * jax.random.uniform(streams_of[4], (OBS,), jnp.float32) ** block_scale(streams_of[4], (OBS,), ((0, 256),), -0.2, 0.2), 0.0, 1.0)
    live_count = with_ends(jax.random.randint(streams_of[5], (SLOTS, TILES), OBS_DEV // 8, OBS_DEV + 1), jax.random.fold_in(streams_of[5], 1), OBS_DEV // 8, OBS_DEV).astype(jnp.int32)
    obs_values = centred(streams_of[6], (OBS, CHAN), 1.0, 6.0, ((0, 256),), jnp.float32)
    jacobian = centred(streams_of[7], (LEV, CHAN), LEV ** -0.5, 0.5)
    inv_var = jnp.clip(jnp.exp(jax.random.uniform(streams_of[8], (CHAN,), jnp.float32, math.log(0.25), math.log(4.0))), 0.25, 4.0)
    return {"state": state, "obs_start": obs_start, "foot_weight": foot_weight, "obs_slot": obs_slot, "obs_frac": obs_frac, "live_count": live_count, "obs_values": obs_values, "jacobian": jacobian, "inv_var": inv_var}


def reference(state, obs_start, foot_weight, obs_slot, obs_frac, live_count, obs_values, jacobian, inv_var):
    cols = state.shape[1]
    groups = live_count.shape[0] * live_count.shape[1]
    per_group = obs_start.shape[0] // groups
    offsets = jnp.arange(FOOT, dtype=jnp.int32)

    def visit(adjoint, inputs):
        start, weight, slot, frac, count, values = inputs
        columns = jnp.mod(start[:, None] + offsets[None, :], cols).astype(jnp.int32)
        lower_slot = slot[:, None].astype(jnp.int32)
        upper_slot = (slot[:, None] + 1).astype(jnp.int32)
        lower = state[lower_slot, columns].astype(jnp.float32)
        upper = state[upper_slot, columns].astype(jnp.float32)
        weight_f = weight.astype(jnp.float32)
        p_lower = jnp.einsum("rk,rkl->rl", weight_f, lower, precision=lax.Precision.HIGHEST)
        p_upper = jnp.einsum("rk,rkl->rl", weight_f, upper, precision=lax.Precision.HIGHEST)
        interp = (1.0 - frac)[:, None] * p_lower + frac[:, None] * p_upper
        projected = jnp.dot(interp.astype(jnp.bfloat16), jacobian, preferred_element_type=jnp.float32)
        live = jnp.arange(per_group, dtype=jnp.int32) < count
        departures = jnp.where(live[:, None], values - projected, jnp.float32(0.0))
        scaled = (departures * inv_var[None, :]).astype(jnp.bfloat16)
        back = jnp.dot(scaled, jnp.transpose(jacobian), preferred_element_type=jnp.float32).astype(jnp.bfloat16)
        back = lax.optimization_barrier(back).astype(jnp.float32)
        v_lower = ((1.0 - frac)[:, None] * back).astype(jnp.bfloat16)
        v_upper = (frac[:, None] * back).astype(jnp.bfloat16)
        v_lower = lax.optimization_barrier(v_lower).astype(jnp.float32)
        v_upper = lax.optimization_barrier(v_upper).astype(jnp.float32)
        adjoint = adjoint.at[lower_slot, columns].add(weight_f[:, :, None] * v_lower[:, None, :])
        adjoint = adjoint.at[upper_slot, columns].add(weight_f[:, :, None] * v_upper[:, None, :])
        return adjoint, departures

    inputs = (
        obs_start.reshape(groups, per_group),
        foot_weight.reshape(groups, per_group, FOOT),
        obs_slot.reshape(groups, per_group),
        obs_frac.reshape(groups, per_group),
        live_count.reshape(groups).astype(jnp.int32),
        obs_values.reshape(groups, per_group, obs_values.shape[1]),
    )
    adjoint, departures = lax.scan(visit, jnp.zeros(state.shape, jnp.float32), inputs)
    return departures.reshape(obs_values.shape), adjoint
```

```python
import functools

import jax
import jax.numpy as jnp
from jax import lax
from jax.experimental import pallas as pl
from jax.experimental.pallas import tpu as pltpu
from jax.sharding import PartitionSpec as P

MESH = pl.DeviceIdType.MESH
F32 = jnp.float32
BF16 = jnp.bfloat16

META, Z, RS, AG, BK = 0, 12, 18, 24, 30
COPIES = 36


def nt(a, b):
    return lax.dot_general(a, b, (((1,), (1,)), ((), ())), preferred_element_type=F32)


def kernel(
    n_space, total_cols,
    state_ref, start_ref, w_ref, slot_ref, frac_ref, count_ref, obs_ref, jac_ref, inv_ref,
    dep_ref, adj_ref,
    m_start, m_w, m_slot, m_frac, foot, zbuf, acc, abuf, pout, relay, rin, sbuf, wide, wout, win, rim, obs_t, dep_t, inv_t,
    send, recv,
):
    t = lax.axis_index("tm")
    s = lax.axis_index("space")
    mate = t + 1 - 2 * lax.rem(t, 2)
    y1 = lax.rem(t + 2, 8)
    y2 = lax.rem(t + 4, 8)
    y3 = lax.rem(t + 6, 8)
    left = lax.rem(s + n_space - 1, n_space)
    right = lax.rem(s + 1, n_space)
    chans = 128
    half = 256

    barrier = pltpu.get_barrier_semaphore()
    for peer in ((mate, s), (y1, s), (y2, s), (y3, s), (t, left), (mate, left), (t, right), (mate, right)):
        pl.semaphore_signal(barrier, inc=1, device_id=peer, device_id_type=MESH)

    def copy(index, src, dst, device):
        return pltpu.make_async_remote_copy(
            src_ref=src, dst_ref=dst, send_sem=send.at[index], recv_sem=recv.at[index],
            device_id=device, device_id_type=MESH,
        )

    z = lax.dot_general(jac_ref[...], state_ref[...], (((0,), (0,)), ((), ())), preferred_element_type=F32).astype(BF16)
    zbuf[1, 0] = z[:, :half]
    zbuf[2, 0] = z[:, half:]

    pl.semaphore_wait(barrier, 8)

    z_copies = [
        copy(Z + 2, zbuf.at[1, 0], zbuf.at[3, 0], (t, left)),
        copy(Z + 3, zbuf.at[2, 0], zbuf.at[0, 0], (t, right)),
        copy(Z + 4, zbuf.at[1, 0], zbuf.at[3, 1], (mate, left)),
        copy(Z + 5, zbuf.at[2, 0], zbuf.at[0, 1], (mate, right)),
        copy(Z + 0, zbuf.at[1, 0], zbuf.at[1, 1], (mate, s)),
        copy(Z + 1, zbuf.at[2, 0], zbuf.at[2, 1], (mate, s)),
    ]
    meta = []
    for hop, peer in ((2, y2), (1, y1), (3, y3)):
        at = 3 - hop
        for kind, (src, dst) in enumerate(((start_ref, m_start), (w_ref, m_w), (slot_ref, m_slot), (frac_ref, m_frac))):
            meta.append(copy(META + 4 * at + kind, src, dst.at[at], (peer, s)))
    for c in z_copies[:4] + meta + z_copies[4:]:
        c.start()

    obs_t[...] = jnp.transpose(obs_ref[...])
    inv_t[...] = jnp.transpose(jnp.broadcast_to(inv_ref[...], (chans, chans)))

    def weight_of(slot, frac, held):
        return jnp.where(slot == held, 1.0 - frac, 0.0) + jnp.where(slot + 1 == held, frac, 0.0)

    def build(group, start, w, slot, frac):
        own = weight_of(slot, frac, t)
        other = weight_of(slot, frac, mate)
        for h in range(2):
            lanes = slice(h * half, (h + 1) * half)
            abuf[2 * group + h, 0:1, :] = own[:, lanes]
            abuf[2 * group + h, 1:2, :] = other[:, lanes]
        local = jnp.bitwise_and(start - s * 512 + 256, total_cols - 1)
        row = lax.broadcasted_iota(jnp.int32, (8, 512), 0)
        ahead = jnp.bitwise_and(row - local, 7)
        weights = w.astype(F32)
        turned = jnp.zeros((8, 512), F32)
        for k in range(8):
            turned = turned + jnp.where(ahead == k, weights[k : k + 1, :], 0.0)
        block = lax.shift_right_arithmetic(local - row + 7, 3)

        def rows(index, carry):
            parts = [jnp.where(block == index * 8 + m, turned, 0.0) for m in range(8)]
            value = jnp.concatenate(parts, axis=0).astype(BF16)
            at = pl.ds(pl.multiple_of(index * 64, 64), 64)
            foot[2 * group, at, :] = value[:, :half]
            foot[2 * group + 1, at, :] = value[:, half:]
            return carry

        lax.fori_loop(0, 16, rows, 0)

    build(0, start_ref[...], w_ref[...], slot_ref[...], frac_ref[...])

    def wait_meta(at):
        for kind, (src, dst) in enumerate(((start_ref, m_start), (w_ref, m_w), (slot_ref, m_slot), (frac_ref, m_frac))):
            copy(META + 4 * at + kind, src, dst.at[at], (y1, s)).wait_recv()

    for group in (2, 1, 3):
        at = group - 1
        wait_meta(at)
        build(group, m_start[at], m_w[at], m_slot[at], m_frac[at])

    z_copies[4].wait_recv()
    z_copies[5].wait_recv()

    def stacked(chunk):
        return jnp.concatenate([zbuf[chunk, 0], zbuf[chunk, 1]], axis=0)

    def centre(piece, carry):
        acc[piece] = jnp.dot(stacked(1), foot[piece, half : 2 * half], preferred_element_type=F32) + jnp.dot(
            stacked(2), foot[piece, 2 * half : 3 * half], preferred_element_type=F32
        )
        return carry

    lax.fori_loop(0, 8, centre, 0)

    for c in z_copies[:4]:
        c.wait_recv()

    def finish(piece):
        total = (
            acc[piece]
            + jnp.dot(stacked(0), foot[piece, 0:half], preferred_element_type=F32)
            + jnp.dot(stacked(3), foot[piece, 3 * half : 4 * half], preferred_element_type=F32)
        )
        return abuf[piece, 0:1, :] * total[:chans] + abuf[piece, 1:2, :] * total[chans:]

    pout[0] = finish(4).astype(BF16)
    pout[1] = finish(5).astype(BF16)
    rs = [
        copy(RS + 0, pout.at[0], relay.at[0], (y1, s)),
        copy(RS + 1, pout.at[1], relay.at[1], (y3, s)),
        copy(RS + 2, pout.at[2], rin.at[1], (y1, s)),
        copy(RS + 3, pout.at[3], rin.at[2], (y3, s)),
        copy(RS + 4, pout.at[4], rin.at[0], (y1, s)),
        copy(RS + 5, pout.at[5], rin.at[3], (y3, s)),
    ]
    rs[0].start()
    rs[1].start()
    pout[2] = finish(3).astype(BF16)
    rs[2].start()
    pout[3] = finish(6).astype(BF16)
    rs[3].start()
    first = finish(2)
    second = finish(7)
    rs[0].wait_recv()
    pout[4] = (first + relay[0].astype(F32)).astype(BF16)
    rs[4].start()
    rs[1].wait_recv()
    pout[5] = (second + relay[1].astype(F32)).astype(BF16)
    rs[5].start()
    acc[0, 0:chans] = finish(0)
    acc[1, 0:chans] = finish(1)

    count = count_ref[0, 0]
    column = lax.broadcasted_iota(jnp.int32, (1, half), 1)
    for h, waits in ((0, (rs[4], rs[3])), (1, (rs[2], rs[5]))):
        for c in waits:
            c.wait_recv()
        projected = acc[h, 0:chans] + rin[h].astype(F32) + rin[2 + h].astype(F32)
        live = column + h * half < count
        departed = jnp.where(live, obs_t[:, h * half : (h + 1) * half] - projected, 0.0)
        dep_t[:, h * half : (h + 1) * half] = departed
        sbuf[h] = (departed * inv_t[:, 0:1]).astype(BF16)

    ag = [
        copy(AG + 0, sbuf.at[0], sbuf.at[6], (y1, s)),
        copy(AG + 1, sbuf.at[1], sbuf.at[3], (y3, s)),
        copy(AG + 2, sbuf.at[1], sbuf.at[7], (y1, s)),
        copy(AG + 3, sbuf.at[0], sbuf.at[2], (y3, s)),
        copy(AG + 4, sbuf.at[6], sbuf.at[4], (y1, s)),
        copy(AG + 5, sbuf.at[3], sbuf.at[5], (y3, s)),
    ]
    for c in ag[:4]:
        c.start()
    dep_ref[...] = jnp.transpose(dep_t[...])

    def scaled_by_slot(piece):
        values = sbuf[piece].astype(F32)
        return jnp.concatenate(
            [(abuf[piece, 0:1, :] * values).astype(BF16), (abuf[piece, 1:2, :] * values).astype(BF16)], axis=0
        )

    def spread(piece, fresh):
        v = scaled_by_slot(piece)
        for chunk in (0, 3, 1, 2):
            part = nt(v, foot[piece, chunk * half : (chunk + 1) * half])
            if fresh:
                wide[chunk] = part
            else:
                wide[chunk] += part

    spread(0, True)
    spread(1, False)
    ag[0].wait_recv()
    ag[4].start()
    ag[1].wait_recv()
    ag[5].start()
    spread(6, False)
    spread(3, False)
    ag[2].wait_recv()
    spread(7, False)
    ag[3].wait_recv()
    spread(2, False)
    ag[4].wait_recv()
    spread(4, False)
    ag[5].wait_recv()
    spread(5, False)

    for place, chunk in enumerate((0, 3, 1, 2)):
        wout[place, 0] = wide[chunk, 0:chans].astype(BF16)
        wout[place, 1] = wide[chunk, chans:].astype(BF16)
    bk = [
        copy(BK + 0, wout.at[0, 0], rim.at[2], (t, left)),
        copy(BK + 1, wout.at[1, 0], rim.at[0], (t, right)),
        copy(BK + 2, wout.at[0, 1], rim.at[3], (mate, left)),
        copy(BK + 3, wout.at[1, 1], rim.at[1], (mate, right)),
        copy(BK + 4, wout.at[2, 1], win.at[0], (mate, s)),
        copy(BK + 5, wout.at[3, 1], win.at[1], (mate, s)),
    ]
    for c in bk:
        c.start()
    for h, waits in ((0, (bk[4], bk[1], bk[3])), (1, (bk[5], bk[0], bk[2]))):
        for c in waits:
            c.wait_recv()
        whole = wide[1 + h, 0:chans] + win[h].astype(F32) + rim[2 * h].astype(F32) + rim[2 * h + 1].astype(F32)
        adj_ref[:, h * half : (h + 1) * half] = jnp.dot(jac_ref[...], whole.astype(BF16), preferred_element_type=F32)

    for c in z_copies + meta + rs + ag + bk:
        c.wait_send()


def body(state, obs_start, foot_weight, obs_slot, obs_frac, live_count, obs_values, jacobian, inv_var):
    n_space = lax.axis_size("space")
    levels = jacobian.shape[0]
    vmem = pl.BlockSpec(memory_space=pltpu.VMEM)
    departures, adjoint = pl.pallas_call(
        functools.partial(kernel, n_space, 512 * n_space),
        out_shape=(
            jax.ShapeDtypeStruct((512, 128), F32),
            jax.ShapeDtypeStruct((levels, 512), F32),
        ),
        in_specs=[vmem] * 5 + [pl.BlockSpec(memory_space=pltpu.SMEM)] + [vmem] * 3,
        out_specs=(vmem, vmem),
        scratch_shapes=[
            pltpu.VMEM((3, 1, 512), jnp.int32),
            pltpu.VMEM((3, 8, 512), BF16),
            pltpu.VMEM((3, 1, 512), jnp.int32),
            pltpu.VMEM((3, 1, 512), F32),
            pltpu.VMEM((8, 1024, 256), BF16),
            pltpu.VMEM((4, 2, 128, 256), BF16),
            pltpu.VMEM((8, 256, 256), F32),
            pltpu.VMEM((8, 2, 256), F32),
            pltpu.VMEM((6, 128, 256), BF16),
            pltpu.VMEM((2, 128, 256), BF16),
            pltpu.VMEM((4, 128, 256), BF16),
            pltpu.VMEM((8, 128, 256), BF16),
            pltpu.VMEM((4, 256, 256), F32),
            pltpu.VMEM((4, 2, 128, 256), BF16),
            pltpu.VMEM((2, 128, 256), BF16),
            pltpu.VMEM((4, 128, 256), BF16),
            pltpu.VMEM((128, 512), F32),
            pltpu.VMEM((128, 512), F32),
            pltpu.VMEM((128, 128), F32),
            pltpu.SemaphoreType.DMA((COPIES,)),
            pltpu.SemaphoreType.DMA((COPIES,)),
        ],
        compiler_params=pltpu.CompilerParams(collective_id=0, has_side_effects=True),
        name="window",
    )(
        jnp.transpose(state[0]),
        obs_start[None],
        jnp.transpose(foot_weight),
        obs_slot[None],
        obs_frac[None],
        live_count,
        obs_values,
        jacobian,
        inv_var[None],
    )
    return departures, jnp.transpose(adjoint)[None]


def solution(mesh):
    return jax.shard_map(
        body,
        mesh=mesh,
        in_specs=(
            P("tm", "space", None),
            P(("tm", "space")),
            P(("tm", "space"), None),
            P(("tm", "space")),
            P(("tm", "space")),
            P("tm", "space"),
            P(("tm", "space"), None),
            P(),
            P(),
        ),
        out_specs=(P(("tm", "space"), None), P("tm", "space", None)),
        check_vma=False,
    )
```

```python
import functools

import jax
import jax.numpy as jnp
from jax import lax
from jax.experimental import pallas as pl
from jax.experimental.pallas import tpu as pltpu
from jax.sharding import PartitionSpec as P

MESH = pl.DeviceIdType.MESH
F32 = jnp.float32
BF16 = jnp.bfloat16

META, Z, RS, AG, BK = 0, 12, 18, 30, 42
COPIES = 48

LEFT, RIGHT, HEAD, TAIL = 0, 1, 2, 3


def nt(a, b):
    return lax.dot_general(a, b, (((1,), (1,)), ((), ())), preferred_element_type=F32)


def kernel(
    n_space, total_cols,
    state_in, start_in, w_in, slot_in, frac_in, count_ref, obs_in, jac_in, inv_in,
    dep_out, adj_out,
    state_ref, start_ref, w_ref, slot_ref, frac_ref, obs_ref, jac_ref, inv_ref, dep_ref, adj_ref,
    m_start, m_w, m_slot, m_frac, foot, zbuf, acc, abuf, pout, relay, rin, sbuf, wide, wout, win, rim, obs_t, inv_t, dep_t,
    load, store, send, recv,
):
    t = lax.axis_index("tm")
    s = lax.axis_index("space")
    mate = t + 1 - 2 * lax.rem(t, 2)
    y1 = lax.rem(t + 2, 8)
    y2 = lax.rem(t + 4, 8)
    y3 = lax.rem(t + 6, 8)
    left = lax.rem(s + n_space - 1, n_space)
    right = lax.rem(s + 1, n_space)
    chans = 128
    quarter = 128

    barrier = pltpu.get_barrier_semaphore()
    for peer in ((t, right), (t, left), (mate, left), (mate, right), (y2, s), (y1, s), (y3, s), (mate, s)):
        pl.semaphore_signal(barrier, inc=1, device_id=peer, device_id_type=MESH)

    loads = [
        pltpu.make_async_copy(src, dst, load.at[k])
        for k, (src, dst) in enumerate(
            (
                (state_in, state_ref), (jac_in, jac_ref), (start_in, start_ref), (w_in, w_ref), (slot_in, slot_ref),
                (frac_in, frac_ref), (obs_in, obs_ref), (inv_in, inv_ref),
            )
        )
    ]
    for c in loads:
        c.start()

    def copy(index, src, dst, device):
        return pltpu.make_async_remote_copy(
            src_ref=src, dst_ref=dst, send_sem=send.at[index], recv_sem=recv.at[index],
            device_id=device, device_id_type=MESH,
        )

    loads[0].wait()
    loads[1].wait()
    z = lax.dot_general(jac_ref[...], state_ref[...], (((0,), (0,)), ((), ())), preferred_element_type=F32).astype(BF16)
    zbuf[HEAD, 0] = z[:, :256]
    zbuf[TAIL, 0] = z[:, 256:]
    for c in loads[2:6]:
        c.wait()

    pl.semaphore_wait(barrier, 8)

    z_copies = [
        copy(Z + 0, zbuf.at[HEAD, 0], zbuf.at[RIGHT, 0], (t, left)),
        copy(Z + 1, zbuf.at[TAIL, 0], zbuf.at[LEFT, 0], (t, right)),
        copy(Z + 2, zbuf.at[HEAD, 0], zbuf.at[RIGHT, 1], (mate, left)),
        copy(Z + 3, zbuf.at[TAIL, 0], zbuf.at[LEFT, 1], (mate, right)),
        copy(Z + 4, zbuf.at[HEAD, 0], zbuf.at[HEAD, 1], (mate, s)),
        copy(Z + 5, zbuf.at[TAIL, 0], zbuf.at[TAIL, 1], (mate, s)),
    ]
    fields = ((start_ref, m_start), (w_ref, m_w), (slot_ref, m_slot), (frac_ref, m_frac))
    meta = {}
    for hop, peer in ((2, y2), (1, y1), (3, y3)):
        at = 3 - hop
        meta[at] = [copy(META + 4 * at + kind, src, dst.at[at], (peer, s)) for kind, (src, dst) in enumerate(fields)]
    for c in z_copies[:4] + meta[1] + meta[2] + meta[0] + z_copies[4:]:
        c.start()

    def weight_of(slot, frac, held):
        return jnp.where(slot == held, 1.0 - frac, 0.0) + jnp.where(slot + 1 == held, frac, 0.0)

    def build(group, start, w, slot, frac):
        abuf[group, 0:1, :] = weight_of(slot, frac, t)
        abuf[group, 1:2, :] = weight_of(slot, frac, mate)
        local = jnp.bitwise_and(start - s * 512 + 256, total_cols - 1)
        row = lax.broadcasted_iota(jnp.int32, (8, 512), 0)
        ahead = jnp.bitwise_and(row - local, 7)
        weights = w.astype(F32)
        turned = jnp.zeros((8, 512), F32)
        for k in range(8):
            turned = turned + jnp.where(ahead == k, weights[k : k + 1, :], 0.0)
        block = lax.shift_right_arithmetic(local - row + 7, 3)

        for first, last, shift in ((0, 4, 0), (4, 8, 8), (8, 16, -4)):

            def rows(index, carry):
                parts = [jnp.where(block == (index + shift) * 8 + m, turned, 0.0) for m in range(8)]
                at = pl.ds(pl.multiple_of(index * 64, 64), 64)
                foot[group, at, :] = jnp.concatenate(parts, axis=0).astype(BF16)
                return carry

            lax.fori_loop(first, last, rows, 0)

    def columns(first):
        return jnp.concatenate(
            [
                jnp.concatenate([zbuf[first, 0], zbuf[first + 1, 0]], axis=1),
                jnp.concatenate([zbuf[first, 1], zbuf[first + 1, 1]], axis=1),
            ],
            axis=0,
        )

    def centre(group):
        acc[group] = jnp.dot(columns(HEAD), foot[group, 512:1024, :], preferred_element_type=F32)

    build(0, start_ref[...], w_ref[...], slot_ref[...], frac_ref[...])
    for c in loads[6:]:
        c.wait()
    obs_t[...] = jnp.transpose(obs_ref[...])
    inv_t[...] = jnp.transpose(jnp.broadcast_to(inv_ref[...], (chans, chans)))
    z_copies[4].wait_recv()
    z_copies[5].wait_recv()
    centre(0)
    for group in (2, 1, 3):
        at = group - 1
        for c in meta[at]:
            c.wait_recv()
        build(group, m_start[at], m_w[at], m_slot[at], m_frac[at])
        centre(group)
    for c in z_copies[:4]:
        c.wait_recv()

    def finish(group):
        total = acc[group] + jnp.dot(columns(LEFT), foot[group, 0:512, :], preferred_element_type=F32)
        return abuf[group, 0:1, :] * total[:chans] + abuf[group, 1:2, :] * total[chans:]

    def lanes(q):
        return slice(q * quarter, (q + 1) * quarter)

    far = [copy(RS + q, pout.at[q], relay.at[q], ((y1, y1, y3, y3)[q], s)) for q in range(4)]
    to_next = [copy(RS + 4 + q, pout.at[4 + q], rin.at[0, q], (y1, s)) for q in range(4)]
    to_last = [copy(RS + 8 + q, pout.at[8 + q], rin.at[1, q], (y3, s)) for q in range(4)]
    partial = finish(2)
    for q in range(4):
        pout[q] = partial[:, lanes(q)].astype(BF16)
    for q in (0, 2, 1, 3):
        far[q].start()
    partial = finish(1)
    for q in (2, 3):
        pout[4 + q] = partial[:, lanes(q)].astype(BF16)
        to_next[q].start()
    acc[1, 0:chans, 0:256] = partial[:, :256]
    partial = finish(3)
    for q in (0, 1):
        pout[8 + q] = partial[:, lanes(q)].astype(BF16)
        to_last[q].start()
    acc[3, 0:chans, 256:512] = partial[:, 256:]
    acc[0, 0:chans] = finish(0)
    for q, group, base, copies in ((0, 1, 4, to_next), (2, 3, 8, to_last), (1, 1, 4, to_next), (3, 3, 8, to_last)):
        far[q].wait_recv()
        pout[base + q] = (acc[group, 0:chans, lanes(q)] + relay[q].astype(F32)).astype(BF16)
        copies[q].start()

    ag_next = [copy(AG + q, sbuf.at[0, q], sbuf.at[3, q], (y1, s)) for q in range(4)]
    ag_last = [copy(AG + 4 + q, sbuf.at[0, q], sbuf.at[1, q], (y3, s)) for q in range(4)]
    ag_far = [
        copy(AG + 8 + q, sbuf.at[(3, 3, 1, 1)[q], q], sbuf.at[2, q], ((y1, y1, y3, y3)[q], s)) for q in range(4)
    ]
    column = lax.broadcasted_iota(jnp.int32, (1, quarter), 1)
    for q in (0, 2, 1, 3):
        to_next[q].wait_recv()
        to_last[q].wait_recv()
        projected = acc[0, 0:chans, lanes(q)] + rin[0, q].astype(F32) + rin[1, q].astype(F32)
        live = column + q * quarter < count_ref[0, 0]
        departed = jnp.where(live, obs_t[:, lanes(q)] - projected, 0.0)
        dep_t[:, lanes(q)] = departed
        sbuf[0, q] = (departed * inv_t[:, 0:1]).astype(BF16)
        (ag_next if q < 2 else ag_last)[q].start()
    ag_next[2].start()
    ag_last[0].start()
    ag_next[3].start()
    ag_last[1].start()

    dep_ref[...] = jnp.transpose(dep_t[...])
    stores = [
        pltpu.make_async_copy(dep_ref, dep_out, store.at[0]),
        pltpu.make_async_copy(adj_ref.at[:, :, 0:256], adj_out.at[:, :, 0:256], store.at[1]),
        pltpu.make_async_copy(adj_ref.at[:, :, 256:512], adj_out.at[:, :, 256:512], store.at[2]),
    ]
    stores[0].start()

    def by_slot(group, quarters):
        values = jnp.concatenate([sbuf[group, q] for q in quarters], axis=1).astype(F32)
        span = slice(quarters[0] * quarter, (quarters[-1] + 1) * quarter)
        return jnp.concatenate(
            [(abuf[group, 0:1, span] * values).astype(BF16), (abuf[group, 1:2, span] * values).astype(BF16)], axis=0
        )

    def spread(group, quarters, fresh=False):
        v = by_slot(group, quarters)
        span = slice(quarters[0] * quarter, (quarters[-1] + 1) * quarter)
        for chunk in range(4):
            part = nt(v, foot[group, chunk * 256 : (chunk + 1) * 256, span])
            if fresh:
                wide[chunk] = part
            else:
                wide[chunk] += part

    spread(0, (0, 1, 2, 3), True)
    for q in (0, 2, 1, 3):
        (ag_next if q < 2 else ag_last)[q].wait_recv()
        ag_far[q].start()
    spread(3, (0, 1))
    spread(1, (2, 3))
    ag_next[2].wait_recv()
    ag_next[3].wait_recv()
    spread(3, (2, 3))
    ag_last[0].wait_recv()
    ag_last[1].wait_recv()
    spread(1, (0, 1))
    for q in (0, 2, 1, 3):
        ag_far[q].wait_recv()
    bk = [
        copy(BK + 0, wout.at[LEFT, 0], rim.at[1, 0], (t, left)),
        copy(BK + 1, wout.at[RIGHT, 0], rim.at[0, 0], (t, right)),
        copy(BK + 2, wout.at[LEFT, 1], rim.at[1, 1], (mate, left)),
        copy(BK + 3, wout.at[RIGHT, 1], rim.at[0, 1], (mate, right)),
        copy(BK + 4, wout.at[HEAD, 1], win.at[0], (mate, s)),
        copy(BK + 5, wout.at[TAIL, 1], win.at[1], (mate, s)),
    ]
    v = by_slot(2, (0, 1, 2, 3))
    for chunk in (LEFT, RIGHT):
        total = wide[chunk] + nt(v, foot[2, chunk * 256 : (chunk + 1) * 256, :])
        wout[chunk, 0] = total[:chans].astype(BF16)
        wout[chunk, 1] = total[chans:].astype(BF16)
        bk[chunk].start()
        bk[2 + chunk].start()
    for chunk in (HEAD, TAIL):
        total = wide[chunk] + nt(v, foot[2, chunk * 256 : (chunk + 1) * 256, :])
        wide[chunk] = total
        wout[chunk, 1] = total[chans:].astype(BF16)
        bk[2 + chunk].start()
    for h, waits in ((0, (bk[4], bk[1], bk[3])), (1, (bk[5], bk[0], bk[2]))):
        for c in waits:
            c.wait_recv()
        whole = wide[HEAD + h, 0:chans] + win[h].astype(F32) + rim[h, 0].astype(F32) + rim[h, 1].astype(F32)
        adj_ref[:, 0, h * 256 : (h + 1) * 256] = jnp.dot(jac_ref[...], whole.astype(BF16), preferred_element_type=F32)
        stores[1 + h].start()
    for c in z_copies + meta[0] + meta[1] + meta[2] + far + to_next + to_last + ag_next + ag_last + ag_far + bk:
        c.wait_send()
    for c in stores:
        c.wait()


def body(state, obs_start, foot_weight, obs_slot, obs_frac, live_count, obs_values, jacobian, inv_var):
    n_space = lax.axis_size("space")
    levels = jacobian.shape[0]
    anywhere = pl.BlockSpec(memory_space=pl.ANY)
    i32 = jnp.int32
    departures, adjoint = pl.pallas_call(
        functools.partial(kernel, n_space, 512 * n_space),
        out_shape=(
            jax.ShapeDtypeStruct((512, 128), F32),
            jax.ShapeDtypeStruct((levels, 1, 512), F32),
        ),
        in_specs=[anywhere] * 5 + [pl.BlockSpec(memory_space=pltpu.SMEM)] + [anywhere] * 3,
        out_specs=(anywhere, anywhere),
        scratch_shapes=[
            pltpu.VMEM((levels, 512), BF16),
            pltpu.VMEM((1, 512), i32),
            pltpu.VMEM((8, 512), BF16),
            pltpu.VMEM((1, 512), i32),
            pltpu.VMEM((1, 512), F32),
            pltpu.VMEM((512, 128), F32),
            pltpu.VMEM((levels, 128), BF16),
            pltpu.VMEM((1, 128), F32),
            pltpu.VMEM((512, 128), F32),
            pltpu.VMEM((levels, 1, 512), F32),
            pltpu.VMEM((3, 1, 512), i32),
            pltpu.VMEM((3, 8, 512), BF16),
            pltpu.VMEM((3, 1, 512), i32),
            pltpu.VMEM((3, 1, 512), F32),
            pltpu.VMEM((4, 1024, 512), BF16),
            pltpu.VMEM((4, 2, 128, 256), BF16),
            pltpu.VMEM((4, 256, 512), F32),
            pltpu.VMEM((4, 2, 512), F32),
            pltpu.VMEM((12, 128, 128), BF16),
            pltpu.VMEM((4, 128, 128), BF16),
            pltpu.VMEM((2, 4, 128, 128), BF16),
            pltpu.VMEM((4, 4, 128, 128), BF16),
            pltpu.VMEM((4, 256, 256), F32),
            pltpu.VMEM((4, 2, 128, 256), BF16),
            pltpu.VMEM((2, 128, 256), BF16),
            pltpu.VMEM((2, 2, 128, 256), BF16),
            pltpu.VMEM((128, 512), F32),
            pltpu.VMEM((128, 128), F32),
            pltpu.VMEM((128, 512), F32),
            pltpu.SemaphoreType.DMA((8,)),
            pltpu.SemaphoreType.DMA((3,)),
            pltpu.SemaphoreType.DMA((COPIES,)),
            pltpu.SemaphoreType.DMA((COPIES,)),
        ],
        compiler_params=pltpu.CompilerParams(collective_id=0, has_side_effects=True),
        name="window",
    )(
        jnp.transpose(state[0]),
        obs_start[None],
        jnp.transpose(foot_weight),
        obs_slot[None],
        obs_frac[None],
        live_count,
        obs_values,
        jacobian,
        inv_var[None],
    )
    return departures, jnp.transpose(adjoint, (1, 2, 0))


def solution(mesh):
    return jax.shard_map(
        body,
        mesh=mesh,
        in_specs=(
            P("tm", "space", None),
            P(("tm", "space")),
            P(("tm", "space"), None),
            P(("tm", "space")),
            P(("tm", "space")),
            P("tm", "space"),
            P(("tm", "space"), None),
            P(),
            P(),
        ),
        out_specs=(P(("tm", "space"), None), P("tm", "space", None)),
        check_vma=False,
    )
```

```python
import functools

import jax
import jax.numpy as jnp
from jax import lax
from jax.experimental import pallas as pl
from jax.experimental.pallas import tpu as pltpu
from jax.sharding import PartitionSpec as P

MESH = pl.DeviceIdType.MESH
F32 = jnp.float32
BF16 = jnp.bfloat16

META, Z, RS, AG, BK = 0, 12, 22, 34, 46
COPIES = 56

LEFT, RIGHT, HEAD, TAIL = 0, 1, 2, 3


def nt(a, b):
    return lax.dot_general(a, b, (((1,), (1,)), ((), ())), preferred_element_type=F32)


def kernel(
    n_space, total_cols,
    state_in, start_in, w_in, slot_in, frac_in, count_ref, obs_in, jac_in, inv_in,
    dep_out, adj_out,
    state_ref, start_ref, w_ref, slot_ref, frac_ref, obs_ref, jac_ref, inv_ref,
    m_start, m_w, m_slot, m_frac, foot, zbuf, acc, abuf, pout, relay, rin, sbuf, wide, wout, win, rim, swap, obs_t, inv_t, dep_t,
    load, send, recv,
):
    t = lax.axis_index("tm")
    s = lax.axis_index("space")
    mate = t + 1 - 2 * lax.rem(t, 2)
    y1 = lax.rem(mate + 2, 8)
    y2 = lax.rem(t + 4, 8)
    y3 = lax.rem(mate + 6, 8)
    left = lax.rem(s + n_space - 1, n_space)
    right = lax.rem(s + 1, n_space)
    chans = 128
    quarter = 128
    top, bottom = pl.ds(0, 64), pl.ds(64, 64)

    barrier = pltpu.get_barrier_semaphore()
    for peer in ((t, right), (t, left), (mate, left), (mate, right), (y2, s), (y1, s), (y3, s), (mate, s)):
        pl.semaphore_signal(barrier, inc=1, device_id=peer, device_id_type=MESH)

    loads = [
        pltpu.make_async_copy(src, dst, load.at[k])
        for k, (src, dst) in enumerate(
            (
                (state_in, state_ref), (jac_in, jac_ref), (start_in, start_ref), (w_in, w_ref), (slot_in, slot_ref),
                (frac_in, frac_ref), (obs_in, obs_ref), (inv_in, inv_ref),
            )
        )
    ]
    for c in loads:
        c.start()

    def copy(index, src, dst, device):
        return pltpu.make_async_remote_copy(
            src_ref=src, dst_ref=dst, send_sem=send.at[index], recv_sem=recv.at[index],
            device_id=device, device_id_type=MESH,
        )

    loads[0].wait()
    loads[1].wait()
    z = lax.dot_general(jac_ref[...], state_ref[...], (((0,), (0,)), ((), ())), preferred_element_type=F32).astype(BF16)
    zbuf[HEAD, 0] = z[:, :256]
    zbuf[TAIL, 0] = z[:, 256:]
    for c in loads[2:6]:
        c.wait()

    pl.semaphore_wait(barrier, 8)

    sides = ((HEAD, RIGHT, left), (TAIL, LEFT, right))
    z_relayed = [copy(Z + k, zbuf.at[a, 0, top], zbuf.at[b, 0, top], (t, d)) for k, (a, b, d) in enumerate(sides)]
    z_direct = [copy(Z + 2 + k, zbuf.at[a, 0, bottom], zbuf.at[b, 0, bottom], (t, d)) for k, (a, b, d) in enumerate(sides)]
    z_cross = [copy(Z + 4 + k, zbuf.at[a, 0, bottom], zbuf.at[b, 1, bottom], (mate, d)) for k, (a, b, d) in enumerate(sides)]
    z_onward = [copy(Z + 6 + k, zbuf.at[b, 0, top], zbuf.at[b, 1, top], (mate, s)) for k, (a, b, d) in enumerate(sides)]
    z_mate = [copy(Z + 8 + k, zbuf.at[a, 0], zbuf.at[a, 1], (mate, s)) for k, (a, b, d) in enumerate(sides)]
    fields = ((start_ref, m_start), (w_ref, m_w), (slot_ref, m_slot), (frac_ref, m_frac))
    meta = {}
    for hop, peer in ((2, y2), (1, y1), (3, y3)):
        at = 3 - hop
        meta[at] = [copy(META + 4 * at + kind, src, dst.at[at], (peer, s)) for kind, (src, dst) in enumerate(fields)]
    for c in z_relayed + z_direct + z_cross + meta[1] + meta[2] + meta[0] + z_mate:
        c.start()

    def weight_of(slot, frac, held):
        return jnp.where(slot == held, 1.0 - frac, 0.0) + jnp.where(slot + 1 == held, frac, 0.0)

    def build(group, start, w, slot, frac):
        abuf[group, 0:1, :] = weight_of(slot, frac, t)
        abuf[group, 1:2, :] = weight_of(slot, frac, mate)
        local = jnp.bitwise_and(start - s * 512 + 256, total_cols - 1)
        row = lax.broadcasted_iota(jnp.int32, (8, 512), 0)
        ahead = jnp.bitwise_and(row - local, 7)
        weights = w.astype(F32)
        turned = jnp.zeros((8, 512), F32)
        for k in range(8):
            turned = turned + jnp.where(ahead == k, weights[k : k + 1, :], 0.0)
        block = lax.shift_right_arithmetic(local - row + 7, 3)

        for first, last, shift in ((0, 4, 0), (4, 8, 8), (8, 16, -4)):

            def rows(index, carry):
                parts = [jnp.where(block == (index + shift) * 8 + m, turned, 0.0) for m in range(8)]
                at = pl.ds(pl.multiple_of(index * 64, 64), 64)
                foot[group, at, :] = jnp.concatenate(parts, axis=0).astype(BF16)
                return carry

            lax.fori_loop(first, last, rows, 0)

    def columns(first):
        return jnp.concatenate(
            [
                jnp.concatenate([zbuf[first, 0], zbuf[first + 1, 0]], axis=1),
                jnp.concatenate([zbuf[first, 1], zbuf[first + 1, 1]], axis=1),
            ],
            axis=0,
        )

    def centre(group):
        acc[group] = jnp.dot(columns(HEAD), foot[group, 512:1024, :], preferred_element_type=F32)

    build(0, start_ref[...], w_ref[...], slot_ref[...], frac_ref[...])
    for c in loads[6:]:
        c.wait()
    obs_t[...] = jnp.transpose(obs_ref[...])
    inv_t[...] = jnp.transpose(jnp.broadcast_to(inv_ref[...], (chans, chans)))
    for c in z_mate:
        c.wait_recv()
    centre(0)
    for group in (1, 3):
        for c in meta[group - 1]:
            c.wait_recv()
        build(group, m_start[group - 1], m_w[group - 1], m_slot[group - 1], m_frac[group - 1])
        centre(group)
    for k in (1, 0):
        z_relayed[k].wait_recv()
        z_onward[k].start()
    for c in meta[1]:
        c.wait_recv()
    build(2, m_start[1], m_w[1], m_slot[1], m_frac[1])
    centre(2)
    for c in z_direct + z_onward + z_cross:
        c.wait_recv()

    def finish(group, half):
        span = slice(half * 256, (half + 1) * 256)
        total = acc[group, :, span] + jnp.dot(columns(LEFT), foot[group, 0:512, span], preferred_element_type=F32)
        return abuf[group, 0:1, span] * total[:chans] + abuf[group, 1:2, span] * total[chans:]

    def lanes(q):
        return slice(q * quarter, (q + 1) * quarter)

    far = [copy(RS + q, pout.at[q], relay.at[q], ((y1, y3)[q % 2], s)) for q in range(4)]
    to_next = [copy(RS + 4 + q, pout.at[4 + q], rin.at[0, q], (y1, s)) for q in range(4)]
    to_last = [copy(RS + 8 + q, pout.at[8 + q], rin.at[1, q], (y3, s)) for q in range(4)]
    for half in range(2):
        partial = finish(2, half)
        for k in range(2):
            pout[2 * half + k] = partial[:, lanes(k)].astype(BF16)
            far[2 * half + k].start()
    for half in range(2):
        for group, base, copies, now in ((1, 4, to_next, 1), (3, 8, to_last, 0)):
            partial = finish(group, half)
            q = 2 * half + now
            pout[base + q] = partial[:, lanes(now)].astype(BF16)
            copies[q].start()
            acc[group, 0:chans, lanes(q + 1 - 2 * now)] = partial[:, lanes(1 - now)]
    for half in range(2):
        acc[0, 0:chans, half * 256 : (half + 1) * 256] = finish(0, half)
    for q in range(4):
        group, base, copies = ((1, 4, to_next), (3, 8, to_last))[q % 2]
        far[q].wait_recv()
        pout[base + q] = (acc[group, 0:chans, lanes(q)] + relay[q].astype(F32)).astype(BF16)
        copies[q].start()

    ag_next = [copy(AG + q, sbuf.at[0, q], sbuf.at[3, q], (y1, s)) for q in range(4)]
    ag_last = [copy(AG + 4 + q, sbuf.at[0, q], sbuf.at[1, q], (y3, s)) for q in range(4)]
    ag_far = [
        copy(AG + 8 + q, sbuf.at[(3, 1)[q % 2], q], sbuf.at[2, q], ((y1, y3)[q % 2], s)) for q in range(4)
    ]
    column = lax.broadcasted_iota(jnp.int32, (1, quarter), 1)
    for q in range(4):
        to_next[q].wait_recv()
        to_last[q].wait_recv()
        projected = acc[0, 0:chans, lanes(q)] + rin[0, q].astype(F32) + rin[1, q].astype(F32)
        live = column + q * quarter < count_ref[0, 0]
        departed = jnp.where(live, obs_t[:, lanes(q)] - projected, 0.0)
        dep_t[:, lanes(q)] = departed
        sbuf[0, q] = (departed * inv_t[:, 0:1]).astype(BF16)
        (ag_next, ag_last)[q % 2][q].start()
    for q in (0, 2):
        ag_next[q + 1].start()
        ag_last[q].start()

    dep_out[...] = jnp.transpose(dep_t[...])

    def lanes_of(ref, group, rows, quarters):
        if quarters[-1] - quarters[0] == len(quarters) - 1:
            return ref[group, rows, quarters[0] * quarter : (quarters[-1] + 1) * quarter]
        return jnp.concatenate([ref[group, rows, lanes(q)] for q in quarters], axis=1)

    def by_slot(pieces):
        parts = []
        for slot in range(2):
            row = []
            for group, quarters in pieces:
                values = jnp.concatenate([sbuf[group, q] for q in quarters], axis=1).astype(F32)
                row.append((lanes_of(abuf, group, slice(slot, slot + 1), quarters) * values).astype(BF16))
            parts.append(jnp.concatenate(row, axis=1))
        return jnp.concatenate(parts, axis=0)

    def sums(v, pieces, chunk):
        rows = slice(chunk * 256, (chunk + 1) * 256)
        return nt(v, jnp.concatenate([lanes_of(foot, group, rows, quarters) for group, quarters in pieces], axis=1))

    def spread(*pieces, fresh=False):
        v = by_slot(pieces)
        for chunk in range(4):
            if fresh:
                wide[chunk] = sums(v, pieces, chunk)
            else:
                wide[chunk] += sums(v, pieces, chunk)

    spread((0, (0, 1, 2, 3)), fresh=True)
    for q in range(4):
        (ag_next, ag_last)[q % 2][q].wait_recv()
        ag_far[q].start()
    spread((3, (0, 2)), (1, (1, 3)))
    for c in (ag_next[1], ag_last[0], ag_next[3], ag_last[2]):
        c.wait_recv()
    spread((3, (1, 3)), (1, (0, 2)))
    ag_far[0].wait_recv()
    ag_far[1].wait_recv()
    spread((2, (0, 1)))
    ag_far[2].wait_recv()
    ag_far[3].wait_recv()
    ends = ((LEFT, left), (RIGHT, right))
    r_own = [copy(BK + k, wout.at[k, 0, top], rim.at[1 - k, 0], (t, d)) for k, d in ends]
    r_other = [copy(BK + 2 + k, wout.at[k, 1, top], rim.at[1 - k, 1], (mate, d)) for k, d in ends]
    r_swap = [copy(BK + 4 + k, wout.at[k, 0, bottom], swap.at[k], (mate, s)) for k, d in ends]
    r_sum = [copy(BK + 6 + k, wout.at[k, 1, bottom], rim.at[1 - k, 2], (mate, d)) for k, d in ends]
    r_mate = [copy(BK + 8 + k, wout.at[2 + k, 1], win.at[k], (mate, s)) for k in range(2)]
    last = ((2, (2, 3)),)
    v = by_slot(last)
    for k in (LEFT, RIGHT):
        total = wide[k] + sums(v, last, k)
        wide[k] = total
        wout[k, 0] = total[:chans].astype(BF16)
        wout[k, 1, 0:64] = total[chans : chans + 64].astype(BF16)
        r_swap[k].start()
        r_own[k].start()
        r_other[k].start()
    for k in range(2):
        total = wide[HEAD + k] + sums(v, last, HEAD + k)
        wide[HEAD + k] = total
        wout[2 + k, 1] = total[chans:].astype(BF16)
        r_mate[k].start()
    for k in (LEFT, RIGHT):
        r_swap[k].wait_recv()
        wout[k, 1, 64:128] = (wide[k, chans + 64 : 2 * chans] + swap[k].astype(F32)).astype(BF16)
        r_sum[k].start()
    for c in r_mate:
        c.wait_recv()
    for h in (1, 0):
        for c in (r_own[1 - h], r_other[1 - h], r_sum[1 - h]):
            c.wait_recv()
        rims = jnp.concatenate([rim[h, 0].astype(F32) + rim[h, 1].astype(F32), rim[h, 2].astype(F32)], axis=0)
        whole = wide[HEAD + h, 0:chans] + win[h].astype(F32) + rims
        adj_out[:, 0, h * 256 : (h + 1) * 256] = jnp.dot(jac_ref[...], whole.astype(BF16), preferred_element_type=F32)
    for group in (
        z_relayed, z_direct, z_cross, z_onward, z_mate, meta[0], meta[1], meta[2], far, to_next, to_last, ag_next, ag_last,
        ag_far, r_own, r_other, r_swap, r_sum, r_mate,
    ):
        for c in group:
            c.wait_send()


def body(state, obs_start, foot_weight, obs_slot, obs_frac, live_count, obs_values, jacobian, inv_var):
    n_space = lax.axis_size("space")
    levels = jacobian.shape[0]
    anywhere = pl.BlockSpec(memory_space=pl.ANY)
    vmem = pl.BlockSpec(memory_space=pltpu.VMEM)
    i32 = jnp.int32
    departures, adjoint = pl.pallas_call(
        functools.partial(kernel, n_space, 512 * n_space),
        out_shape=(
            pltpu.VMEM((512, 128), F32),
            pltpu.VMEM((levels, 1, 512), F32),
        ),
        in_specs=[anywhere] * 5 + [pl.BlockSpec(memory_space=pltpu.SMEM)] + [anywhere] * 3,
        out_specs=(vmem, vmem),
        scratch_shapes=[
            pltpu.VMEM((levels, 512), BF16),
            pltpu.VMEM((1, 512), i32),
            pltpu.VMEM((8, 512), BF16),
            pltpu.VMEM((1, 512), i32),
            pltpu.VMEM((1, 512), F32),
            pltpu.VMEM((512, 128), F32),
            pltpu.VMEM((levels, 128), BF16),
            pltpu.VMEM((1, 128), F32),
            pltpu.VMEM((3, 1, 512), i32),
            pltpu.VMEM((3, 8, 512), BF16),
            pltpu.VMEM((3, 1, 512), i32),
            pltpu.VMEM((3, 1, 512), F32),
            pltpu.VMEM((4, 1024, 512), BF16),
            pltpu.VMEM((4, 2, 128, 256), BF16),
            pltpu.VMEM((4, 256, 512), F32),
            pltpu.VMEM((4, 2, 512), F32),
            pltpu.VMEM((12, 128, 128), BF16),
            pltpu.VMEM((4, 128, 128), BF16),
            pltpu.VMEM((2, 4, 128, 128), BF16),
            pltpu.VMEM((4, 4, 128, 128), BF16),
            pltpu.VMEM((4, 256, 256), F32),
            pltpu.VMEM((4, 2, 128, 256), BF16),
            pltpu.VMEM((2, 128, 256), BF16),
            pltpu.VMEM((2, 3, 64, 256), BF16),
            pltpu.VMEM((2, 64, 256), BF16),
            pltpu.VMEM((128, 512), F32),
            pltpu.VMEM((128, 128), F32),
            pltpu.VMEM((128, 512), F32),
            pltpu.SemaphoreType.DMA((8,)),
            pltpu.SemaphoreType.DMA((COPIES,)),
            pltpu.SemaphoreType.DMA((COPIES,)),
        ],
        compiler_params=pltpu.CompilerParams(collective_id=0, has_side_effects=True),
        name="window",
    )(
        jnp.transpose(state[0]),
        obs_start[None],
        jnp.transpose(foot_weight),
        obs_slot[None],
        obs_frac[None],
        live_count,
        obs_values,
        jacobian,
        inv_var[None],
    )
    return departures, jnp.transpose(adjoint, (1, 2, 0))


def solution(mesh):
    return jax.shard_map(
        body,
        mesh=mesh,
        in_specs=(
            P("tm", "space", None),
            P(("tm", "space")),
            P(("tm", "space"), None),
            P(("tm", "space")),
            P(("tm", "space")),
            P("tm", "space"),
            P(("tm", "space"), None),
            P(),
            P(),
        ),
        out_specs=(P(("tm", "space"), None), P("tm", "space", None)),
        check_vma=False,
    )
```

```python
import functools

import jax
import jax.numpy as jnp
from jax import lax
from jax.experimental import pallas as pl
from jax.experimental.pallas import tpu as pltpu
from jax.sharding import PartitionSpec as P

MESH = pl.DeviceIdType.MESH
F32 = jnp.float32
BF16 = jnp.bfloat16

META, Z_MATE, Z_RELAYED, Z_REST, FAR, SUM, FIRST, SECOND, LAST, SWAP, RIMS = 0, 3, 4, 6, 7, 11, 15, 19, 20, 22, 24
ARRIVALS = 25

LEFT, RIGHT, HEAD, TAIL = 0, 1, 2, 3


def nt(a, b):
    return lax.dot_general(a, b, (((1,), (1,)), ((), ())), preferred_element_type=F32)


def kernel(
    n_space, total_cols,
    state_in, start_in, w_in, slot_in, frac_in, count_ref, obs_in, jac_in, inv_in,
    dep_out, adj_out,
    state_ref, start_ref, w_ref, slot_ref, frac_ref, obs_ref, jac_ref, inv_ref,
    o_pack, m_pack, m_w, foot, zbuf, acc, abuf, pout, relay, rin, sbuf, wide, wout, win, rim, swap, obs_t, inv_t, dep_t,
    load, send, recv,
):
    t = lax.axis_index("tm")
    s = lax.axis_index("space")
    mate = t + 1 - 2 * lax.rem(t, 2)
    y1 = lax.rem(mate + 2, 8)
    y2 = lax.rem(t + 4, 8)
    y3 = lax.rem(mate + 6, 8)
    left = lax.rem(s + n_space - 1, n_space)
    right = lax.rem(s + 1, n_space)
    chans = 128
    quarter = 128
    top, bottom = pl.ds(0, 64), pl.ds(64, 64)

    barrier = pltpu.get_barrier_semaphore()
    for peer in ((t, right), (t, left), (mate, left), (mate, right), (y2, s), (y1, s), (y3, s), (mate, s)):
        pl.semaphore_signal(barrier, inc=1, device_id=peer, device_id_type=MESH)

    loads = [
        pltpu.make_async_copy(src, dst, load.at[k])
        for k, (src, dst) in enumerate(
            (
                (state_in, state_ref), (jac_in, jac_ref), (start_in, start_ref), (w_in, w_ref), (slot_in, slot_ref),
                (frac_in, frac_ref), (obs_in, obs_ref), (inv_in, inv_ref),
            )
        )
    ]
    for c in loads:
        c.start()

    def copy(index, src, dst, device):
        return pltpu.make_async_remote_copy(
            src_ref=src, dst_ref=dst, send_sem=send.at[0], recv_sem=recv.at[index],
            device_id=device, device_id_type=MESH,
        )

    def arrived(index, ref):
        copy(index, ref, ref, (mate, s)).wait_recv()

    loads[0].wait()
    loads[1].wait()
    z = lax.dot_general(jac_ref[...], state_ref[...], (((0,), (0,)), ((), ())), preferred_element_type=F32).astype(BF16)
    zbuf[HEAD, 0] = z[:, :256]
    zbuf[TAIL, 0] = z[:, 256:]
    for c in loads[2:6]:
        c.wait()
    o_pack[0] = start_ref[...].astype(F32)
    o_pack[1] = slot_ref[...].astype(F32)
    o_pack[2] = frac_ref[...]
    o_pack[3] = jnp.zeros((1, 512), F32)

    pl.semaphore_wait(barrier, 8)

    sides = ((HEAD, RIGHT, left), (TAIL, LEFT, right))
    z_relayed = [copy(Z_RELAYED + k, zbuf.at[a, 0, top], zbuf.at[b, 0, top], (t, d)) for k, (a, b, d) in enumerate(sides)]
    z_direct = [copy(Z_REST, zbuf.at[a, 0, bottom], zbuf.at[b, 0, bottom], (t, d)) for a, b, d in sides]
    z_cross = [copy(Z_REST, zbuf.at[a, 0, bottom], zbuf.at[b, 1, bottom], (mate, d)) for a, b, d in sides]
    z_onward = [copy(Z_REST, zbuf.at[b, 0, top], zbuf.at[b, 1, top], (mate, s)) for a, b, d in sides]
    z_mate = [copy(Z_MATE, zbuf.at[a, 0], zbuf.at[a, 1], (mate, s)) for a, b, d in sides]
    fields = ((o_pack, m_pack), (w_ref, m_w))
    meta = {}
    for hop, peer in ((2, y2), (1, y1), (3, y3)):
        at = 3 - hop
        meta[at] = [copy(META + at, src, dst.at[at], (peer, s)) for src, dst in fields]
    for c in z_relayed + z_direct + z_cross + meta[1] + meta[2] + meta[0] + z_mate:
        c.start()

    def weight_of(slot, frac, held):
        return jnp.where(slot == held, 1.0 - frac, 0.0) + jnp.where(slot + 1 == held, frac, 0.0)

    def build(group, start, w, slot, frac):
        abuf[group, 0:1, :] = weight_of(slot, frac, t)
        abuf[group, 1:2, :] = weight_of(slot, frac, mate)
        local = jnp.bitwise_and(start - s * 512 + 256, total_cols - 1)
        row = lax.broadcasted_iota(jnp.int32, (8, 512), 0)
        ahead = jnp.bitwise_and(row - local, 7)
        weights = w.astype(F32)
        turned = jnp.zeros((8, 512), F32)
        for k in range(8):
            turned = turned + jnp.where(ahead == k, weights[k : k + 1, :], 0.0)
        block = lax.shift_right_arithmetic(local - row + 7, 3)

        for first, last, shift in ((0, 4, 0), (4, 8, 8), (8, 16, -4)):

            def rows(index, carry):
                parts = [jnp.where(block == (index + shift) * 8 + m, turned, 0.0) for m in range(8)]
                at = pl.ds(pl.multiple_of(index * 64, 64), 64)
                foot[group, at, :] = jnp.concatenate(parts, axis=0).astype(BF16)
                return carry

            lax.fori_loop(first, last, rows, 0)

    def columns(first):
        return jnp.concatenate(
            [
                jnp.concatenate([zbuf[first, 0], zbuf[first + 1, 0]], axis=1),
                jnp.concatenate([zbuf[first, 1], zbuf[first + 1, 1]], axis=1),
            ],
            axis=0,
        )

    def centre(group):
        acc[group] = jnp.dot(columns(HEAD), foot[group, 512:1024, :], preferred_element_type=F32)

    def gathered(group):
        at = group - 1
        arrived(META + at, foot.at[group, 0:16])
        build(group, m_pack[at, 0].astype(jnp.int32), m_w[at], m_pack[at, 1].astype(jnp.int32), m_pack[at, 2])

    build(0, start_ref[...], w_ref[...], slot_ref[...], frac_ref[...])
    for c in loads[6:]:
        c.wait()
    obs_t[...] = jnp.transpose(obs_ref[...])
    inv_t[...] = jnp.transpose(jnp.broadcast_to(inv_ref[...], (chans, chans)))
    arrived(Z_MATE, zbuf.at[HEAD : HEAD + 2, 1])
    centre(0)
    for group in (1, 3):
        gathered(group)
        centre(group)
    for k in (1, 0):
        z_relayed[k].wait_recv()
        z_onward[k].start()
    gathered(2)
    centre(2)
    arrived(Z_REST, zbuf.at[0:3, 0])

    def finish(group):
        total = acc[group] + jnp.dot(columns(LEFT), foot[group, 0:512, :], preferred_element_type=F32)
        return abuf[group, 0:1, :] * total[:chans] + abuf[group, 1:2, :] * total[chans:]

    def lanes(q):
        return slice(q * quarter, (q + 1) * quarter)

    far = [copy(FAR + q, pout.at[q], relay.at[q], ((y1, y3)[q % 2], s)) for q in range(4)]
    to_next = [copy(SUM + q, pout.at[4 + q], rin.at[0, q], (y1, s)) for q in range(4)]
    to_last = [copy(SUM + q, pout.at[8 + q], rin.at[1, q], (y3, s)) for q in range(4)]
    partial = finish(2)
    for q in range(4):
        pout[q] = partial[:, lanes(q)].astype(BF16)
        far[q].start()
    for group, base, copies, now in ((1, 4, to_next, 1), (3, 8, to_last, 0)):
        partial = finish(group)
        for q in (now, now + 2):
            pout[base + q] = partial[:, lanes(q)].astype(BF16)
            copies[q].start()
        for q in (1 - now, 3 - now):
            acc[group, 0:chans, lanes(q)] = partial[:, lanes(q)]
    acc[0, 0:chans] = finish(0)
    for q in range(4):
        group, base, copies = ((1, 4, to_next), (3, 8, to_last))[q % 2]
        far[q].wait_recv()
        pout[base + q] = (acc[group, 0:chans, lanes(q)] + relay[q].astype(F32)).astype(BF16)
        copies[q].start()

    ag_next = [copy(FIRST + q if q % 2 == 0 else SECOND, sbuf.at[0, q], sbuf.at[3, q], (y1, s)) for q in range(4)]
    ag_last = [copy(FIRST + q if q % 2 else SECOND, sbuf.at[0, q], sbuf.at[1, q], (y3, s)) for q in range(4)]
    ag_far = [
        copy(LAST + q // 2, sbuf.at[(3, 1)[q % 2], q], sbuf.at[2, q], ((y1, y3)[q % 2], s)) for q in range(4)
    ]
    column = lax.broadcasted_iota(jnp.int32, (1, quarter), 1)
    for q in range(4):
        arrived(SUM + q, rin.at[:, q])
        projected = acc[0, 0:chans, lanes(q)] + rin[0, q].astype(F32) + rin[1, q].astype(F32)
        live = column + q * quarter < count_ref[0, 0]
        departed = jnp.where(live, obs_t[:, lanes(q)] - projected, 0.0)
        dep_t[:, lanes(q)] = departed
        sbuf[0, q] = (departed * inv_t[:, 0:1]).astype(BF16)
        (ag_next, ag_last)[q % 2][q].start()
    for q in (0, 2):
        ag_next[q + 1].start()
        ag_last[q].start()

    dep_out[...] = jnp.transpose(dep_t[...])

    def lanes_of(ref, group, rows, quarters):
        if quarters[-1] - quarters[0] == len(quarters) - 1:
            return ref[group, rows, quarters[0] * quarter : (quarters[-1] + 1) * quarter]
        return jnp.concatenate([ref[group, rows, lanes(q)] for q in quarters], axis=1)

    def by_slot(pieces):
        parts = []
        for slot in range(2):
            row = []
            for group, quarters in pieces:
                values = jnp.concatenate([sbuf[group, q] for q in quarters], axis=1).astype(F32)
                row.append((lanes_of(abuf, group, slice(slot, slot + 1), quarters) * values).astype(BF16))
            parts.append(jnp.concatenate(row, axis=1))
        return jnp.concatenate(parts, axis=0)

    def sums(v, pieces, chunk):
        rows = slice(chunk * 256, (chunk + 1) * 256)
        return nt(v, jnp.concatenate([lanes_of(foot, group, rows, quarters) for group, quarters in pieces], axis=1))

    def spread(*pieces, fresh=False):
        v = by_slot(pieces)
        for chunk in range(4):
            if fresh:
                wide[chunk] = sums(v, pieces, chunk)
            else:
                wide[chunk] += sums(v, pieces, chunk)

    spread((0, (0, 1, 2, 3)), fresh=True)
    for q in range(4):
        (ag_next, ag_last)[q % 2][q].wait_recv()
        ag_far[q].start()
    spread((3, (0, 2)), (1, (1, 3)))
    arrived(SECOND, sbuf.at[3])
    spread((3, (1, 3)), (1, (0, 2)))
    arrived(LAST, sbuf.at[2, 0:2])
    spread((2, (0, 1)))
    arrived(LAST + 1, sbuf.at[2, 2:4])
    ends = ((LEFT, left), (RIGHT, right))
    r_own = [copy(RIMS, wout.at[k, 0, top], rim.at[1 - k, 0], (t, d)) for k, d in ends]
    r_other = [copy(RIMS, wout.at[k, 1, top], rim.at[1 - k, 1], (mate, d)) for k, d in ends]
    r_swap = [copy(SWAP + k, wout.at[k, 0, bottom], swap.at[k], (mate, s)) for k, d in ends]
    r_sum = [copy(RIMS, wout.at[k, 1, bottom], rim.at[1 - k, 2], (mate, d)) for k, d in ends]
    r_mate = [copy(RIMS, wout.at[2 + k, 1], win.at[k], (mate, s)) for k in range(2)]
    last = ((2, (2, 3)),)
    v = by_slot(last)
    for k in (LEFT, RIGHT):
        total = wide[k] + sums(v, last, k)
        wide[k] = total
        wout[k, 0] = total[:chans].astype(BF16)
        wout[k, 1, 0:64] = total[chans : chans + 64].astype(BF16)
        r_swap[k].start()
        r_own[k].start()
        r_other[k].start()
    for k in range(2):
        total = wide[HEAD + k] + sums(v, last, HEAD + k)
        wide[HEAD + k] = total
        wout[2 + k, 1] = total[chans:].astype(BF16)
        r_mate[k].start()
    for k in (LEFT, RIGHT):
        r_swap[k].wait_recv()
        wout[k, 1, 64:128] = (wide[k, chans + 64 : 2 * chans] + swap[k].astype(F32)).astype(BF16)
        r_sum[k].start()
    arrived(RIMS, pout.at[0:10])
    for h in range(2):
        rims = jnp.concatenate([rim[h, 0].astype(F32) + rim[h, 1].astype(F32), rim[h, 2].astype(F32)], axis=0)
        whole = wide[HEAD + h, 0:chans] + win[h].astype(F32) + rims
        adj_out[:, 0, h * 256 : (h + 1) * 256] = jnp.dot(jac_ref[...], whole.astype(BF16), preferred_element_type=F32)
    sent = foot.at[0:3, 0:528]
    copy(META, sent, sent, (mate, s)).wait_send()


def write(dep_in, adj_in, dep_out, adj_out, done):
    copies = [pltpu.make_async_copy(dep_in, dep_out, done.at[0]), pltpu.make_async_copy(adj_in, adj_out, done.at[1])]
    for c in copies:
        c.start()
    for c in copies:
        c.wait()


def body(state, obs_start, foot_weight, obs_slot, obs_frac, live_count, obs_values, jacobian, inv_var):
    n_space = lax.axis_size("space")
    levels = jacobian.shape[0]
    anywhere = pl.BlockSpec(memory_space=pl.ANY)
    vmem = pl.BlockSpec(memory_space=pltpu.VMEM)
    i32 = jnp.int32
    departures, adjoint = pl.pallas_call(
        functools.partial(kernel, n_space, 512 * n_space),
        out_shape=(
            pltpu.VMEM((512, 128), F32),
            pltpu.VMEM((levels, 1, 512), F32),
        ),
        in_specs=[anywhere] * 5 + [pl.BlockSpec(memory_space=pltpu.SMEM)] + [anywhere] * 3,
        out_specs=(vmem, vmem),
        scratch_shapes=[
            pltpu.VMEM((levels, 512), BF16),
            pltpu.VMEM((1, 512), i32),
            pltpu.VMEM((8, 512), BF16),
            pltpu.VMEM((1, 512), i32),
            pltpu.VMEM((1, 512), F32),
            pltpu.VMEM((512, 128), F32),
            pltpu.VMEM((levels, 128), BF16),
            pltpu.VMEM((1, 128), F32),
            pltpu.VMEM((4, 1, 512), F32),
            pltpu.VMEM((3, 4, 1, 512), F32),
            pltpu.VMEM((3, 8, 512), BF16),
            pltpu.VMEM((4, 1024, 512), BF16),
            pltpu.VMEM((4, 2, 128, 256), BF16),
            pltpu.VMEM((4, 256, 512), F32),
            pltpu.VMEM((4, 2, 512), F32),
            pltpu.VMEM((12, 128, 128), BF16),
            pltpu.VMEM((4, 128, 128), BF16),
            pltpu.VMEM((2, 4, 128, 128), BF16),
            pltpu.VMEM((4, 4, 128, 128), BF16),
            pltpu.VMEM((4, 256, 256), F32),
            pltpu.VMEM((4, 2, 128, 256), BF16),
            pltpu.VMEM((2, 128, 256), BF16),
            pltpu.VMEM((2, 3, 64, 256), BF16),
            pltpu.VMEM((2, 64, 256), BF16),
            pltpu.VMEM((128, 512), F32),
            pltpu.VMEM((128, 128), F32),
            pltpu.VMEM((128, 512), F32),
            pltpu.SemaphoreType.DMA((8,)),
            pltpu.SemaphoreType.DMA((1,)),
            pltpu.SemaphoreType.DMA((ARRIVALS,)),
        ],
        compiler_params=pltpu.CompilerParams(collective_id=0, has_side_effects=True),
        name="window",
    )(
        jnp.transpose(state[0]),
        obs_start[None],
        jnp.transpose(foot_weight),
        obs_slot[None],
        obs_frac[None],
        live_count,
        obs_values,
        jacobian,
        inv_var[None],
    )
    departures, adjoint = pl.pallas_call(
        write,
        out_shape=(jax.ShapeDtypeStruct(departures.shape, F32), jax.ShapeDtypeStruct(adjoint.shape, F32)),
        in_specs=[vmem] * 2,
        out_specs=(anywhere, anywhere),
        scratch_shapes=[pltpu.SemaphoreType.DMA((2,))],
        name="write",
    )(pltpu.with_memory_space_constraint(departures, pltpu.VMEM), pltpu.with_memory_space_constraint(adjoint, pltpu.VMEM))
    return departures, jnp.transpose(adjoint, (1, 2, 0))


def solution(mesh):
    return jax.shard_map(
        body,
        mesh=mesh,
        in_specs=(
            P("tm", "space", None),
            P(("tm", "space")),
            P(("tm", "space"), None),
            P(("tm", "space")),
            P(("tm", "space")),
            P("tm", "space"),
            P(("tm", "space"), None),
            P(),
            P(),
        ),
        out_specs=(P(("tm", "space"), None), P("tm", "space", None)),
        check_vma=False,
    )
```

```python
import functools

import jax
import jax.numpy as jnp
from jax import lax
from jax.experimental import pallas as pl
from jax.experimental.pallas import tpu as pltpu
from jax.sharding import PartitionSpec as P

MESH = pl.DeviceIdType.MESH
F32 = jnp.float32
BF16 = jnp.bfloat16

META, Z_MATE, Z_RELAYED, Z_REST, FAR, SUM, FIRST, SECOND, LAST, SWAP, RIMS, HELD = 0, 3, 4, 6, 7, 11, 15, 19, 20, 22, 24, 25
ARRIVALS = 26

LEFT, RIGHT, HEAD, TAIL = 0, 1, 2, 3


def nt(a, b):
    return lax.dot_general(a, b, (((1,), (1,)), ((), ())), preferred_element_type=F32)


def kernel(
    n_space, total_cols, holder,
    state_in, start_in, w_in, slot_in, frac_in, count_ref, obs_in, jac_in, inv_in,
    dep_out, adj_out,
    state_ref, start_ref, w_ref, slot_ref, frac_ref, obs_ref, jac_ref, inv_ref,
    o_pack, m_pack, m_w, held, foot, zbuf, acc, abuf, pout, relay, rin, sbuf, wide, wout, win, rim, swap, obs_t, inv_t, dep_t,
    load, send, recv, gate,
):
    t = lax.axis_index("tm")
    s = lax.axis_index("space")
    mate = t + 1 - 2 * lax.rem(t, 2)
    y1 = lax.rem(mate + 2, 8)
    y2 = lax.rem(t + 4, 8)
    y3 = lax.rem(mate + 6, 8)
    left = lax.rem(s + n_space - 1, n_space)
    right = lax.rem(s + 1, n_space)
    chans = 128
    quarter = 128
    top, bottom = pl.ds(0, 64), pl.ds(64, 64)

    core = lax.rem(t, 2)
    first_core, second_core = t - core, t - core + 1
    is_zero, is_last, is_holder = s == 0, s == n_space - 1, s == holder
    is_keeper = jnp.logical_and(is_holder, core == 1)

    barrier = pltpu.get_barrier_semaphore()

    def greet(core_index, tile):
        pl.semaphore_signal(barrier, inc=1, device_id=(core_index, tile), device_id_type=MESH)

    for peer in (t, mate):
        goes_on = jnp.where(is_last, 1, 0)
        to_holder = jnp.where(right == holder, 1, 0)
        normal = peer - to_holder * lax.rem(peer, 2)
        greet(goes_on * second_core + (1 - goes_on) * normal, goes_on * holder + (1 - goes_on) * right)
    for peer in (t, mate):
        greet(peer - jnp.where(left == holder, 1, 0) * lax.rem(peer, 2), left)
    for peer in (y2, y1, y3):
        greet(peer - jnp.where(is_holder, 1, 0) * lax.rem(peer, 2), s)
    greet(mate, s)

    @pl.when(is_zero)
    def _():
        greet(second_core, holder)

    @pl.when(is_holder)
    def _():
        greet(t, 0)
        greet(mate, 0)

    loads = [
        pltpu.make_async_copy(src, dst, load.at[k])
        for k, (src, dst) in enumerate(
            (
                (state_in, state_ref), (jac_in, jac_ref), (start_in, start_ref), (w_in, w_ref), (slot_in, slot_ref),
                (frac_in, frac_ref), (obs_in, obs_ref), (inv_in, inv_ref),
            )
        )
    ]
    for c in loads:
        c.start()

    def copy(index, src, dst, device, out=0):
        return pltpu.make_async_remote_copy(
            src_ref=src, dst_ref=dst, send_sem=send.at[out], recv_sem=recv.at[index],
            device_id=device, device_id_type=MESH,
        )

    def arrived(index, ref):
        copy(index, ref, ref, (mate, s)).wait_recv()

    loads[0].wait()
    loads[1].wait()
    z = lax.dot_general(jac_ref[...], state_ref[...], (((0,), (0,)), ((), ())), preferred_element_type=F32).astype(BF16)
    zbuf[HEAD, 0] = z[:, :256]
    zbuf[TAIL, 0] = z[:, 256:]
    for c in loads[2:6]:
        c.wait()
    o_pack[0] = start_ref[...].astype(F32)
    o_pack[1] = slot_ref[...].astype(F32)
    o_pack[2] = frac_ref[...]
    o_pack[3] = jnp.zeros((1, 512), F32)

    @pl.when(jnp.logical_not(is_keeper))
    def _():
        pl.semaphore_wait(barrier, 8 + 7 * jnp.where(is_holder, 1, 0))

    @pl.when(jnp.logical_and(is_holder, core == 0))
    def _():
        pl.semaphore_signal(gate, inc=1, device_id=(mate, s), device_id_type=MESH)

    @pl.when(is_keeper)
    def _():
        pl.semaphore_wait(gate, 1)

    sides = ((HEAD, RIGHT, left), (TAIL, LEFT, right))
    z_relayed = [copy(Z_RELAYED + k, zbuf.at[a, 0, top], zbuf.at[b, 0, top], (t, d), 1 - k) for k, (a, b, d) in enumerate(sides)]
    z_direct = [copy(Z_REST, zbuf.at[a, 0, bottom], zbuf.at[b, 0, bottom], (t, d), 1 - k) for k, (a, b, d) in enumerate(sides)]
    z_cross = [copy(Z_REST, zbuf.at[a, 0, bottom], zbuf.at[b, 1, bottom], (mate, d), 1 - k) for k, (a, b, d) in enumerate(sides)]
    z_onward = [copy(Z_REST, zbuf.at[b, 0, top], zbuf.at[b, 1, top], (mate, s)) for a, b, d in sides]
    z_mate = [copy(Z_MATE, zbuf.at[a, 0], zbuf.at[a, 1], (mate, s)) for a, b, d in sides]
    z_held = [copy(HELD, zbuf.at[HEAD, k], held.at[k], (t, holder), 1) for k in range(2)]
    last = n_space - 1
    z_passed = [
        copy(Z_RELAYED, held.at[1, top], zbuf.at[RIGHT, 0, top], (mate, last), 2),
        copy(Z_RELAYED, held.at[0, top], zbuf.at[RIGHT, 0, top], (t, last), 2),
        copy(Z_REST, held.at[1, bottom], zbuf.at[RIGHT, 0, bottom], (mate, last), 2),
        copy(Z_REST, held.at[0, bottom], zbuf.at[RIGHT, 1, bottom], (mate, last), 2),
        copy(Z_REST, held.at[0, bottom], zbuf.at[RIGHT, 0, bottom], (t, last), 2),
        copy(Z_REST, held.at[1, bottom], zbuf.at[RIGHT, 1, bottom], (t, last), 2),
    ]
    sends_ahead = jnp.logical_and(is_zero, core == 1)
    fields = ((o_pack, m_pack), (w_ref, m_w))
    meta = {}
    for hop, peer in ((2, y2), (1, y1), (3, y3)):
        at = 3 - hop
        meta[at] = [copy(META + at, src, dst.at[at], (peer, s)) for src, dst in fields]
    @pl.when(sends_ahead)
    def _():
        z_held[0].start()

    @pl.when(jnp.logical_not(is_zero))
    def _():
        for c in (z_relayed[0], z_direct[0], z_cross[0]):
            c.start()

    for c in [z_relayed[1], z_direct[1], z_cross[1]] + meta[1] + meta[2] + meta[0] + z_mate:
        c.start()

    def weight_of(slot, frac, held):
        return jnp.where(slot == held, 1.0 - frac, 0.0) + jnp.where(slot + 1 == held, frac, 0.0)

    def build(group, start, w, slot, frac):
        abuf[group, 0:1, :] = weight_of(slot, frac, t)
        abuf[group, 1:2, :] = weight_of(slot, frac, mate)
        local = jnp.bitwise_and(start - s * 512 + 256, total_cols - 1)
        row = lax.broadcasted_iota(jnp.int32, (8, 512), 0)
        ahead = jnp.bitwise_and(row - local, 7)
        weights = w.astype(F32)
        turned = jnp.zeros((8, 512), F32)
        for k in range(8):
            turned = turned + jnp.where(ahead == k, weights[k : k + 1, :], 0.0)
        block = lax.shift_right_arithmetic(local - row + 7, 3)

        for first, last, shift in ((0, 4, 0), (4, 8, 8), (8, 16, -4)):

            def rows(index, carry):
                parts = [jnp.where(block == (index + shift) * 8 + m, turned, 0.0) for m in range(8)]
                at = pl.ds(pl.multiple_of(index * 64, 64), 64)
                foot[group, at, :] = jnp.concatenate(parts, axis=0).astype(BF16)
                return carry

            lax.fori_loop(first, last, rows, 0)

    def columns(first):
        return jnp.concatenate(
            [
                jnp.concatenate([zbuf[first, 0], zbuf[first + 1, 0]], axis=1),
                jnp.concatenate([zbuf[first, 1], zbuf[first + 1, 1]], axis=1),
            ],
            axis=0,
        )

    def centre(group):
        acc[group] = jnp.dot(columns(HEAD), foot[group, 512:1024, :], preferred_element_type=F32)

    def gathered(group):
        at = group - 1
        arrived(META + at, foot.at[group, 0:16])
        build(group, m_pack[at, 0].astype(jnp.int32), m_w[at], m_pack[at, 1].astype(jnp.int32), m_pack[at, 2])

    build(0, start_ref[...], w_ref[...], slot_ref[...], frac_ref[...])
    for c in loads[6:]:
        c.wait()
    obs_t[...] = jnp.transpose(obs_ref[...])
    inv_t[...] = jnp.transpose(jnp.broadcast_to(inv_ref[...], (chans, chans)))
    arrived(Z_MATE, zbuf.at[HEAD : HEAD + 2, 1])

    @pl.when(sends_ahead)
    def _():
        z_held[1].start()

    centre(0)
    @pl.when(is_keeper)
    def _():
        pl.semaphore_wait(barrier, 7)
        arrived(HELD, held)
        for c in z_passed:
            c.start()
        for device in ((t, 0), (mate, 0)):
            pl.semaphore_signal(gate, inc=1, device_id=device, device_id_type=MESH)

    for k in (1, 0):
        z_relayed[k].wait_recv()
        z_onward[k].start()

    for group in (1, 3):
        gathered(group)
        centre(group)
    gathered(2)
    centre(2)
    arrived(Z_REST, zbuf.at[0:3, 0])

    def finish(group):
        total = acc[group] + jnp.dot(columns(LEFT), foot[group, 0:512, :], preferred_element_type=F32)
        return abuf[group, 0:1, :] * total[:chans] + abuf[group, 1:2, :] * total[chans:]

    def lanes(q):
        return slice(q * quarter, (q + 1) * quarter)

    far = [copy(FAR + q, pout.at[q], relay.at[q], ((y1, y3)[q % 2], s)) for q in range(4)]
    to_next = [copy(SUM + q, pout.at[4 + q], rin.at[0, q], (y1, s)) for q in range(4)]
    to_last = [copy(SUM + q, pout.at[8 + q], rin.at[1, q], (y3, s)) for q in range(4)]
    partial = finish(2)
    for q in range(4):
        pout[q] = partial[:, lanes(q)].astype(BF16)
        far[q].start()
    for group, base, copies, now in ((1, 4, to_next, 1), (3, 8, to_last, 0)):
        partial = finish(group)
        for q in (now, now + 2):
            pout[base + q] = partial[:, lanes(q)].astype(BF16)
            copies[q].start()
        for q in (1 - now, 3 - now):
            acc[group, 0:chans, lanes(q)] = partial[:, lanes(q)]
    acc[0, 0:chans] = finish(0)
    for q in range(4):
        group, base, copies = ((1, 4, to_next), (3, 8, to_last))[q % 2]
        far[q].wait_recv()
        pout[base + q] = (acc[group, 0:chans, lanes(q)] + relay[q].astype(F32)).astype(BF16)
        copies[q].start()

    ag_next = [copy(FIRST + q if q % 2 == 0 else SECOND, sbuf.at[0, q], sbuf.at[3, q], (y1, s)) for q in range(4)]
    ag_last = [copy(FIRST + q if q % 2 else SECOND, sbuf.at[0, q], sbuf.at[1, q], (y3, s)) for q in range(4)]
    ag_far = [
        copy(LAST + q // 2, sbuf.at[(3, 1)[q % 2], q], sbuf.at[2, q], ((y1, y3)[q % 2], s)) for q in range(4)
    ]
    column = lax.broadcasted_iota(jnp.int32, (1, quarter), 1)
    for q in range(4):
        arrived(SUM + q, rin.at[:, q])
        projected = acc[0, 0:chans, lanes(q)] + rin[0, q].astype(F32) + rin[1, q].astype(F32)
        live = column + q * quarter < count_ref[0, 0]
        departed = jnp.where(live, obs_t[:, lanes(q)] - projected, 0.0)
        dep_t[:, lanes(q)] = departed
        sbuf[0, q] = (departed * inv_t[:, 0:1]).astype(BF16)
        (ag_next, ag_last)[q % 2][q].start()
    for q in (0, 2):
        ag_next[q + 1].start()
        ag_last[q].start()

    dep_out[...] = jnp.transpose(dep_t[...])

    def lanes_of(ref, group, rows, quarters):
        if quarters[-1] - quarters[0] == len(quarters) - 1:
            return ref[group, rows, quarters[0] * quarter : (quarters[-1] + 1) * quarter]
        return jnp.concatenate([ref[group, rows, lanes(q)] for q in quarters], axis=1)

    def by_slot(pieces):
        parts = []
        for slot in range(2):
            row = []
            for group, quarters in pieces:
                values = jnp.concatenate([sbuf[group, q] for q in quarters], axis=1).astype(F32)
                row.append((lanes_of(abuf, group, slice(slot, slot + 1), quarters) * values).astype(BF16))
            parts.append(jnp.concatenate(row, axis=1))
        return jnp.concatenate(parts, axis=0)

    def sums(v, pieces, chunk):
        rows = slice(chunk * 256, (chunk + 1) * 256)
        return nt(v, jnp.concatenate([lanes_of(foot, group, rows, quarters) for group, quarters in pieces], axis=1))

    def spread(*pieces, fresh=False):
        v = by_slot(pieces)
        for chunk in range(4):
            if fresh:
                wide[chunk] = sums(v, pieces, chunk)
            else:
                wide[chunk] += sums(v, pieces, chunk)

    spread((0, (0, 1, 2, 3)), fresh=True)
    for q in range(4):
        (ag_next, ag_last)[q % 2][q].wait_recv()
        ag_far[q].start()
    spread((3, (0, 2)), (1, (1, 3)))
    arrived(SECOND, sbuf.at[3])
    spread((3, (1, 3)), (1, (0, 2)))
    arrived(LAST, sbuf.at[2, 0:2])
    spread((2, (0, 1)))
    arrived(LAST + 1, sbuf.at[2, 2:4])
    ends = ((LEFT, left), (RIGHT, right))
    r_own = [copy(RIMS, wout.at[k, 0, top], rim.at[1 - k, 0], (t, d)) for k, d in ends]
    r_other = [copy(RIMS, wout.at[k, 1, top], rim.at[1 - k, 1], (mate, d)) for k, d in ends]
    r_swap = [copy(SWAP + k, wout.at[k, 0, bottom], swap.at[k], (mate, s)) for k, d in ends]
    r_sum = [copy(RIMS, wout.at[k, 1, bottom], rim.at[1 - k, 2], (mate, d)) for k, d in ends]
    r_mate = [copy(RIMS, wout.at[2 + k, 1], win.at[k], (mate, s)) for k in range(2)]
    @pl.when(is_zero)
    def _():
        pl.semaphore_wait(gate, 1)

    final = ((2, (2, 3)),)
    v = by_slot(final)
    for k in (RIGHT, LEFT):
        total = wide[k] + sums(v, final, k)
        wide[k] = total
        wout[k, 0] = total[:chans].astype(BF16)
        wout[k, 1, 0:64] = total[chans : chans + 64].astype(BF16)
        r_swap[k].start()
        r_own[k].start()
        r_other[k].start()
    for k in range(2):
        total = wide[HEAD + k] + sums(v, final, HEAD + k)
        wide[HEAD + k] = total
        wout[2 + k, 1] = total[chans:].astype(BF16)
        r_mate[k].start()
    for k in (RIGHT, LEFT):
        r_swap[k].wait_recv()
        wout[k, 1, 64:128] = (wide[k, chans + 64 : 2 * chans] + swap[k].astype(F32)).astype(BF16)
        r_sum[k].start()
    arrived(RIMS, pout.at[0:10])
    for h in range(2):
        rims = jnp.concatenate([rim[h, 0].astype(F32) + rim[h, 1].astype(F32), rim[h, 2].astype(F32)], axis=0)
        whole = wide[HEAD + h, 0:chans] + win[h].astype(F32) + rims
        adj_out[:, 0, h * 256 : (h + 1) * 256] = jnp.dot(jac_ref[...], whole.astype(BF16), preferred_element_type=F32)
    def left_here(ref, out):
        copy(META, ref, ref, (mate, s), out).wait_send()

    left_here(foot.at[0:3, 0:496], 0)

    @pl.when(sends_ahead)
    def _():
        left_here(held, 1)

    @pl.when(jnp.logical_not(is_zero))
    def _():
        left_here(foot.at[0:3, 0:32], 1)

    @pl.when(is_keeper)
    def _():
        left_here(foot.at[0:3, 0:64], 2)


def write(dep_in, adj_in, dep_out, adj_out, done):
    copies = [pltpu.make_async_copy(dep_in, dep_out, done.at[0]), pltpu.make_async_copy(adj_in, adj_out, done.at[1])]
    for c in copies:
        c.start()
    for c in copies:
        c.wait()


def body(state, obs_start, foot_weight, obs_slot, obs_frac, live_count, obs_values, jacobian, inv_var):
    n_space = lax.axis_size("space")
    levels = jacobian.shape[0]
    anywhere = pl.BlockSpec(memory_space=pl.ANY)
    vmem = pl.BlockSpec(memory_space=pltpu.VMEM)
    i32 = jnp.int32
    departures, adjoint = pl.pallas_call(
        functools.partial(kernel, n_space, 512 * n_space, 3 if n_space > 4 else 2),
        out_shape=(
            pltpu.VMEM((512, 128), F32),
            pltpu.VMEM((levels, 1, 512), F32),
        ),
        in_specs=[anywhere] * 5 + [pl.BlockSpec(memory_space=pltpu.SMEM)] + [anywhere] * 3,
        out_specs=(vmem, vmem),
        scratch_shapes=[
            pltpu.VMEM((levels, 512), BF16),
            pltpu.VMEM((1, 512), i32),
            pltpu.VMEM((8, 512), BF16),
            pltpu.VMEM((1, 512), i32),
            pltpu.VMEM((1, 512), F32),
            pltpu.VMEM((512, 128), F32),
            pltpu.VMEM((levels, 128), BF16),
            pltpu.VMEM((1, 128), F32),
            pltpu.VMEM((4, 1, 512), F32),
            pltpu.VMEM((3, 4, 1, 512), F32),
            pltpu.VMEM((3, 8, 512), BF16),
            pltpu.VMEM((2, 128, 256), BF16),
            pltpu.VMEM((4, 1024, 512), BF16),
            pltpu.VMEM((4, 2, 128, 256), BF16),
            pltpu.VMEM((4, 256, 512), F32),
            pltpu.VMEM((4, 2, 512), F32),
            pltpu.VMEM((12, 128, 128), BF16),
            pltpu.VMEM((4, 128, 128), BF16),
            pltpu.VMEM((2, 4, 128, 128), BF16),
            pltpu.VMEM((4, 4, 128, 128), BF16),
            pltpu.VMEM((4, 256, 256), F32),
            pltpu.VMEM((4, 2, 128, 256), BF16),
            pltpu.VMEM((2, 128, 256), BF16),
            pltpu.VMEM((2, 3, 64, 256), BF16),
            pltpu.VMEM((2, 64, 256), BF16),
            pltpu.VMEM((128, 512), F32),
            pltpu.VMEM((128, 128), F32),
            pltpu.VMEM((128, 512), F32),
            pltpu.SemaphoreType.DMA((8,)),
            pltpu.SemaphoreType.DMA((3,)),
            pltpu.SemaphoreType.DMA((ARRIVALS,)),
            pltpu.SemaphoreType.REGULAR,
        ],
        compiler_params=pltpu.CompilerParams(collective_id=0, has_side_effects=True),
        name="window",
    )(
        jnp.transpose(state[0]),
        obs_start[None],
        jnp.transpose(foot_weight),
        obs_slot[None],
        obs_frac[None],
        live_count,
        obs_values,
        jacobian,
        inv_var[None],
    )
    departures, adjoint = pl.pallas_call(
        write,
        out_shape=(jax.ShapeDtypeStruct(departures.shape, F32), jax.ShapeDtypeStruct(adjoint.shape, F32)),
        in_specs=[vmem] * 2,
        out_specs=(anywhere, anywhere),
        scratch_shapes=[pltpu.SemaphoreType.DMA((2,))],
        name="write",
    )(pltpu.with_memory_space_constraint(departures, pltpu.VMEM), pltpu.with_memory_space_constraint(adjoint, pltpu.VMEM))
    return departures, jnp.transpose(adjoint, (1, 2, 0))


def solution(mesh):
    return jax.shard_map(
        body,
        mesh=mesh,
        in_specs=(
            P("tm", "space", None),
            P(("tm", "space")),
            P(("tm", "space"), None),
            P(("tm", "space")),
            P(("tm", "space")),
            P("tm", "space"),
            P(("tm", "space"), None),
            P(),
            P(),
        ),
        out_specs=(P(("tm", "space"), None), P("tm", "space", None)),
        check_vma=False,
    )
```

```python
import functools

import jax
import jax.numpy as jnp
from jax import lax
from jax.experimental import pallas as pl
from jax.experimental.pallas import tpu as pltpu
from jax.sharding import PartitionSpec as P

MESH = pl.DeviceIdType.MESH
F32 = jnp.float32
BF16 = jnp.bfloat16

META, Z_MATE, Z_RELAYED, Z_REST, FAR, SUM, FIRST, SECOND, LAST, SWAP, RIMS, HELD = 0, 3, 4, 6, 7, 11, 15, 19, 20, 22, 24, 25
ARRIVALS = 27

LEFT, RIGHT, HEAD, TAIL = 0, 1, 2, 3


def nt(a, b):
    return lax.dot_general(a, b, (((1,), (1,)), ((), ())), preferred_element_type=F32)


def kernel(
    n_space, total_cols, holder,
    state_in, start_in, w_in, slot_in, frac_in, count_ref, obs_in, jac_in, inv_in,
    dep_out, adj_out,
    state_ref, start_ref, w_ref, slot_ref, frac_ref, obs_ref, jac_ref, inv_ref,
    o_pack, m_pack, m_w, held, foot, zbuf, acc, abuf, pout, relay, rin, sbuf, wide, wout, win, rim, swap, obs_t, inv_t, dep_t,
    load, send, recv, gate,
):
    t = lax.axis_index("tm")
    s = lax.axis_index("space")
    mate = t + 1 - 2 * lax.rem(t, 2)
    y1 = lax.rem(mate + 2, 8)
    y2 = lax.rem(t + 4, 8)
    y3 = lax.rem(mate + 6, 8)
    left = lax.rem(s + n_space - 1, n_space)
    right = lax.rem(s + 1, n_space)
    chans = 128
    quarter = 128
    top, bottom = pl.ds(0, 64), pl.ds(64, 64)

    core = lax.rem(t, 2)
    first_core, second_core = t - core, t - core + 1
    is_zero, is_last, is_holder = s == 0, s == n_space - 1, s == holder
    is_keeper = jnp.logical_and(is_holder, core == 1)

    barrier = pltpu.get_barrier_semaphore()

    def greet(core_index, tile):
        pl.semaphore_signal(barrier, inc=1, device_id=(core_index, tile), device_id_type=MESH)

    for peer in (t, mate):
        goes_on = jnp.where(is_last, 1, 0)
        to_holder = jnp.where(right == holder, 1, 0)
        normal = peer - to_holder * lax.rem(peer, 2)
        greet(goes_on * second_core + (1 - goes_on) * normal, goes_on * holder + (1 - goes_on) * right)
    for peer in (t, mate):
        greet(peer - jnp.where(left == holder, 1, 0) * lax.rem(peer, 2), left)
    for peer in (y2, y1, y3):
        greet(peer - jnp.where(is_holder, 1, 0) * lax.rem(peer, 2), s)
    greet(mate, s)

    @pl.when(is_zero)
    def _():
        greet(second_core, holder)

    @pl.when(is_holder)
    def _():
        greet(t, 0)
        greet(mate, 0)

    loads = [
        pltpu.make_async_copy(src, dst, load.at[k])
        for k, (src, dst) in enumerate(
            (
                (state_in, state_ref), (jac_in, jac_ref), (start_in, start_ref), (w_in, w_ref), (slot_in, slot_ref),
                (frac_in, frac_ref), (obs_in, obs_ref), (inv_in, inv_ref),
            )
        )
    ]
    for c in loads:
        c.start()

    def copy(index, src, dst, device, out=0):
        return pltpu.make_async_remote_copy(
            src_ref=src, dst_ref=dst, send_sem=send.at[out], recv_sem=recv.at[index],
            device_id=device, device_id_type=MESH,
        )

    def arrived(index, ref):
        copy(index, ref, ref, (mate, s)).wait_recv()

    loads[0].wait()
    loads[1].wait()
    z = lax.dot_general(jac_ref[...], state_ref[...], (((0,), (0,)), ((), ())), preferred_element_type=F32).astype(BF16)
    zbuf[HEAD, 0] = z[:, :256]
    zbuf[TAIL, 0] = z[:, 256:]
    for c in loads[2:6]:
        c.wait()
    o_pack[0] = start_ref[...].astype(F32)
    o_pack[1] = slot_ref[...].astype(F32)
    o_pack[2] = frac_ref[...]
    o_pack[3] = jnp.zeros((1, 512), F32)

    @pl.when(jnp.logical_not(is_keeper))
    def _():
        pl.semaphore_wait(barrier, 8 + 7 * jnp.where(is_holder, 1, 0))

    @pl.when(jnp.logical_and(is_holder, core == 0))
    def _():
        pl.semaphore_signal(gate, inc=1, device_id=(mate, s), device_id_type=MESH)

    @pl.when(is_keeper)
    def _():
        pl.semaphore_wait(gate, 1)

    sides = ((HEAD, RIGHT, left), (TAIL, LEFT, right))
    z_relayed = [copy(Z_RELAYED + k, zbuf.at[a, 0, top], zbuf.at[b, 0, top], (t, d), 1 - k) for k, (a, b, d) in enumerate(sides)]
    z_direct = [copy(Z_REST, zbuf.at[a, 0, bottom], zbuf.at[b, 0, bottom], (t, d), 1 - k) for k, (a, b, d) in enumerate(sides)]
    z_cross = [copy(Z_REST, zbuf.at[a, 0, bottom], zbuf.at[b, 1, bottom], (mate, d), 1 - k) for k, (a, b, d) in enumerate(sides)]
    z_onward = [copy(Z_REST, zbuf.at[b, 0, top], zbuf.at[b, 1, top], (mate, s)) for a, b, d in sides]
    z_mate = [copy(Z_MATE, zbuf.at[a, 0], zbuf.at[a, 1], (mate, s)) for a, b, d in sides]
    z_held = [
        [copy(HELD + j, zbuf.at[HEAD, 0, rows], held.at[1 - k, rows], (second_core, holder), 1) for j, rows in ((0, top), (1, bottom))]
        for k in range(2)
    ]
    last = n_space - 1
    z_passed = [
        copy(Z_RELAYED, held.at[1, top], zbuf.at[RIGHT, 0, top], (mate, last), 2),
        copy(Z_RELAYED, held.at[0, top], zbuf.at[RIGHT, 0, top], (t, last), 2),
        copy(Z_REST, held.at[1, bottom], zbuf.at[RIGHT, 0, bottom], (mate, last), 2),
        copy(Z_REST, held.at[0, bottom], zbuf.at[RIGHT, 1, bottom], (mate, last), 2),
        copy(Z_REST, held.at[0, bottom], zbuf.at[RIGHT, 0, bottom], (t, last), 2),
        copy(Z_REST, held.at[1, bottom], zbuf.at[RIGHT, 1, bottom], (t, last), 2),
    ]
    fields = ((o_pack, m_pack), (w_ref, m_w))
    meta = {}
    for hop, peer in ((2, y2), (1, y1), (3, y3)):
        at = 3 - hop
        meta[at] = [copy(META + at, src, dst.at[at], (peer, s)) for src, dst in fields]
    for k in range(2):

        @pl.when(jnp.logical_and(is_zero, core == k))
        def _():
            for c in z_held[k]:
                c.start()

    @pl.when(jnp.logical_not(is_zero))
    def _():
        for c in (z_relayed[0], z_direct[0], z_cross[0]):
            c.start()

    for c in [z_relayed[1], z_direct[1], z_cross[1]] + meta[1] + meta[2] + meta[0] + z_mate:
        c.start()

    def weight_of(slot, frac, held):
        return jnp.where(slot == held, 1.0 - frac, 0.0) + jnp.where(slot + 1 == held, frac, 0.0)

    def build(group, start, w, slot, frac):
        abuf[group, 0:1, :] = weight_of(slot, frac, t)
        abuf[group, 1:2, :] = weight_of(slot, frac, mate)
        local = jnp.bitwise_and(start - s * 512 + 256, total_cols - 1)
        row = lax.broadcasted_iota(jnp.int32, (8, 512), 0)
        ahead = jnp.bitwise_and(row - local, 7)
        weights = w.astype(F32)
        turned = jnp.zeros((8, 512), F32)
        for k in range(8):
            turned = turned + jnp.where(ahead == k, weights[k : k + 1, :], 0.0)
        block = lax.shift_right_arithmetic(local - row + 7, 3)

        for first, last, shift in ((0, 4, 0), (4, 8, 8), (8, 16, -4)):

            def rows(index, carry):
                parts = [jnp.where(block == (index + shift) * 8 + m, turned, 0.0) for m in range(8)]
                at = pl.ds(pl.multiple_of(index * 64, 64), 64)
                foot[group, at, :] = jnp.concatenate(parts, axis=0).astype(BF16)
                return carry

            lax.fori_loop(first, last, rows, 0)

    def columns(first):
        return jnp.concatenate(
            [
                jnp.concatenate([zbuf[first, 0], zbuf[first + 1, 0]], axis=1),
                jnp.concatenate([zbuf[first, 1], zbuf[first + 1, 1]], axis=1),
            ],
            axis=0,
        )

    def centre(group):
        acc[group] = jnp.dot(columns(HEAD), foot[group, 512:1024, :], preferred_element_type=F32)

    def gathered(group):
        at = group - 1
        arrived(META + at, foot.at[group, 0:16])
        build(group, m_pack[at, 0].astype(jnp.int32), m_w[at], m_pack[at, 1].astype(jnp.int32), m_pack[at, 2])

    build(0, start_ref[...], w_ref[...], slot_ref[...], frac_ref[...])
    for c in loads[6:]:
        c.wait()
    obs_t[...] = jnp.transpose(obs_ref[...])
    inv_t[...] = jnp.transpose(jnp.broadcast_to(inv_ref[...], (chans, chans)))
    arrived(Z_MATE, zbuf.at[HEAD : HEAD + 2, 1])
    centre(0)
    @pl.when(is_keeper)
    def _():
        pl.semaphore_wait(barrier, 7)
        arrived(HELD, held.at[:, top])
        for c in z_passed[:2]:
            c.start()
        arrived(HELD + 1, held.at[:, bottom])
        for c in z_passed[2:]:
            c.start()
        for device in ((t, 0), (mate, 0)):
            pl.semaphore_signal(gate, inc=1, device_id=device, device_id_type=MESH)

    z_relayed[1].wait_recv()
    z_onward[1].start()
    z_relayed[0].wait_recv()
    z_onward[0].start()
    for group in (1, 3):
        gathered(group)
        centre(group)
    gathered(2)
    centre(2)
    arrived(Z_REST, zbuf.at[0:3, 0])

    def finish(group):
        total = acc[group] + jnp.dot(columns(LEFT), foot[group, 0:512, :], preferred_element_type=F32)
        return abuf[group, 0:1, :] * total[:chans] + abuf[group, 1:2, :] * total[chans:]

    def lanes(q):
        return slice(q * quarter, (q + 1) * quarter)

    far = [copy(FAR + q, pout.at[q], relay.at[q], ((y1, y3)[q % 2], s)) for q in range(4)]
    to_next = [copy(SUM + q, pout.at[4 + q], rin.at[0, q], (y1, s)) for q in range(4)]
    to_last = [copy(SUM + q, pout.at[8 + q], rin.at[1, q], (y3, s)) for q in range(4)]
    partial = finish(2)
    for q in range(4):
        pout[q] = partial[:, lanes(q)].astype(BF16)
        far[q].start()
    for group, base, copies, now in ((1, 4, to_next, 1), (3, 8, to_last, 0)):
        partial = finish(group)
        for q in (now, now + 2):
            pout[base + q] = partial[:, lanes(q)].astype(BF16)
            copies[q].start()
        for q in (1 - now, 3 - now):
            acc[group, 0:chans, lanes(q)] = partial[:, lanes(q)]
    acc[0, 0:chans] = finish(0)
    for q in range(4):
        group, base, copies = ((1, 4, to_next), (3, 8, to_last))[q % 2]
        far[q].wait_recv()
        pout[base + q] = (acc[group, 0:chans, lanes(q)] + relay[q].astype(F32)).astype(BF16)
        copies[q].start()

    ag_next = [copy(FIRST + q if q % 2 == 0 else SECOND, sbuf.at[0, q], sbuf.at[3, q], (y1, s)) for q in range(4)]
    ag_last = [copy(FIRST + q if q % 2 else SECOND, sbuf.at[0, q], sbuf.at[1, q], (y3, s)) for q in range(4)]
    ag_far = [
        copy(LAST + q // 2, sbuf.at[(3, 1)[q % 2], q], sbuf.at[2, q], ((y1, y3)[q % 2], s)) for q in range(4)
    ]
    column = lax.broadcasted_iota(jnp.int32, (1, quarter), 1)
    for q in range(4):
        arrived(SUM + q, rin.at[:, q])
        projected = acc[0, 0:chans, lanes(q)] + rin[0, q].astype(F32) + rin[1, q].astype(F32)
        live = column + q * quarter < count_ref[0, 0]
        departed = jnp.where(live, obs_t[:, lanes(q)] - projected, 0.0)
        dep_t[:, lanes(q)] = departed
        sbuf[0, q] = (departed * inv_t[:, 0:1]).astype(BF16)
        (ag_next, ag_last)[q % 2][q].start()
    for q in (0, 2):
        ag_next[q + 1].start()
        ag_last[q].start()

    dep_out[...] = jnp.transpose(dep_t[...])

    def lanes_of(ref, group, rows, quarters):
        if quarters[-1] - quarters[0] == len(quarters) - 1:
            return ref[group, rows, quarters[0] * quarter : (quarters[-1] + 1) * quarter]
        return jnp.concatenate([ref[group, rows, lanes(q)] for q in quarters], axis=1)

    def by_slot(pieces):
        parts = []
        for slot in range(2):
            row = []
            for group, quarters in pieces:
                values = jnp.concatenate([sbuf[group, q] for q in quarters], axis=1).astype(F32)
                row.append((lanes_of(abuf, group, slice(slot, slot + 1), quarters) * values).astype(BF16))
            parts.append(jnp.concatenate(row, axis=1))
        return jnp.concatenate(parts, axis=0)

    def sums(v, pieces, chunk):
        rows = slice(chunk * 256, (chunk + 1) * 256)
        return nt(v, jnp.concatenate([lanes_of(foot, group, rows, quarters) for group, quarters in pieces], axis=1))

    def spread(*pieces, fresh=False):
        v = by_slot(pieces)
        for chunk in range(4):
            if fresh:
                wide[chunk] = sums(v, pieces, chunk)
            else:
                wide[chunk] += sums(v, pieces, chunk)

    spread((0, (0, 1, 2, 3)), fresh=True)
    for q in range(4):
        (ag_next, ag_last)[q % 2][q].wait_recv()
        ag_far[q].start()
    spread((3, (0, 2)), (1, (1, 3)))
    arrived(SECOND, sbuf.at[3])
    spread((3, (1, 3)), (1, (0, 2)))
    arrived(LAST, sbuf.at[2, 0:2])
    spread((2, (0, 1)))
    arrived(LAST + 1, sbuf.at[2, 2:4])
    ends = ((LEFT, left), (RIGHT, right))
    r_own = [copy(RIMS, wout.at[k, 0, top], rim.at[1 - k, 0], (t, d)) for k, d in ends]
    r_other = [copy(RIMS, wout.at[k, 1, top], rim.at[1 - k, 1], (mate, d)) for k, d in ends]
    r_swap = [copy(SWAP + k, wout.at[k, 0, bottom], swap.at[k], (mate, s)) for k, d in ends]
    r_sum = [copy(RIMS, wout.at[k, 1, bottom], rim.at[1 - k, 2], (mate, d)) for k, d in ends]
    r_mate = [copy(RIMS, wout.at[2 + k, 1], win.at[k], (mate, s)) for k in range(2)]
    @pl.when(is_zero)
    def _():
        pl.semaphore_wait(gate, 1)

    final = ((2, (2, 3)),)
    v = by_slot(final)
    for k in (RIGHT, LEFT):
        total = wide[k] + sums(v, final, k)
        wide[k] = total
        wout[k, 0] = total[:chans].astype(BF16)
        wout[k, 1, 0:64] = total[chans : chans + 64].astype(BF16)
        r_swap[k].start()

        @pl.when(core == 0)
        def _():
            r_other[k].start()

        @pl.when(core == 1)
        def _():
            r_own[k].start()

    for k in (RIGHT, LEFT):
        r_swap[k].wait_recv()
        wout[k, 1, 64:128] = (wide[k, chans + 64 : 2 * chans] + swap[k].astype(F32)).astype(BF16)
        r_sum[k].start()

    @pl.when(core == 0)
    def _():
        for k in (RIGHT, LEFT):
            r_own[k].start()

    @pl.when(core == 1)
    def _():
        for k in (RIGHT, LEFT):
            r_other[k].start()

    for k in range(2):
        total = wide[HEAD + k] + sums(v, final, HEAD + k)
        wide[HEAD + k] = total
        wout[2 + k, 1] = total[chans:].astype(BF16)
        r_mate[k].start()
    arrived(RIMS, pout.at[0:10])
    for h in range(2):
        rims = jnp.concatenate([rim[h, 0].astype(F32) + rim[h, 1].astype(F32), rim[h, 2].astype(F32)], axis=0)
        whole = wide[HEAD + h, 0:chans] + win[h].astype(F32) + rims
        adj_out[:, 0, h * 256 : (h + 1) * 256] = jnp.dot(jac_ref[...], whole.astype(BF16), preferred_element_type=F32)
    def left_here(ref, out):
        copy(META, ref, ref, (mate, s), out).wait_send()

    left_here(foot.at[0:3, 0:496], 0)

    @pl.when(is_zero)
    def _():
        left_here(held.at[0], 1)

    @pl.when(jnp.logical_not(is_zero))
    def _():
        left_here(foot.at[0:3, 0:32], 1)

    @pl.when(is_keeper)
    def _():
        left_here(foot.at[0:3, 0:64], 2)


def write(dep_in, adj_in, dep_out, adj_out, done):
    copies = [pltpu.make_async_copy(dep_in, dep_out, done.at[0]), pltpu.make_async_copy(adj_in, adj_out, done.at[1])]
    for c in copies:
        c.start()
    for c in copies:
        c.wait()


def body(state, obs_start, foot_weight, obs_slot, obs_frac, live_count, obs_values, jacobian, inv_var):
    n_space = lax.axis_size("space")
    levels = jacobian.shape[0]
    anywhere = pl.BlockSpec(memory_space=pl.ANY)
    vmem = pl.BlockSpec(memory_space=pltpu.VMEM)
    i32 = jnp.int32
    departures, adjoint = pl.pallas_call(
        functools.partial(kernel, n_space, 512 * n_space, 3 if n_space > 4 else 2),
        out_shape=(
            pltpu.VMEM((512, 128), F32),
            pltpu.VMEM((levels, 1, 512), F32),
        ),
        in_specs=[anywhere] * 5 + [pl.BlockSpec(memory_space=pltpu.SMEM)] + [anywhere] * 3,
        out_specs=(vmem, vmem),
        scratch_shapes=[
            pltpu.VMEM((levels, 512), BF16),
            pltpu.VMEM((1, 512), i32),
            pltpu.VMEM((8, 512), BF16),
            pltpu.VMEM((1, 512), i32),
            pltpu.VMEM((1, 512), F32),
            pltpu.VMEM((512, 128), F32),
            pltpu.VMEM((levels, 128), BF16),
            pltpu.VMEM((1, 128), F32),
            pltpu.VMEM((4, 1, 512), F32),
            pltpu.VMEM((3, 4, 1, 512), F32),
            pltpu.VMEM((3, 8, 512), BF16),
            pltpu.VMEM((2, 128, 256), BF16),
            pltpu.VMEM((4, 1024, 512), BF16),
            pltpu.VMEM((4, 2, 128, 256), BF16),
            pltpu.VMEM((4, 256, 512), F32),
            pltpu.VMEM((4, 2, 512), F32),
            pltpu.VMEM((12, 128, 128), BF16),
            pltpu.VMEM((4, 128, 128), BF16),
            pltpu.VMEM((2, 4, 128, 128), BF16),
            pltpu.VMEM((4, 4, 128, 128), BF16),
            pltpu.VMEM((4, 256, 256), F32),
            pltpu.VMEM((4, 2, 128, 256), BF16),
            pltpu.VMEM((2, 128, 256), BF16),
            pltpu.VMEM((2, 3, 64, 256), BF16),
            pltpu.VMEM((2, 64, 256), BF16),
            pltpu.VMEM((128, 512), F32),
            pltpu.VMEM((128, 128), F32),
            pltpu.VMEM((128, 512), F32),
            pltpu.SemaphoreType.DMA((8,)),
            pltpu.SemaphoreType.DMA((3,)),
            pltpu.SemaphoreType.DMA((ARRIVALS,)),
            pltpu.SemaphoreType.REGULAR,
        ],
        compiler_params=pltpu.CompilerParams(collective_id=0, has_side_effects=True),
        name="window",
    )(
        jnp.transpose(state[0]),
        obs_start[None],
        jnp.transpose(foot_weight),
        obs_slot[None],
        obs_frac[None],
        live_count,
        obs_values,
        jacobian,
        inv_var[None],
    )
    departures, adjoint = pl.pallas_call(
        write,
        out_shape=(jax.ShapeDtypeStruct(departures.shape, F32), jax.ShapeDtypeStruct(adjoint.shape, F32)),
        in_specs=[vmem] * 2,
        out_specs=(anywhere, anywhere),
        scratch_shapes=[pltpu.SemaphoreType.DMA((2,))],
        name="write",
    )(pltpu.with_memory_space_constraint(departures, pltpu.VMEM), pltpu.with_memory_space_constraint(adjoint, pltpu.VMEM))
    return departures, jnp.transpose(adjoint, (1, 2, 0))


def solution(mesh):
    return jax.shard_map(
        body,
        mesh=mesh,
        in_specs=(
            P("tm", "space", None),
            P(("tm", "space")),
            P(("tm", "space"), None),
            P(("tm", "space")),
            P(("tm", "space")),
            P("tm", "space"),
            P(("tm", "space"), None),
            P(),
            P(),
        ),
        out_specs=(P(("tm", "space"), None), P("tm", "space", None)),
        check_vma=False,
    )
```

```python
import functools

import jax
import jax.numpy as jnp
from jax import lax
from jax.experimental import pallas as pl
from jax.experimental.pallas import tpu as pltpu
from jax.sharding import PartitionSpec as P

MESH = pl.DeviceIdType.MESH
F32 = jnp.float32
BF16 = jnp.bfloat16

META, Z_MATE, Z_RELAYED, Z_REST, FAR, SUM, FIRST, SECOND, LAST, SWAP, RIMS, W_MATE, HELD = 0, 3, 4, 6, 7, 11, 15, 19, 20, 22, 24, 26, 27
ARRIVALS = 29

LEFT, RIGHT, HEAD, TAIL = 0, 1, 2, 3


def nt(a, b):
    return lax.dot_general(a, b, (((1,), (1,)), ((), ())), preferred_element_type=F32)


def kernel(
    n_space, total_cols, holder,
    state_in, start_in, w_in, slot_in, frac_in, count_ref, obs_in, jac_in, inv_in,
    dep_out, adj_out,
    state_ref, start_ref, w_ref, slot_ref, frac_ref, obs_ref, jac_ref, inv_ref,
    o_pack, m_pack, m_w, held, foot, zbuf, acc, abuf, pout, relay, rin, sbuf, wide, wout, win, rim, swap, obs_t, inv_t, dep_t,
    load, send, recv, gate,
):
    t = lax.axis_index("tm")
    s = lax.axis_index("space")
    mate = t + 1 - 2 * lax.rem(t, 2)
    y1 = lax.rem(mate + 2, 8)
    y2 = lax.rem(t + 4, 8)
    y3 = lax.rem(mate + 6, 8)
    left = lax.rem(s + n_space - 1, n_space)
    right = lax.rem(s + 1, n_space)
    chans = 128
    quarter = 128
    top, bottom = pl.ds(0, 64), pl.ds(64, 64)

    core = lax.rem(t, 2)
    first_core, second_core = t - core, t - core + 1
    is_zero, is_last, is_holder = s == 0, s == n_space - 1, s == holder
    is_keeper = jnp.logical_and(is_holder, core == 1)

    barrier = pltpu.get_barrier_semaphore()

    def greet(core_index, tile):
        pl.semaphore_signal(barrier, inc=1, device_id=(core_index, tile), device_id_type=MESH)

    for peer in (t, mate):
        goes_on = jnp.where(is_last, 1, 0)
        to_holder = jnp.where(right == holder, 1, 0)
        normal = peer - to_holder * lax.rem(peer, 2)
        greet(goes_on * second_core + (1 - goes_on) * normal, goes_on * holder + (1 - goes_on) * right)
    for peer in (t, mate):
        greet(peer - jnp.where(left == holder, 1, 0) * lax.rem(peer, 2), left)
    for peer in (y2, y1, y3):
        greet(peer - jnp.where(is_holder, 1, 0) * lax.rem(peer, 2), s)
    greet(mate, s)

    @pl.when(is_zero)
    def _():
        greet(second_core, holder)

    @pl.when(is_holder)
    def _():
        greet(t, 0)
        greet(mate, 0)

    loads = [
        pltpu.make_async_copy(src, dst, load.at[k])
        for k, (src, dst) in enumerate(
            (
                (state_in, state_ref), (jac_in, jac_ref), (start_in, start_ref), (w_in, w_ref), (slot_in, slot_ref),
                (frac_in, frac_ref), (obs_in, obs_ref), (inv_in, inv_ref),
            )
        )
    ]
    for c in loads:
        c.start()

    def copy(index, src, dst, device, out=0):
        return pltpu.make_async_remote_copy(
            src_ref=src, dst_ref=dst, send_sem=send.at[out], recv_sem=recv.at[index],
            device_id=device, device_id_type=MESH,
        )

    def arrived(index, ref):
        copy(index, ref, ref, (mate, s)).wait_recv()

    loads[0].wait()
    loads[1].wait()
    z = lax.dot_general(jac_ref[...], state_ref[...], (((0,), (0,)), ((), ())), preferred_element_type=F32).astype(BF16)
    zbuf[HEAD, 0] = z[:, :256]
    zbuf[TAIL, 0] = z[:, 256:]
    for c in loads[2:6]:
        c.wait()
    o_pack[0] = start_ref[...].astype(F32)
    o_pack[1] = slot_ref[...].astype(F32)
    o_pack[2] = frac_ref[...]
    o_pack[3] = jnp.zeros((1, 512), F32)

    @pl.when(jnp.logical_not(is_keeper))
    def _():
        pl.semaphore_wait(barrier, 8 + 7 * jnp.where(is_holder, 1, 0))

    @pl.when(jnp.logical_and(is_holder, core == 0))
    def _():
        pl.semaphore_signal(gate, inc=1, device_id=(mate, s), device_id_type=MESH)

    @pl.when(is_keeper)
    def _():
        pl.semaphore_wait(gate, 1)

    sides = ((HEAD, RIGHT, left), (TAIL, LEFT, right))
    z_relayed = [copy(Z_RELAYED + k, zbuf.at[a, 0, top], zbuf.at[b, 0, top], (t, d), 1 - k) for k, (a, b, d) in enumerate(sides)]
    z_direct = [copy(Z_REST, zbuf.at[a, 0, bottom], zbuf.at[b, 0, bottom], (t, d), 1 - k) for k, (a, b, d) in enumerate(sides)]
    z_cross = [copy(Z_REST, zbuf.at[a, 0, bottom], zbuf.at[b, 1, bottom], (mate, d), 1 - k) for k, (a, b, d) in enumerate(sides)]
    z_onward = [copy(Z_REST, zbuf.at[b, 0, top], zbuf.at[b, 1, top], (mate, s)) for a, b, d in sides]
    z_mate = [copy(Z_MATE, zbuf.at[a, 0], zbuf.at[a, 1], (mate, s)) for a, b, d in sides]
    z_held = [
        [copy(HELD + j, zbuf.at[HEAD, 0, rows], held.at[1 - k, rows], (second_core, holder), 1) for j, rows in ((0, top), (1, bottom))]
        for k in range(2)
    ]
    last = n_space - 1
    z_passed = [
        copy(Z_RELAYED, held.at[1, top], zbuf.at[RIGHT, 0, top], (mate, last), 2),
        copy(Z_RELAYED, held.at[0, top], zbuf.at[RIGHT, 0, top], (t, last), 2),
        copy(Z_REST, held.at[1, bottom], zbuf.at[RIGHT, 0, bottom], (mate, last), 2),
        copy(Z_REST, held.at[0, bottom], zbuf.at[RIGHT, 1, bottom], (mate, last), 2),
        copy(Z_REST, held.at[0, bottom], zbuf.at[RIGHT, 0, bottom], (t, last), 2),
        copy(Z_REST, held.at[1, bottom], zbuf.at[RIGHT, 1, bottom], (t, last), 2),
    ]
    fields = ((o_pack, m_pack), (w_ref, m_w))
    meta = {}
    for hop, peer in ((2, y2), (1, y1), (3, y3)):
        at = 3 - hop
        meta[at] = [copy(META + at, src, dst.at[at], (peer, s)) for src, dst in fields]
    for k in range(2):

        @pl.when(jnp.logical_and(is_zero, core == k))
        def _():
            for c in z_held[k]:
                c.start()

    gives_way = s == holder + 1

    @pl.when(jnp.logical_not(jnp.logical_or(is_zero, gives_way)))
    def _():
        for c in (z_relayed[0], z_direct[0], z_cross[0]):
            c.start()

    for c in [z_relayed[1], z_direct[1], z_cross[1]] + meta[1] + meta[2] + meta[0] + z_mate:
        c.start()

    def weight_of(slot, frac, held):
        return jnp.where(slot == held, 1.0 - frac, 0.0) + jnp.where(slot + 1 == held, frac, 0.0)

    def build(group, start, w, slot, frac):
        abuf[group, 0:1, :] = weight_of(slot, frac, t)
        abuf[group, 1:2, :] = weight_of(slot, frac, mate)
        local = jnp.bitwise_and(start - s * 512 + 256, total_cols - 1)
        row = lax.broadcasted_iota(jnp.int32, (8, 512), 0)
        ahead = jnp.bitwise_and(row - local, 7)
        weights = w.astype(F32)
        turned = jnp.zeros((8, 512), F32)
        for k in range(8):
            turned = turned + jnp.where(ahead == k, weights[k : k + 1, :], 0.0)
        block = lax.shift_right_arithmetic(local - row + 7, 3)

        for first, last, shift in ((0, 4, 0), (4, 8, 8), (8, 16, -4)):

            def rows(index, carry):
                parts = [jnp.where(block == (index + shift) * 8 + m, turned, 0.0) for m in range(8)]
                at = pl.ds(pl.multiple_of(index * 64, 64), 64)
                foot[group, at, :] = jnp.concatenate(parts, axis=0).astype(BF16)
                return carry

            lax.fori_loop(first, last, rows, 0)

    def columns(first):
        return jnp.concatenate(
            [
                jnp.concatenate([zbuf[first, 0], zbuf[first + 1, 0]], axis=1),
                jnp.concatenate([zbuf[first, 1], zbuf[first + 1, 1]], axis=1),
            ],
            axis=0,
        )

    def centre(group):
        acc[group] = jnp.dot(columns(HEAD), foot[group, 512:1024, :], preferred_element_type=F32)

    def gathered(group):
        at = group - 1
        arrived(META + at, foot.at[group, 0:16])
        build(group, m_pack[at, 0].astype(jnp.int32), m_w[at], m_pack[at, 1].astype(jnp.int32), m_pack[at, 2])

    build(0, start_ref[...], w_ref[...], slot_ref[...], frac_ref[...])
    for c in loads[6:]:
        c.wait()
    obs_t[...] = jnp.transpose(obs_ref[...])
    inv_t[...] = jnp.transpose(jnp.broadcast_to(inv_ref[...], (chans, chans)))
    arrived(Z_MATE, zbuf.at[HEAD : HEAD + 2, 1])

    @pl.when(gives_way)
    def _():
        for c in (z_relayed[0], z_direct[0], z_cross[0]):
            c.start()

    centre(0)
    @pl.when(is_keeper)
    def _():
        pl.semaphore_wait(barrier, 7)
        arrived(HELD, held.at[:, top])
        for c in z_passed[:2]:
            c.start()
        arrived(HELD + 1, held.at[:, bottom])
        for c in z_passed[2:]:
            c.start()
        for device in ((t, 0), (mate, 0)):
            pl.semaphore_signal(gate, inc=1, device_id=device, device_id_type=MESH)

    z_relayed[1].wait_recv()
    z_onward[1].start()
    z_relayed[0].wait_recv()
    z_onward[0].start()
    for group in (1, 3):
        gathered(group)
        centre(group)
    gathered(2)
    centre(2)
    arrived(Z_REST, zbuf.at[0:3, 0])

    def finish(group):
        total = acc[group] + jnp.dot(columns(LEFT), foot[group, 0:512, :], preferred_element_type=F32)
        return abuf[group, 0:1, :] * total[:chans] + abuf[group, 1:2, :] * total[chans:]

    def lanes(q):
        return slice(q * quarter, (q + 1) * quarter)

    far = [copy(FAR + q, pout.at[q], relay.at[q], ((y1, y3)[q % 2], s)) for q in range(4)]
    to_next = [copy(SUM + q, pout.at[4 + q], rin.at[0, q], (y1, s)) for q in range(4)]
    to_last = [copy(SUM + q, pout.at[8 + q], rin.at[1, q], (y3, s)) for q in range(4)]
    partial = finish(2)
    for q in range(4):
        pout[q] = partial[:, lanes(q)].astype(BF16)
        far[q].start()
    for group, base, copies, now in ((1, 4, to_next, 1), (3, 8, to_last, 0)):
        partial = finish(group)
        for q in (now, now + 2):
            pout[base + q] = partial[:, lanes(q)].astype(BF16)
            copies[q].start()
        for q in (1 - now, 3 - now):
            acc[group, 0:chans, lanes(q)] = partial[:, lanes(q)]
    acc[0, 0:chans] = finish(0)
    for q in range(4):
        group, base, copies = ((1, 4, to_next), (3, 8, to_last))[q % 2]
        far[q].wait_recv()
        pout[base + q] = (acc[group, 0:chans, lanes(q)] + relay[q].astype(F32)).astype(BF16)
        copies[q].start()

    ag_next = [copy(FIRST + q if q % 2 == 0 else SECOND, sbuf.at[0, q], sbuf.at[3, q], (y1, s)) for q in range(4)]
    ag_last = [copy(FIRST + q if q % 2 else SECOND, sbuf.at[0, q], sbuf.at[1, q], (y3, s)) for q in range(4)]
    ag_far = [
        copy(LAST + q // 2, sbuf.at[(3, 1)[q % 2], q], sbuf.at[2, q], ((y1, y3)[q % 2], s)) for q in range(4)
    ]
    column = lax.broadcasted_iota(jnp.int32, (1, quarter), 1)
    for q in range(4):
        arrived(SUM + q, rin.at[:, q])
        projected = acc[0, 0:chans, lanes(q)] + rin[0, q].astype(F32) + rin[1, q].astype(F32)
        live = column + q * quarter < count_ref[0, 0]
        departed = jnp.where(live, obs_t[:, lanes(q)] - projected, 0.0)
        dep_t[:, lanes(q)] = departed
        sbuf[0, q] = (departed * inv_t[:, 0:1]).astype(BF16)
        (ag_next, ag_last)[q % 2][q].start()
    for q in (0, 2):
        ag_next[q + 1].start()
        ag_last[q].start()

    dep_out[...] = jnp.transpose(dep_t[...])

    def lanes_of(ref, group, rows, quarters):
        if quarters[-1] - quarters[0] == len(quarters) - 1:
            return ref[group, rows, quarters[0] * quarter : (quarters[-1] + 1) * quarter]
        return jnp.concatenate([ref[group, rows, lanes(q)] for q in quarters], axis=1)

    def by_slot(pieces):
        parts = []
        for slot in range(2):
            row = []
            for group, quarters in pieces:
                values = jnp.concatenate([sbuf[group, q] for q in quarters], axis=1).astype(F32)
                row.append((lanes_of(abuf, group, slice(slot, slot + 1), quarters) * values).astype(BF16))
            parts.append(jnp.concatenate(row, axis=1))
        return jnp.concatenate(parts, axis=0)

    def sums(v, pieces, chunk):
        rows = slice(chunk * 256, (chunk + 1) * 256)
        return nt(v, jnp.concatenate([lanes_of(foot, group, rows, quarters) for group, quarters in pieces], axis=1))

    def spread(*pieces, fresh=False):
        v = by_slot(pieces)
        for chunk in range(4):
            if fresh:
                wide[chunk] = sums(v, pieces, chunk)
            else:
                wide[chunk] += sums(v, pieces, chunk)

    spread((0, (0, 1, 2, 3)), fresh=True)
    for q in range(4):
        (ag_next, ag_last)[q % 2][q].wait_recv()
        ag_far[q].start()
    spread((3, (0, 2)), (1, (1, 3)))
    arrived(SECOND, sbuf.at[3])
    spread((3, (1, 3)), (1, (0, 2)))
    arrived(LAST, sbuf.at[2, 0:2])
    spread((2, (0, 1)))
    arrived(LAST + 1, sbuf.at[2, 2:4])
    ends = ((LEFT, left), (RIGHT, right))
    r_own = [copy(RIMS + k, wout.at[k, 0, top], rim.at[1 - k, 0], (t, d)) for k, d in ends]
    r_other = [copy(RIMS + k, wout.at[k, 1, top], rim.at[1 - k, 1], (mate, d)) for k, d in ends]
    r_swap = [copy(SWAP + k, wout.at[k, 0, bottom], swap.at[k], (mate, s)) for k, d in ends]
    r_sum = [copy(RIMS + k, wout.at[k, 1, bottom], rim.at[1 - k, 2], (mate, d)) for k, d in ends]
    r_mate = [copy(W_MATE, wout.at[2 + k, 1], win.at[k], (mate, s)) for k in range(2)]
    @pl.when(is_zero)
    def _():
        pl.semaphore_wait(gate, 1)

    final = ((2, (2, 3)),)
    v = by_slot(final)
    for k in (RIGHT, LEFT):
        total = wide[k] + sums(v, final, k)
        wide[k] = total
        wout[k, 0] = total[:chans].astype(BF16)
        wout[k, 1, 0:64] = total[chans : chans + 64].astype(BF16)
        r_swap[k].start()

        @pl.when(core == 0)
        def _():
            r_other[k].start()

        @pl.when(core == 1)
        def _():
            r_own[k].start()

    for k in (RIGHT, LEFT):
        r_swap[k].wait_recv()
        wout[k, 1, 64:128] = (wide[k, chans + 64 : 2 * chans] + swap[k].astype(F32)).astype(BF16)
        r_sum[k].start()

    @pl.when(core == 0)
    def _():
        for k in (RIGHT, LEFT):
            r_own[k].start()

    @pl.when(core == 1)
    def _():
        for k in (RIGHT, LEFT):
            r_other[k].start()

    for k in range(2):
        total = wide[HEAD + k] + sums(v, final, HEAD + k)
        wide[HEAD + k] = total
        wout[2 + k, 1] = total[chans:].astype(BF16)
        r_mate[k].start()
    arrived(W_MATE, win)
    for h in (1, 0):
        arrived(RIMS + 1 - h, rim.at[h])
        rims = jnp.concatenate([rim[h, 0].astype(F32) + rim[h, 1].astype(F32), rim[h, 2].astype(F32)], axis=0)
        whole = wide[HEAD + h, 0:chans] + win[h].astype(F32) + rims
        adj_out[:, 0, h * 256 : (h + 1) * 256] = jnp.dot(jac_ref[...], whole.astype(BF16), preferred_element_type=F32)
    def left_here(ref, out):
        copy(META, ref, ref, (mate, s), out).wait_send()

    left_here(foot.at[0:3, 0:496], 0)

    @pl.when(is_zero)
    def _():
        left_here(held.at[0], 1)

    @pl.when(jnp.logical_not(is_zero))
    def _():
        left_here(foot.at[0:3, 0:32], 1)

    @pl.when(is_keeper)
    def _():
        left_here(foot.at[0:3, 0:64], 2)


def write(dep_in, adj_in, dep_out, adj_out, done):
    copies = [pltpu.make_async_copy(dep_in, dep_out, done.at[0]), pltpu.make_async_copy(adj_in, adj_out, done.at[1])]
    for c in copies:
        c.start()
    for c in copies:
        c.wait()


def body(state, obs_start, foot_weight, obs_slot, obs_frac, live_count, obs_values, jacobian, inv_var):
    n_space = lax.axis_size("space")
    levels = jacobian.shape[0]
    anywhere = pl.BlockSpec(memory_space=pl.ANY)
    vmem = pl.BlockSpec(memory_space=pltpu.VMEM)
    i32 = jnp.int32
    departures, adjoint = pl.pallas_call(
        functools.partial(kernel, n_space, 512 * n_space, 3 if n_space > 4 else 2),
        out_shape=(
            pltpu.VMEM((512, 128), F32),
            pltpu.VMEM((levels, 1, 512), F32),
        ),
        in_specs=[anywhere] * 5 + [pl.BlockSpec(memory_space=pltpu.SMEM)] + [anywhere] * 3,
        out_specs=(vmem, vmem),
        scratch_shapes=[
            pltpu.VMEM((levels, 512), BF16),
            pltpu.VMEM((1, 512), i32),
            pltpu.VMEM((8, 512), BF16),
            pltpu.VMEM((1, 512), i32),
            pltpu.VMEM((1, 512), F32),
            pltpu.VMEM((512, 128), F32),
            pltpu.VMEM((levels, 128), BF16),
            pltpu.VMEM((1, 128), F32),
            pltpu.VMEM((4, 1, 512), F32),
            pltpu.VMEM((3, 4, 1, 512), F32),
            pltpu.VMEM((3, 8, 512), BF16),
            pltpu.VMEM((2, 128, 256), BF16),
            pltpu.VMEM((4, 1024, 512), BF16),
            pltpu.VMEM((4, 2, 128, 256), BF16),
            pltpu.VMEM((4, 256, 512), F32),
            pltpu.VMEM((4, 2, 512), F32),
            pltpu.VMEM((12, 128, 128), BF16),
            pltpu.VMEM((4, 128, 128), BF16),
            pltpu.VMEM((2, 4, 128, 128), BF16),
            pltpu.VMEM((4, 4, 128, 128), BF16),
            pltpu.VMEM((4, 256, 256), F32),
            pltpu.VMEM((4, 2, 128, 256), BF16),
            pltpu.VMEM((2, 128, 256), BF16),
            pltpu.VMEM((2, 3, 64, 256), BF16),
            pltpu.VMEM((2, 64, 256), BF16),
            pltpu.VMEM((128, 512), F32),
            pltpu.VMEM((128, 128), F32),
            pltpu.VMEM((128, 512), F32),
            pltpu.SemaphoreType.DMA((8,)),
            pltpu.SemaphoreType.DMA((3,)),
            pltpu.SemaphoreType.DMA((ARRIVALS,)),
            pltpu.SemaphoreType.REGULAR,
        ],
        compiler_params=pltpu.CompilerParams(collective_id=0, has_side_effects=True),
        name="window",
    )(
        jnp.transpose(state[0]),
        obs_start[None],
        jnp.transpose(foot_weight),
        obs_slot[None],
        obs_frac[None],
        live_count,
        obs_values,
        jacobian,
        inv_var[None],
    )
    departures, adjoint = pl.pallas_call(
        write,
        out_shape=(jax.ShapeDtypeStruct(departures.shape, F32), jax.ShapeDtypeStruct(adjoint.shape, F32)),
        in_specs=[vmem] * 2,
        out_specs=(anywhere, anywhere),
        scratch_shapes=[pltpu.SemaphoreType.DMA((2,))],
        name="write",
    )(pltpu.with_memory_space_constraint(departures, pltpu.VMEM), pltpu.with_memory_space_constraint(adjoint, pltpu.VMEM))
    return departures, jnp.transpose(adjoint, (1, 2, 0))


def solution(mesh):
    return jax.shard_map(
        body,
        mesh=mesh,
        in_specs=(
            P("tm", "space", None),
            P(("tm", "space")),
            P(("tm", "space"), None),
            P(("tm", "space")),
            P(("tm", "space")),
            P("tm", "space"),
            P(("tm", "space"), None),
            P(),
            P(),
        ),
        out_specs=(P(("tm", "space"), None), P("tm", "space", None)),
        check_vma=False,
    )
```

```python
import functools

import jax
import jax.numpy as jnp
from jax import lax
from jax.experimental import pallas as pl
from jax.experimental.pallas import tpu as pltpu
from jax.sharding import PartitionSpec as P

MESH = pl.DeviceIdType.MESH
F32 = jnp.float32
BF16 = jnp.bfloat16

META, Z_MATE, Z_RELAYED, Z_REST, FAR, SUM, FIRST, SECOND, LAST, SWAP, RIMS, W_MATE, HELD = 0, 3, 4, 6, 7, 11, 15, 19, 20, 22, 24, 26, 27
ARRIVALS = 29

LEFT, RIGHT, HEAD, TAIL = 0, 1, 2, 3


def nt(a, b):
    return lax.dot_general(a, b, (((1,), (1,)), ((), ())), preferred_element_type=F32)


def kernel(
    n_space, total_cols, holder,
    state_in, start_in, w_in, slot_in, frac_in, count_ref, obs_in, jac_in, inv_in,
    dep_out, adj_out,
    state_ref, start_ref, w_ref, slot_ref, frac_ref, obs_ref, jac_ref, inv_ref,
    o_pack, m_pack, m_w, held, foot, zbuf, acc, abuf, pout, relay, rin, sbuf, wide, wout, win, rim, swap, obs_t, inv_t, dep_t,
    load, send, recv, gate,
):
    t = lax.axis_index("tm")
    s = lax.axis_index("space")
    mate = t + 1 - 2 * lax.rem(t, 2)
    y1 = lax.rem(mate + 2, 8)
    y2 = lax.rem(t + 4, 8)
    y3 = lax.rem(mate + 6, 8)
    left = lax.rem(s + n_space - 1, n_space)
    right = lax.rem(s + 1, n_space)
    chans = 128
    quarter = 128
    top, bottom = pl.ds(0, 64), pl.ds(64, 64)

    core = lax.rem(t, 2)
    first_core, second_core = t - core, t - core + 1
    is_zero, is_last, is_holder = s == 0, s == n_space - 1, s == holder
    is_keeper = jnp.logical_and(is_holder, core == 1)

    barrier = pltpu.get_barrier_semaphore()

    def greet(core_index, tile):
        pl.semaphore_signal(barrier, inc=1, device_id=(core_index, tile), device_id_type=MESH)

    for peer in (t, mate):
        goes_on = jnp.where(is_last, 1, 0)
        to_holder = jnp.where(right == holder, 1, 0)
        normal = peer - to_holder * lax.rem(peer, 2)
        greet(goes_on * second_core + (1 - goes_on) * normal, goes_on * holder + (1 - goes_on) * right)
    for peer in (t, mate):
        greet(peer - jnp.where(left == holder, 1, 0) * lax.rem(peer, 2), left)
    for peer in (y2, y1, y3):
        greet(peer - jnp.where(is_holder, 1, 0) * lax.rem(peer, 2), s)
    greet(mate, s)

    @pl.when(is_zero)
    def _():
        greet(second_core, holder)

    @pl.when(is_holder)
    def _():
        greet(t, 0)
        greet(mate, 0)

    loads = [
        pltpu.make_async_copy(src, dst, load.at[k])
        for k, (src, dst) in enumerate(
            (
                (state_in, state_ref), (jac_in, jac_ref), (start_in, start_ref), (w_in, w_ref), (slot_in, slot_ref),
                (frac_in, frac_ref), (obs_in, obs_ref), (inv_in, inv_ref),
            )
        )
    ]
    for c in loads:
        c.start()

    def copy(index, src, dst, device, out=0):
        return pltpu.make_async_remote_copy(
            src_ref=src, dst_ref=dst, send_sem=send.at[out], recv_sem=recv.at[index],
            device_id=device, device_id_type=MESH,
        )

    def arrived(index, ref):
        copy(index, ref, ref, (mate, s)).wait_recv()

    loads[0].wait()
    loads[1].wait()
    z = lax.dot_general(jac_ref[...], state_ref[...], (((0,), (0,)), ((), ())), preferred_element_type=F32).astype(BF16)
    zbuf[HEAD, 0] = z[:, :256]
    zbuf[TAIL, 0] = z[:, 256:]
    for c in loads[2:6]:
        c.wait()
    o_pack[0] = start_ref[...].astype(F32)
    o_pack[1] = slot_ref[...].astype(F32)
    o_pack[2] = frac_ref[...]
    o_pack[3] = jnp.zeros((1, 512), F32)

    @pl.when(jnp.logical_not(is_keeper))
    def _():
        pl.semaphore_wait(barrier, 8 + 7 * jnp.where(is_holder, 1, 0))

    @pl.when(jnp.logical_and(is_holder, core == 0))
    def _():
        pl.semaphore_signal(gate, inc=1, device_id=(mate, s), device_id_type=MESH)

    @pl.when(is_keeper)
    def _():
        pl.semaphore_wait(gate, 1)

    sides = ((HEAD, RIGHT, left), (TAIL, LEFT, right))
    z_relayed = [copy(Z_RELAYED + k, zbuf.at[a, 0, top], zbuf.at[b, 0, top], (t, d), 1 - k) for k, (a, b, d) in enumerate(sides)]
    z_direct = [copy(Z_REST, zbuf.at[a, 0, bottom], zbuf.at[b, 0, bottom], (t, d), 1 - k) for k, (a, b, d) in enumerate(sides)]
    z_cross = [copy(Z_REST, zbuf.at[a, 0, bottom], zbuf.at[b, 1, bottom], (mate, d), 1 - k) for k, (a, b, d) in enumerate(sides)]
    z_onward = [copy(Z_REST, zbuf.at[b, 0, top], zbuf.at[b, 1, top], (mate, s)) for a, b, d in sides]
    z_mate = [copy(Z_MATE, zbuf.at[a, 0], zbuf.at[a, 1], (mate, s)) for a, b, d in sides]
    z_held = [
        [copy(HELD + j, zbuf.at[HEAD, 0, rows], held.at[1 - k, rows], (second_core, holder), 1) for j, rows in ((0, top), (1, bottom))]
        for k in range(2)
    ]
    last = n_space - 1
    z_passed = [
        copy(Z_RELAYED, held.at[1, top], zbuf.at[RIGHT, 0, top], (mate, last), 2),
        copy(Z_RELAYED, held.at[0, top], zbuf.at[RIGHT, 0, top], (t, last), 2),
        copy(Z_REST, held.at[1, bottom], zbuf.at[RIGHT, 0, bottom], (mate, last), 2),
        copy(Z_REST, held.at[0, bottom], zbuf.at[RIGHT, 1, bottom], (mate, last), 2),
        copy(Z_REST, held.at[0, bottom], zbuf.at[RIGHT, 0, bottom], (t, last), 2),
        copy(Z_REST, held.at[1, bottom], zbuf.at[RIGHT, 1, bottom], (t, last), 2),
    ]
    fields = ((o_pack, m_pack), (w_ref, m_w))
    meta = {}
    for hop, peer in ((2, y2), (1, y1), (3, y3)):
        at = 3 - hop
        meta[at] = [copy(META + at, src, dst.at[at], (peer, s)) for src, dst in fields]
    for k in range(2):

        @pl.when(jnp.logical_and(is_zero, core == k))
        def _():
            for c in z_held[k]:
                c.start()

    gives_way = s == holder + 1

    @pl.when(jnp.logical_not(jnp.logical_or(is_zero, gives_way)))
    def _():
        for c in (z_relayed[0], z_direct[0], z_cross[0]):
            c.start()

    for c in [z_relayed[1], z_direct[1], z_cross[1]] + meta[1] + meta[2] + meta[0] + z_mate:
        c.start()

    def weight_of(slot, frac, held):
        return jnp.where(slot == held, 1.0 - frac, 0.0) + jnp.where(slot + 1 == held, frac, 0.0)

    def build(group, start, w, slot, frac):
        abuf[group, 0:1, :] = weight_of(slot, frac, t)
        abuf[group, 1:2, :] = weight_of(slot, frac, mate)
        local = jnp.bitwise_and(start - s * 512 + 256, total_cols - 1)
        row = lax.broadcasted_iota(jnp.int32, (8, 512), 0)
        ahead = jnp.bitwise_and(row - local, 7)
        weights = w.astype(F32)
        turned = jnp.zeros((8, 512), F32)
        for k in range(8):
            turned = turned + jnp.where(ahead == k, weights[k : k + 1, :], 0.0)
        block = lax.shift_right_arithmetic(local - row + 7, 3)

        for first, last, shift in ((0, 4, 0), (4, 8, 8), (8, 16, -4)):

            def rows(index, carry):
                parts = [jnp.where(block == (index + shift) * 8 + m, turned, 0.0) for m in range(8)]
                at = pl.ds(pl.multiple_of(index * 64, 64), 64)
                foot[group, at, :] = jnp.concatenate(parts, axis=0).astype(BF16)
                return carry

            lax.fori_loop(first, last, rows, 0)

    def columns(first):
        return jnp.concatenate(
            [
                jnp.concatenate([zbuf[first, 0], zbuf[first + 1, 0]], axis=1),
                jnp.concatenate([zbuf[first, 1], zbuf[first + 1, 1]], axis=1),
            ],
            axis=0,
        )

    def centre(group):
        acc[group] = jnp.dot(columns(HEAD), foot[group, 512:1024, :], preferred_element_type=F32)

    def gathered(group):
        at = group - 1
        arrived(META + at, foot.at[group, 0:16])
        build(group, m_pack[at, 0].astype(jnp.int32), m_w[at], m_pack[at, 1].astype(jnp.int32), m_pack[at, 2])

    build(0, start_ref[...], w_ref[...], slot_ref[...], frac_ref[...])
    for c in loads[6:]:
        c.wait()
    obs_t[...] = jnp.transpose(obs_ref[...])
    inv_t[...] = jnp.transpose(jnp.broadcast_to(inv_ref[...], (chans, chans)))
    arrived(Z_MATE, zbuf.at[HEAD : HEAD + 2, 1])

    @pl.when(gives_way)
    def _():
        for c in (z_relayed[0], z_direct[0], z_cross[0]):
            c.start()

    @pl.when(is_keeper)
    def _():
        pl.semaphore_wait(barrier, 7)
        arrived(HELD, held.at[:, top])
        for c in z_passed[:2]:
            c.start()
        arrived(HELD + 1, held.at[:, bottom])
        for c in z_passed[2:]:
            c.start()
        for device in ((t, 0), (mate, 0)):
            pl.semaphore_signal(gate, inc=1, device_id=device, device_id_type=MESH)

    z_relayed[1].wait_recv()
    z_onward[1].start()
    z_relayed[0].wait_recv()
    z_onward[0].start()
    for group in (3,):
        gathered(group)
    for group in (2,):
        gathered(group)
        centre(group)
    gathered(1)
    arrived(Z_REST, zbuf.at[0:3, 0])

    def weighted(group, total):
        return abuf[group, 0:1, :] * total[:chans] + abuf[group, 1:2, :] * total[chans:]

    def partials(group):
        whole = jnp.concatenate([columns(LEFT), columns(HEAD)], axis=1)
        return weighted(group, jnp.dot(whole, foot[group], preferred_element_type=F32))

    def lanes(q):
        return slice(q * quarter, (q + 1) * quarter)

    far = [copy(FAR + q, pout.at[q], relay.at[q], ((y1, y3)[q % 2], s)) for q in range(4)]
    to_next = [copy(SUM + q, pout.at[4 + q], rin.at[0, q], (y1, s)) for q in range(4)]
    to_last = [copy(SUM + q, pout.at[8 + q], rin.at[1, q], (y3, s)) for q in range(4)]
    partial = weighted(2, acc[2] + jnp.dot(columns(LEFT), foot[2, 0:512, :], preferred_element_type=F32))
    for q in range(4):
        pout[q] = partial[:, lanes(q)].astype(BF16)
        far[q].start()
    for group, base, copies, now in ((1, 4, to_next, 1), (3, 8, to_last, 0)):
        partial = partials(group)
        for q in (now, now + 2):
            pout[base + q] = partial[:, lanes(q)].astype(BF16)
            copies[q].start()
        for q in (1 - now, 3 - now):
            acc[group, 0:chans, lanes(q)] = partial[:, lanes(q)]
    acc[0, 0:chans] = partials(0)
    for q in range(4):
        group, base, copies = ((1, 4, to_next), (3, 8, to_last))[q % 2]
        far[q].wait_recv()
        pout[base + q] = (acc[group, 0:chans, lanes(q)] + relay[q].astype(F32)).astype(BF16)
        copies[q].start()

    ag_next = [copy(FIRST + q if q % 2 == 0 else SECOND, sbuf.at[0, q], sbuf.at[3, q], (y1, s)) for q in range(4)]
    ag_last = [copy(FIRST + q if q % 2 else SECOND, sbuf.at[0, q], sbuf.at[1, q], (y3, s)) for q in range(4)]
    ag_far = [
        copy(LAST + q // 2, sbuf.at[(3, 1)[q % 2], q], sbuf.at[2, q], ((y1, y3)[q % 2], s)) for q in range(4)
    ]
    column = lax.broadcasted_iota(jnp.int32, (1, quarter), 1)
    for q in range(4):
        arrived(SUM + q, rin.at[:, q])
        projected = acc[0, 0:chans, lanes(q)] + rin[0, q].astype(F32) + rin[1, q].astype(F32)
        live = column + q * quarter < count_ref[0, 0]
        departed = jnp.where(live, obs_t[:, lanes(q)] - projected, 0.0)
        dep_t[:, lanes(q)] = departed
        sbuf[0, q] = (departed * inv_t[:, 0:1]).astype(BF16)
        (ag_next, ag_last)[q % 2][q].start()
    for q in (0, 2):
        ag_next[q + 1].start()
        ag_last[q].start()

    dep_out[...] = jnp.transpose(dep_t[...])

    def lanes_of(ref, group, rows, quarters):
        if quarters[-1] - quarters[0] == len(quarters) - 1:
            return ref[group, rows, quarters[0] * quarter : (quarters[-1] + 1) * quarter]
        return jnp.concatenate([ref[group, rows, lanes(q)] for q in quarters], axis=1)

    def by_slot(pieces):
        parts = []
        for slot in range(2):
            row = []
            for group, quarters in pieces:
                values = jnp.concatenate([sbuf[group, q] for q in quarters], axis=1).astype(F32)
                row.append((lanes_of(abuf, group, slice(slot, slot + 1), quarters) * values).astype(BF16))
            parts.append(jnp.concatenate(row, axis=1))
        return jnp.concatenate(parts, axis=0)

    def sums(v, pieces, chunk):
        rows = slice(chunk * 256, (chunk + 1) * 256)
        return nt(v, jnp.concatenate([lanes_of(foot, group, rows, quarters) for group, quarters in pieces], axis=1))

    def spread(*pieces, fresh=False):
        v = by_slot(pieces)
        for chunk in range(4):
            if fresh:
                wide[chunk] = sums(v, pieces, chunk)
            else:
                wide[chunk] += sums(v, pieces, chunk)

    spread((0, (0, 1, 2, 3)), fresh=True)
    for q in range(4):
        (ag_next, ag_last)[q % 2][q].wait_recv()
        ag_far[q].start()
    spread((3, (0, 2)), (1, (1, 3)))
    arrived(SECOND, sbuf.at[3])
    spread((3, (1, 3)), (1, (0, 2)))
    arrived(LAST, sbuf.at[2, 0:2])
    spread((2, (0, 1)))
    arrived(LAST + 1, sbuf.at[2, 2:4])
    ends = ((LEFT, left), (RIGHT, right))
    r_own = [copy(RIMS + k, wout.at[k, 0, top], rim.at[1 - k, 0], (t, d)) for k, d in ends]
    r_other = [copy(RIMS + k, wout.at[k, 1, top], rim.at[1 - k, 1], (mate, d)) for k, d in ends]
    r_swap = [copy(SWAP + k, wout.at[k, 0, bottom], swap.at[k], (mate, s)) for k, d in ends]
    r_sum = [copy(RIMS + k, wout.at[k, 1, bottom], rim.at[1 - k, 2], (mate, d)) for k, d in ends]
    r_mate = [copy(W_MATE, wout.at[2 + k, 1], win.at[k], (mate, s)) for k in range(2)]
    @pl.when(is_zero)
    def _():
        pl.semaphore_wait(gate, 1)

    final = ((2, (2, 3)),)
    v = by_slot(final)
    for k in (RIGHT, LEFT):
        total = wide[k] + sums(v, final, k)
        wide[k] = total
        wout[k, 0] = total[:chans].astype(BF16)
        wout[k, 1, 0:64] = total[chans : chans + 64].astype(BF16)
        r_swap[k].start()

        @pl.when(core == 0)
        def _():
            r_other[k].start()

        @pl.when(core == 1)
        def _():
            r_own[k].start()

    for k in (RIGHT, LEFT):
        r_swap[k].wait_recv()
        wout[k, 1, 64:128] = (wide[k, chans + 64 : 2 * chans] + swap[k].astype(F32)).astype(BF16)
        r_sum[k].start()

    @pl.when(core == 0)
    def _():
        for k in (RIGHT, LEFT):
            r_own[k].start()

    @pl.when(core == 1)
    def _():
        for k in (RIGHT, LEFT):
            r_other[k].start()

    for k in range(2):
        total = wide[HEAD + k] + sums(v, final, HEAD + k)
        wide[HEAD + k] = total
        wout[2 + k, 1] = total[chans:].astype(BF16)
        r_mate[k].start()
    arrived(W_MATE, win)
    for h in (1, 0):
        arrived(RIMS + 1 - h, rim.at[h])
        rims = jnp.concatenate([rim[h, 0].astype(F32) + rim[h, 1].astype(F32), rim[h, 2].astype(F32)], axis=0)
        whole = wide[HEAD + h, 0:chans] + win[h].astype(F32) + rims
        adj_out[:, 0, h * 256 : (h + 1) * 256] = jnp.dot(jac_ref[...], whole.astype(BF16), preferred_element_type=F32)
    def left_here(ref, out):
        copy(META, ref, ref, (mate, s), out).wait_send()

    left_here(foot.at[0:3, 0:496], 0)

    @pl.when(is_zero)
    def _():
        left_here(held.at[0], 1)

    @pl.when(jnp.logical_not(is_zero))
    def _():
        left_here(foot.at[0:3, 0:32], 1)

    @pl.when(is_keeper)
    def _():
        left_here(foot.at[0:3, 0:64], 2)


def write(dep_in, adj_in, dep_out, adj_out, done):
    copies = [pltpu.make_async_copy(dep_in, dep_out, done.at[0]), pltpu.make_async_copy(adj_in, adj_out, done.at[1])]
    for c in copies:
        c.start()
    for c in copies:
        c.wait()


def body(state, obs_start, foot_weight, obs_slot, obs_frac, live_count, obs_values, jacobian, inv_var):
    n_space = lax.axis_size("space")
    levels = jacobian.shape[0]
    anywhere = pl.BlockSpec(memory_space=pl.ANY)
    vmem = pl.BlockSpec(memory_space=pltpu.VMEM)
    i32 = jnp.int32
    departures, adjoint = pl.pallas_call(
        functools.partial(kernel, n_space, 512 * n_space, 3 if n_space > 4 else 2),
        out_shape=(
            pltpu.VMEM((512, 128), F32),
            pltpu.VMEM((levels, 1, 512), F32),
        ),
        in_specs=[anywhere] * 5 + [pl.BlockSpec(memory_space=pltpu.SMEM)] + [anywhere] * 3,
        out_specs=(vmem, vmem),
        scratch_shapes=[
            pltpu.VMEM((levels, 512), BF16),
            pltpu.VMEM((1, 512), i32),
            pltpu.VMEM((8, 512), BF16),
            pltpu.VMEM((1, 512), i32),
            pltpu.VMEM((1, 512), F32),
            pltpu.VMEM((512, 128), F32),
            pltpu.VMEM((levels, 128), BF16),
            pltpu.VMEM((1, 128), F32),
            pltpu.VMEM((4, 1, 512), F32),
            pltpu.VMEM((3, 4, 1, 512), F32),
            pltpu.VMEM((3, 8, 512), BF16),
            pltpu.VMEM((2, 128, 256), BF16),
            pltpu.VMEM((4, 1024, 512), BF16),
            pltpu.VMEM((4, 2, 128, 256), BF16),
            pltpu.VMEM((4, 256, 512), F32),
            pltpu.VMEM((4, 2, 512), F32),
            pltpu.VMEM((12, 128, 128), BF16),
            pltpu.VMEM((4, 128, 128), BF16),
            pltpu.VMEM((2, 4, 128, 128), BF16),
            pltpu.VMEM((4, 4, 128, 128), BF16),
            pltpu.VMEM((4, 256, 256), F32),
            pltpu.VMEM((4, 2, 128, 256), BF16),
            pltpu.VMEM((2, 128, 256), BF16),
            pltpu.VMEM((2, 3, 64, 256), BF16),
            pltpu.VMEM((2, 64, 256), BF16),
            pltpu.VMEM((128, 512), F32),
            pltpu.VMEM((128, 128), F32),
            pltpu.VMEM((128, 512), F32),
            pltpu.SemaphoreType.DMA((8,)),
            pltpu.SemaphoreType.DMA((3,)),
            pltpu.SemaphoreType.DMA((ARRIVALS,)),
            pltpu.SemaphoreType.REGULAR,
        ],
        compiler_params=pltpu.CompilerParams(collective_id=0, has_side_effects=True),
        name="window",
    )(
        jnp.transpose(state[0]),
        obs_start[None],
        jnp.transpose(foot_weight),
        obs_slot[None],
        obs_frac[None],
        live_count,
        obs_values,
        jacobian,
        inv_var[None],
    )
    departures, adjoint = pl.pallas_call(
        write,
        out_shape=(jax.ShapeDtypeStruct(departures.shape, F32), jax.ShapeDtypeStruct(adjoint.shape, F32)),
        in_specs=[vmem] * 2,
        out_specs=(anywhere, anywhere),
        scratch_shapes=[pltpu.SemaphoreType.DMA((2,))],
        name="write",
    )(pltpu.with_memory_space_constraint(departures, pltpu.VMEM), pltpu.with_memory_space_constraint(adjoint, pltpu.VMEM))
    return departures, jnp.transpose(adjoint, (1, 2, 0))


def solution(mesh):
    return jax.shard_map(
        body,
        mesh=mesh,
        in_specs=(
            P("tm", "space", None),
            P(("tm", "space")),
            P(("tm", "space"), None),
            P(("tm", "space")),
            P(("tm", "space")),
            P("tm", "space"),
            P(("tm", "space"), None),
            P(),
            P(),
        ),
        out_specs=(P(("tm", "space"), None), P("tm", "space", None)),
        check_vma=False,
    )
```

```python
import functools

import jax
import jax.numpy as jnp
from jax import lax
from jax.experimental import pallas as pl
from jax.experimental.pallas import tpu as pltpu
from jax.sharding import PartitionSpec as P

MESH = pl.DeviceIdType.MESH
F32 = jnp.float32
BF16 = jnp.bfloat16

META, Z_MATE, Z_RELAYED, Z_REST, FAR, SUM, FIRST, SECOND, LAST, SWAP, RIMS, W_MATE, HELD = 0, 3, 4, 6, 7, 11, 15, 19, 20, 22, 24, 26, 27
ARRIVALS = 29

LEFT, RIGHT, HEAD, TAIL = 0, 1, 2, 3


def nt(a, b):
    return lax.dot_general(a, b, (((1,), (1,)), ((), ())), preferred_element_type=F32)


def kernel(
    n_space, total_cols, holder,
    state_in, start_in, w_in, slot_in, frac_in, count_ref, obs_in, jac_in, inv_in,
    dep_out, adj_out,
    state_ref, start_ref, w_ref, slot_ref, frac_ref, obs_ref, jac_ref, inv_ref,
    o_pack, m_pack, m_w, held, foot, zbuf, acc, abuf, pout, relay, rin, sbuf, wide, wout, win, rim, swap, obs_t, inv_t, dep_t,
    load, send, recv, gate,
):
    t = lax.axis_index("tm")
    s = lax.axis_index("space")
    mate = t + 1 - 2 * lax.rem(t, 2)
    y1 = lax.rem(mate + 2, 8)
    y2 = lax.rem(t + 4, 8)
    y3 = lax.rem(mate + 6, 8)
    left = lax.rem(s + n_space - 1, n_space)
    right = lax.rem(s + 1, n_space)
    chans = 128
    quarter = 128
    top, bottom = pl.ds(0, 64), pl.ds(64, 64)

    core = lax.rem(t, 2)
    first_core, second_core = t - core, t - core + 1
    is_zero, is_last, is_holder = s == 0, s == n_space - 1, s == holder
    is_keeper = jnp.logical_and(is_holder, core == 1)

    barrier = pltpu.get_barrier_semaphore()

    def greet(core_index, tile):
        pl.semaphore_signal(barrier, inc=1, device_id=(core_index, tile), device_id_type=MESH)

    for peer in (t, mate):
        goes_on = jnp.where(is_last, 1, 0)
        to_holder = jnp.where(right == holder, 1, 0)
        normal = peer - to_holder * lax.rem(peer, 2)
        greet(goes_on * second_core + (1 - goes_on) * normal, goes_on * holder + (1 - goes_on) * right)
    for peer in (t, mate):
        greet(peer - jnp.where(left == holder, 1, 0) * lax.rem(peer, 2), left)
    for peer in (y2, y1, y3):
        greet(peer - jnp.where(is_holder, 1, 0) * lax.rem(peer, 2), s)
    greet(mate, s)

    @pl.when(is_zero)
    def _():
        greet(second_core, holder)

    @pl.when(is_holder)
    def _():
        greet(t, 0)
        greet(mate, 0)

    loads = [
        pltpu.make_async_copy(src, dst, load.at[k])
        for k, (src, dst) in enumerate(
            (
                (state_in, state_ref), (jac_in, jac_ref), (start_in, start_ref), (w_in, w_ref), (slot_in, slot_ref),
                (frac_in, frac_ref), (obs_in, obs_ref), (inv_in, inv_ref),
            )
        )
    ]
    for c in loads:
        c.start()

    def copy(index, src, dst, device, out=0):
        return pltpu.make_async_remote_copy(
            src_ref=src, dst_ref=dst, send_sem=send.at[out], recv_sem=recv.at[index],
            device_id=device, device_id_type=MESH,
        )

    def arrived(index, ref):
        copy(index, ref, ref, (mate, s)).wait_recv()

    loads[0].wait()
    loads[1].wait()
    z = lax.dot_general(jac_ref[...], state_ref[...], (((0,), (0,)), ((), ())), preferred_element_type=F32).astype(BF16)
    zbuf[HEAD, 0] = z[:, :256]
    zbuf[TAIL, 0] = z[:, 256:]
    for c in loads[2:6]:
        c.wait()
    o_pack[0] = start_ref[...].astype(F32)
    o_pack[1] = slot_ref[...].astype(F32)
    o_pack[2] = frac_ref[...]
    o_pack[3] = jnp.zeros((1, 512), F32)

    @pl.when(jnp.logical_not(is_keeper))
    def _():
        pl.semaphore_wait(barrier, 8 + 7 * jnp.where(is_holder, 1, 0))

    @pl.when(jnp.logical_and(is_holder, core == 0))
    def _():
        pl.semaphore_signal(gate, inc=1, device_id=(mate, s), device_id_type=MESH)

    @pl.when(is_keeper)
    def _():
        pl.semaphore_wait(gate, 1)

    sides = ((HEAD, RIGHT, left), (TAIL, LEFT, right))
    z_relayed = [copy(Z_RELAYED + k, zbuf.at[a, 0, top], zbuf.at[b, 0, top], (t, d), 1 - k) for k, (a, b, d) in enumerate(sides)]
    z_direct = [copy(Z_REST, zbuf.at[a, 0, bottom], zbuf.at[b, 0, bottom], (t, d), 1 - k) for k, (a, b, d) in enumerate(sides)]
    z_cross = [copy(Z_REST, zbuf.at[a, 0, bottom], zbuf.at[b, 1, bottom], (mate, d), 1 - k) for k, (a, b, d) in enumerate(sides)]
    z_onward = [copy(Z_REST, zbuf.at[b, 0, top], zbuf.at[b, 1, top], (mate, s)) for a, b, d in sides]
    z_mate = [copy(Z_MATE, zbuf.at[a, 0], zbuf.at[a, 1], (mate, s)) for a, b, d in sides]
    z_held = [
        [copy(HELD + j, zbuf.at[HEAD, 0, rows], held.at[1 - k, rows], (second_core, holder), 1) for j, rows in ((0, top), (1, bottom))]
        for k in range(2)
    ]
    last = n_space - 1
    z_passed = [
        copy(Z_RELAYED, held.at[1, top], zbuf.at[RIGHT, 0, top], (mate, last), 2),
        copy(Z_RELAYED, held.at[0, top], zbuf.at[RIGHT, 0, top], (t, last), 2),
        copy(Z_REST, held.at[1, bottom], zbuf.at[RIGHT, 0, bottom], (mate, last), 2),
        copy(Z_REST, held.at[0, bottom], zbuf.at[RIGHT, 1, bottom], (mate, last), 2),
        copy(Z_REST, held.at[0, bottom], zbuf.at[RIGHT, 0, bottom], (t, last), 2),
        copy(Z_REST, held.at[1, bottom], zbuf.at[RIGHT, 1, bottom], (t, last), 2),
    ]
    fields = ((o_pack, m_pack), (w_ref, m_w))
    meta = {}
    for hop, peer in ((2, y2), (1, y1), (3, y3)):
        at = 3 - hop
        meta[at] = [copy(META + at, src, dst.at[at], (peer, s)) for src, dst in fields]
    for c in meta[1]:
        c.start()

    for k in range(2):

        @pl.when(jnp.logical_and(is_zero, core == k))
        def _():
            for c in z_held[k]:
                c.start()

    gives_way = s == holder + 1

    @pl.when(jnp.logical_not(jnp.logical_or(is_zero, gives_way)))
    def _():
        for c in (z_relayed[0], z_direct[0], z_cross[0]):
            c.start()

    for c in [z_relayed[1], z_direct[1], z_cross[1]] + meta[2] + meta[0] + z_mate:
        c.start()

    def weight_of(slot, frac, held):
        return jnp.where(slot == held, 1.0 - frac, 0.0) + jnp.where(slot + 1 == held, frac, 0.0)

    def build(group, start, w, slot, frac):
        abuf[group, 0:1, :] = weight_of(slot, frac, t)
        abuf[group, 1:2, :] = weight_of(slot, frac, mate)
        local = jnp.bitwise_and(start - s * 512 + 256, total_cols - 1)
        row = lax.broadcasted_iota(jnp.int32, (8, 512), 0)
        ahead = jnp.bitwise_and(row - local, 7)
        weights = w.astype(F32)
        turned = jnp.zeros((8, 512), F32)
        for k in range(8):
            turned = turned + jnp.where(ahead == k, weights[k : k + 1, :], 0.0)
        block = lax.shift_right_arithmetic(local - row + 7, 3)

        for first, last, shift in ((0, 4, 0), (4, 8, 8), (8, 16, -4)):

            def rows(index, carry):
                parts = [jnp.where(block == (index + shift) * 8 + m, turned, 0.0) for m in range(8)]
                at = pl.ds(pl.multiple_of(index * 64, 64), 64)
                foot[group, at, :] = jnp.concatenate(parts, axis=0).astype(BF16)
                return carry

            lax.fori_loop(first, last, rows, 0)

    def columns(first):
        return jnp.concatenate(
            [
                jnp.concatenate([zbuf[first, 0], zbuf[first + 1, 0]], axis=1),
                jnp.concatenate([zbuf[first, 1], zbuf[first + 1, 1]], axis=1),
            ],
            axis=0,
        )

    def centre(group):
        acc[group] = jnp.dot(columns(HEAD), foot[group, 512:1024, :], preferred_element_type=F32)

    def gathered(group):
        at = group - 1
        arrived(META + at, foot.at[group, 0:16])
        build(group, m_pack[at, 0].astype(jnp.int32), m_w[at], m_pack[at, 1].astype(jnp.int32), m_pack[at, 2])

    build(0, start_ref[...], w_ref[...], slot_ref[...], frac_ref[...])
    for c in loads[6:]:
        c.wait()
    obs_t[...] = jnp.transpose(obs_ref[...])
    inv_t[...] = jnp.transpose(jnp.broadcast_to(inv_ref[...], (chans, chans)))
    arrived(Z_MATE, zbuf.at[HEAD : HEAD + 2, 1])

    @pl.when(gives_way)
    def _():
        for c in (z_relayed[0], z_direct[0], z_cross[0]):
            c.start()

    @pl.when(is_keeper)
    def _():
        pl.semaphore_wait(barrier, 7)
        arrived(HELD, held.at[:, top])
        for c in z_passed[:2]:
            c.start()
        arrived(HELD + 1, held.at[:, bottom])
        for c in z_passed[2:]:
            c.start()
        for device in ((t, 0), (mate, 0)):
            pl.semaphore_signal(gate, inc=1, device_id=device, device_id_type=MESH)

    z_relayed[1].wait_recv()
    z_onward[1].start()
    z_relayed[0].wait_recv()
    z_onward[0].start()
    for group in (3,):
        gathered(group)
    for group in (2,):
        gathered(group)
        centre(group)
    gathered(1)
    arrived(Z_REST, zbuf.at[0:3, 0])

    def weighted(group, total):
        return abuf[group, 0:1, :] * total[:chans] + abuf[group, 1:2, :] * total[chans:]

    def partials(group):
        whole = jnp.concatenate([columns(LEFT), columns(HEAD)], axis=1)
        return weighted(group, jnp.dot(whole, foot[group], preferred_element_type=F32))

    def lanes(q):
        return slice(q * quarter, (q + 1) * quarter)

    far = [copy(FAR + q, pout.at[q], relay.at[q], ((y1, y3)[q % 2], s)) for q in range(4)]
    to_next = [copy(SUM + q, pout.at[4 + q], rin.at[0, q], (y1, s)) for q in range(4)]
    to_last = [copy(SUM + q, pout.at[8 + q], rin.at[1, q], (y3, s)) for q in range(4)]
    partial = weighted(2, acc[2] + jnp.dot(columns(LEFT), foot[2, 0:512, :], preferred_element_type=F32))
    for q in range(4):
        pout[q] = partial[:, lanes(q)].astype(BF16)
        far[q].start()
    for group, base, copies, now in ((1, 4, to_next, 1), (3, 8, to_last, 0)):
        partial = partials(group)
        for q in (now, now + 2):
            pout[base + q] = partial[:, lanes(q)].astype(BF16)
            copies[q].start()
        for q in (1 - now, 3 - now):
            acc[group, 0:chans, lanes(q)] = partial[:, lanes(q)]
    acc[0, 0:chans] = partials(0)
    for q in range(4):
        group, base, copies = ((1, 4, to_next), (3, 8, to_last))[q % 2]
        far[q].wait_recv()
        pout[base + q] = (acc[group, 0:chans, lanes(q)] + relay[q].astype(F32)).astype(BF16)
        copies[q].start()

    ag_next = [copy(FIRST + q if q % 2 == 0 else SECOND, sbuf.at[0, q], sbuf.at[3, q], (y1, s)) for q in range(4)]
    ag_last = [copy(FIRST + q if q % 2 else SECOND, sbuf.at[0, q], sbuf.at[1, q], (y3, s)) for q in range(4)]
    ag_far = [
        copy(LAST + q // 2, sbuf.at[(3, 1)[q % 2], q], sbuf.at[2, q], ((y1, y3)[q % 2], s)) for q in range(4)
    ]
    column = lax.broadcasted_iota(jnp.int32, (1, quarter), 1)
    for q in range(4):
        arrived(SUM + q, rin.at[:, q])
        projected = acc[0, 0:chans, lanes(q)] + rin[0, q].astype(F32) + rin[1, q].astype(F32)
        live = column + q * quarter < count_ref[0, 0]
        departed = jnp.where(live, obs_t[:, lanes(q)] - projected, 0.0)
        dep_t[:, lanes(q)] = departed
        sbuf[0, q] = (departed * inv_t[:, 0:1]).astype(BF16)
        (ag_next, ag_last)[q % 2][q].start()
    for q in (0, 2):
        ag_next[q + 1].start()
        ag_last[q].start()

    dep_out[...] = jnp.transpose(dep_t[...])

    def lanes_of(ref, group, rows, quarters):
        if quarters[-1] - quarters[0] == len(quarters) - 1:
            return ref[group, rows, quarters[0] * quarter : (quarters[-1] + 1) * quarter]
        return jnp.concatenate([ref[group, rows, lanes(q)] for q in quarters], axis=1)

    def by_slot(pieces):
        parts = []
        for slot in range(2):
            row = []
            for group, quarters in pieces:
                values = jnp.concatenate([sbuf[group, q] for q in quarters], axis=1).astype(F32)
                row.append((lanes_of(abuf, group, slice(slot, slot + 1), quarters) * values).astype(BF16))
            parts.append(jnp.concatenate(row, axis=1))
        return jnp.concatenate(parts, axis=0)

    def sums(v, pieces, chunk):
        rows = slice(chunk * 256, (chunk + 1) * 256)
        return nt(v, jnp.concatenate([lanes_of(foot, group, rows, quarters) for group, quarters in pieces], axis=1))

    def spread(*pieces, fresh=False):
        v = by_slot(pieces)
        for chunk in range(4):
            if fresh:
                wide[chunk] = sums(v, pieces, chunk)
            else:
                wide[chunk] += sums(v, pieces, chunk)

    spread((0, (0, 1, 2, 3)), fresh=True)
    for q in range(4):
        (ag_next, ag_last)[q % 2][q].wait_recv()
        ag_far[q].start()
    spread((3, (0, 2)), (1, (1, 3)))
    arrived(SECOND, sbuf.at[3])
    spread((3, (1, 3)), (1, (0, 2)))
    arrived(LAST, sbuf.at[2, 0:2])
    spread((2, (0, 1)))
    arrived(LAST + 1, sbuf.at[2, 2:4])
    ends = ((LEFT, left), (RIGHT, right))
    r_own = [copy(RIMS + k, wout.at[k, 0, top], rim.at[1 - k, 0], (t, d)) for k, d in ends]
    r_other = [copy(RIMS + k, wout.at[k, 1, top], rim.at[1 - k, 1], (mate, d)) for k, d in ends]
    r_swap = [copy(SWAP + k, wout.at[k, 0, bottom], swap.at[k], (mate, s)) for k, d in ends]
    r_sum = [copy(RIMS + k, wout.at[k, 1, bottom], rim.at[1 - k, 2], (mate, d)) for k, d in ends]
    r_mate = [copy(W_MATE, wout.at[2 + k, 1], win.at[k], (mate, s)) for k in range(2)]
    @pl.when(is_zero)
    def _():
        pl.semaphore_wait(gate, 1)

    final = ((2, (2, 3)),)
    v = by_slot(final)
    for k in (RIGHT, LEFT):
        total = wide[k] + sums(v, final, k)
        wide[k] = total
        wout[k, 0] = total[:chans].astype(BF16)
        wout[k, 1, 0:64] = total[chans : chans + 64].astype(BF16)
        r_swap[k].start()

        @pl.when(core == 0)
        def _():
            r_other[k].start()

        @pl.when(core == 1)
        def _():
            r_own[k].start()

    for k in (RIGHT, LEFT):
        r_swap[k].wait_recv()
        wout[k, 1, 64:128] = (wide[k, chans + 64 : 2 * chans] + swap[k].astype(F32)).astype(BF16)
        r_sum[k].start()

    @pl.when(core == 0)
    def _():
        for k in (RIGHT, LEFT):
            r_own[k].start()

    @pl.when(core == 1)
    def _():
        for k in (RIGHT, LEFT):
            r_other[k].start()

    for k in range(2):
        total = wide[HEAD + k] + sums(v, final, HEAD + k)
        wide[HEAD + k] = total
        wout[2 + k, 1] = total[chans:].astype(BF16)
        r_mate[k].start()
    arrived(W_MATE, win)
    for h in (1, 0):
        arrived(RIMS + 1 - h, rim.at[h])
        rims = jnp.concatenate([rim[h, 0].astype(F32) + rim[h, 1].astype(F32), rim[h, 2].astype(F32)], axis=0)
        whole = wide[HEAD + h, 0:chans] + win[h].astype(F32) + rims
        adj_out[:, 0, h * 256 : (h + 1) * 256] = jnp.dot(jac_ref[...], whole.astype(BF16), preferred_element_type=F32)
    def left_here(ref, out):
        copy(META, ref, ref, (mate, s), out).wait_send()

    left_here(foot.at[0:3, 0:496], 0)

    @pl.when(is_zero)
    def _():
        left_here(held.at[0], 1)

    @pl.when(jnp.logical_not(is_zero))
    def _():
        left_here(foot.at[0:3, 0:32], 1)

    @pl.when(is_keeper)
    def _():
        left_here(foot.at[0:3, 0:64], 2)


def write(dep_in, adj_in, dep_out, adj_out, done):
    copies = [pltpu.make_async_copy(dep_in, dep_out, done.at[0]), pltpu.make_async_copy(adj_in, adj_out, done.at[1])]
    for c in copies:
        c.start()
    for c in copies:
        c.wait()


def body(state, obs_start, foot_weight, obs_slot, obs_frac, live_count, obs_values, jacobian, inv_var):
    n_space = lax.axis_size("space")
    levels = jacobian.shape[0]
    anywhere = pl.BlockSpec(memory_space=pl.ANY)
    vmem = pl.BlockSpec(memory_space=pltpu.VMEM)
    i32 = jnp.int32
    departures, adjoint = pl.pallas_call(
        functools.partial(kernel, n_space, 512 * n_space, 3 if n_space > 4 else 2),
        out_shape=(
            pltpu.VMEM((512, 128), F32),
            pltpu.VMEM((levels, 1, 512), F32),
        ),
        in_specs=[anywhere] * 5 + [pl.BlockSpec(memory_space=pltpu.SMEM)] + [anywhere] * 3,
        out_specs=(vmem, vmem),
        scratch_shapes=[
            pltpu.VMEM((levels, 512), BF16),
            pltpu.VMEM((1, 512), i32),
            pltpu.VMEM((8, 512), BF16),
            pltpu.VMEM((1, 512), i32),
            pltpu.VMEM((1, 512), F32),
            pltpu.VMEM((512, 128), F32),
            pltpu.VMEM((levels, 128), BF16),
            pltpu.VMEM((1, 128), F32),
            pltpu.VMEM((4, 1, 512), F32),
            pltpu.VMEM((3, 4, 1, 512), F32),
            pltpu.VMEM((3, 8, 512), BF16),
            pltpu.VMEM((2, 128, 256), BF16),
            pltpu.VMEM((4, 1024, 512), BF16),
            pltpu.VMEM((4, 2, 128, 256), BF16),
            pltpu.VMEM((4, 256, 512), F32),
            pltpu.VMEM((4, 2, 512), F32),
            pltpu.VMEM((12, 128, 128), BF16),
            pltpu.VMEM((4, 128, 128), BF16),
            pltpu.VMEM((2, 4, 128, 128), BF16),
            pltpu.VMEM((4, 4, 128, 128), BF16),
            pltpu.VMEM((4, 256, 256), F32),
            pltpu.VMEM((4, 2, 128, 256), BF16),
            pltpu.VMEM((2, 128, 256), BF16),
            pltpu.VMEM((2, 3, 64, 256), BF16),
            pltpu.VMEM((2, 64, 256), BF16),
            pltpu.VMEM((128, 512), F32),
            pltpu.VMEM((128, 128), F32),
            pltpu.VMEM((128, 512), F32),
            pltpu.SemaphoreType.DMA((8,)),
            pltpu.SemaphoreType.DMA((3,)),
            pltpu.SemaphoreType.DMA((ARRIVALS,)),
            pltpu.SemaphoreType.REGULAR,
        ],
        compiler_params=pltpu.CompilerParams(collective_id=0, has_side_effects=True),
        name="window",
    )(
        jnp.transpose(state[0]),
        obs_start[None],
        jnp.transpose(foot_weight),
        obs_slot[None],
        obs_frac[None],
        live_count,
        obs_values,
        jacobian,
        inv_var[None],
    )
    departures, adjoint = pl.pallas_call(
        write,
        out_shape=(jax.ShapeDtypeStruct(departures.shape, F32), jax.ShapeDtypeStruct(adjoint.shape, F32)),
        in_specs=[vmem] * 2,
        out_specs=(anywhere, anywhere),
        scratch_shapes=[pltpu.SemaphoreType.DMA((2,))],
        name="write",
    )(pltpu.with_memory_space_constraint(departures, pltpu.VMEM), pltpu.with_memory_space_constraint(adjoint, pltpu.VMEM))
    return departures, jnp.transpose(adjoint, (1, 2, 0))


def solution(mesh):
    return jax.shard_map(
        body,
        mesh=mesh,
        in_specs=(
            P("tm", "space", None),
            P(("tm", "space")),
            P(("tm", "space"), None),
            P(("tm", "space")),
            P(("tm", "space")),
            P("tm", "space"),
            P(("tm", "space"), None),
            P(),
            P(),
        ),
        out_specs=(P(("tm", "space"), None), P("tm", "space", None)),
        check_vma=False,
    )
```

```python
import functools

import jax
import jax.numpy as jnp
from jax import lax
from jax.experimental import pallas as pl
from jax.experimental.pallas import tpu as pltpu
from jax.sharding import PartitionSpec as P

MESH = pl.DeviceIdType.MESH
F32 = jnp.float32
BF16 = jnp.bfloat16

META, Z_MATE, Z_RELAYED, Z_REST, FAR, SUM, FIRST, SECOND, LAST, SWAP, RIMS, W_MATE, HELD = 0, 3, 4, 6, 7, 11, 15, 19, 20, 22, 24, 26, 27
ARRIVALS = 29

LEFT, RIGHT, HEAD, TAIL = 0, 1, 2, 3


def nt(a, b):
    return lax.dot_general(a, b, (((1,), (1,)), ((), ())), preferred_element_type=F32)


def kernel(
    n_space, total_cols, holder,
    state_in, start_in, w_in, slot_in, frac_in, count_ref, obs_in, jac_in, inv_in,
    dep_out, adj_out,
    state_ref, start_ref, w_ref, slot_ref, frac_ref, obs_ref, jac_ref, inv_ref,
    o_pack, m_pack, m_w, held, foot, zbuf, acc, abuf, pout, relay, rin, sbuf, wide, wout, win, rim, swap, obs_t, inv_t, dep_t,
    load, send, recv, gate,
):
    t = lax.axis_index("tm")
    s = lax.axis_index("space")
    mate = t + 1 - 2 * lax.rem(t, 2)
    y1 = lax.rem(mate + 2, 8)
    y2 = lax.rem(t + 4, 8)
    y3 = lax.rem(mate + 6, 8)
    left = lax.rem(s + n_space - 1, n_space)
    right = lax.rem(s + 1, n_space)
    chans = 128
    quarter = 128
    top, bottom = pl.ds(0, 64), pl.ds(64, 64)

    core = lax.rem(t, 2)
    first_core, second_core = t - core, t - core + 1
    is_zero, is_last, is_holder = s == 0, s == n_space - 1, s == holder
    is_keeper = jnp.logical_and(is_holder, core == 1)

    barrier = pltpu.get_barrier_semaphore()

    def greet(core_index, tile):
        pl.semaphore_signal(barrier, inc=1, device_id=(core_index, tile), device_id_type=MESH)

    for peer in (t, mate):
        goes_on = jnp.where(is_last, 1, 0)
        to_holder = jnp.where(right == holder, 1, 0)
        normal = peer - to_holder * lax.rem(peer, 2)
        greet(goes_on * second_core + (1 - goes_on) * normal, goes_on * holder + (1 - goes_on) * right)
    for peer in (t, mate):
        greet(peer - jnp.where(left == holder, 1, 0) * lax.rem(peer, 2), left)
    for peer in (y2, y1, y3):
        greet(peer - jnp.where(is_holder, 1, 0) * lax.rem(peer, 2), s)
    greet(mate, s)

    @pl.when(is_zero)
    def _():
        greet(second_core, holder)

    @pl.when(is_holder)
    def _():
        greet(t, 0)
        greet(mate, 0)

    loads = [
        pltpu.make_async_copy(src, dst, load.at[k])
        for k, (src, dst) in enumerate(
            (
                (state_in, state_ref), (jac_in, jac_ref), (start_in, start_ref), (w_in, w_ref), (slot_in, slot_ref),
                (frac_in, frac_ref), (obs_in, obs_ref), (inv_in, inv_ref),
            )
        )
    ]
    for c in loads:
        c.start()

    def copy(index, src, dst, device, out=0):
        return pltpu.make_async_remote_copy(
            src_ref=src, dst_ref=dst, send_sem=send.at[out], recv_sem=recv.at[index],
            device_id=device, device_id_type=MESH,
        )

    def arrived(index, ref):
        copy(index, ref, ref, (mate, s)).wait_recv()

    loads[0].wait()
    loads[1].wait()
    z = lax.dot_general(jac_ref[...], state_ref[...], (((0,), (0,)), ((), ())), preferred_element_type=F32).astype(BF16)
    zbuf[HEAD, 0] = z[:, :256]
    zbuf[TAIL, 0] = z[:, 256:]
    for c in loads[2:6]:
        c.wait()
    o_pack[0] = start_ref[...].astype(F32)
    o_pack[1] = slot_ref[...].astype(F32)
    o_pack[2] = frac_ref[...]
    o_pack[3] = jnp.zeros((1, 512), F32)

    @pl.when(jnp.logical_not(is_keeper))
    def _():
        pl.semaphore_wait(barrier, 8 + 7 * jnp.where(is_holder, 1, 0))

    @pl.when(jnp.logical_and(is_holder, core == 0))
    def _():
        pl.semaphore_signal(gate, inc=1, device_id=(mate, s), device_id_type=MESH)

    @pl.when(is_keeper)
    def _():
        pl.semaphore_wait(gate, 1)

    sides = ((HEAD, RIGHT, left), (TAIL, LEFT, right))
    z_relayed = [copy(Z_RELAYED + k, zbuf.at[a, 0, top], zbuf.at[b, 0, top], (t, d), 1 - k) for k, (a, b, d) in enumerate(sides)]
    z_direct = [copy(Z_REST, zbuf.at[a, 0, bottom], zbuf.at[b, 0, bottom], (t, d), 1 - k) for k, (a, b, d) in enumerate(sides)]
    z_cross = [copy(Z_REST, zbuf.at[a, 0, bottom], zbuf.at[b, 1, bottom], (mate, d), 1 - k) for k, (a, b, d) in enumerate(sides)]
    z_onward = [copy(Z_REST, zbuf.at[b, 0, top], zbuf.at[b, 1, top], (mate, s)) for a, b, d in sides]
    z_mate = [copy(Z_MATE, zbuf.at[a, 0], zbuf.at[a, 1], (mate, s)) for a, b, d in sides]
    z_held = [
        [copy(HELD + j, zbuf.at[HEAD, 0, rows], held.at[1 - k, rows], (second_core, holder), 1) for j, rows in ((0, top), (1, bottom))]
        for k in range(2)
    ]
    last = n_space - 1
    z_passed = [
        copy(Z_RELAYED, held.at[1, top], zbuf.at[RIGHT, 0, top], (mate, last), 2),
        copy(Z_RELAYED, held.at[0, top], zbuf.at[RIGHT, 0, top], (t, last), 2),
        copy(Z_REST, held.at[1, bottom], zbuf.at[RIGHT, 0, bottom], (mate, last), 2),
        copy(Z_REST, held.at[0, bottom], zbuf.at[RIGHT, 1, bottom], (mate, last), 2),
        copy(Z_REST, held.at[0, bottom], zbuf.at[RIGHT, 0, bottom], (t, last), 2),
        copy(Z_REST, held.at[1, bottom], zbuf.at[RIGHT, 1, bottom], (t, last), 2),
    ]
    fields = ((o_pack, m_pack), (w_ref, m_w))
    meta = {}
    for hop, peer in ((2, y2), (1, y1), (3, y3)):
        at = 3 - hop
        meta[at] = [copy(META + at, src, dst.at[at], (peer, s)) for src, dst in fields]
    for c in meta[1] + meta[2] + meta[0]:
        c.start()

    for k in range(2):

        @pl.when(jnp.logical_and(is_zero, core == k))
        def _():
            for c in z_held[k]:
                c.start()

    gives_way = s == holder + 1

    @pl.when(jnp.logical_not(jnp.logical_or(is_zero, gives_way)))
    def _():
        for c in (z_relayed[0], z_direct[0], z_cross[0]):
            c.start()

    for c in [z_relayed[1], z_direct[1], z_cross[1]] + z_mate:
        c.start()

    def weight_of(slot, frac, held):
        return jnp.where(slot == held, 1.0 - frac, 0.0) + jnp.where(slot + 1 == held, frac, 0.0)

    def build(group, start, w, slot, frac):
        abuf[group, 0:1, :] = weight_of(slot, frac, t)
        abuf[group, 1:2, :] = weight_of(slot, frac, mate)
        local = jnp.bitwise_and(start - s * 512 + 256, total_cols - 1)
        row = lax.broadcasted_iota(jnp.int32, (8, 512), 0)
        ahead = jnp.bitwise_and(row - local, 7)
        weights = w.astype(F32)
        turned = jnp.zeros((8, 512), F32)
        for k in range(8):
            turned = turned + jnp.where(ahead == k, weights[k : k + 1, :], 0.0)
        block = lax.shift_right_arithmetic(local - row + 7, 3)

        for first, last, shift in ((0, 4, 0), (4, 8, 8), (8, 16, -4)):

            def rows(index, carry):
                parts = [jnp.where(block == (index + shift) * 8 + m, turned, 0.0) for m in range(8)]
                at = pl.ds(pl.multiple_of(index * 64, 64), 64)
                foot[group, at, :] = jnp.concatenate(parts, axis=0).astype(BF16)
                return carry

            lax.fori_loop(first, last, rows, 0)

    def columns(first):
        return jnp.concatenate(
            [
                jnp.concatenate([zbuf[first, 0], zbuf[first + 1, 0]], axis=1),
                jnp.concatenate([zbuf[first, 1], zbuf[first + 1, 1]], axis=1),
            ],
            axis=0,
        )

    def centre(group):
        acc[group] = jnp.dot(columns(HEAD), foot[group, 512:1024, :], preferred_element_type=F32)

    def gathered(group):
        at = group - 1
        arrived(META + at, foot.at[group, 0:16])
        build(group, m_pack[at, 0].astype(jnp.int32), m_w[at], m_pack[at, 1].astype(jnp.int32), m_pack[at, 2])

    build(0, start_ref[...], w_ref[...], slot_ref[...], frac_ref[...])
    for c in loads[6:]:
        c.wait()
    obs_t[...] = jnp.transpose(obs_ref[...])
    inv_t[...] = jnp.transpose(jnp.broadcast_to(inv_ref[...], (chans, chans)))
    arrived(Z_MATE, zbuf.at[HEAD : HEAD + 2, 1])

    @pl.when(gives_way)
    def _():
        for c in (z_relayed[0], z_direct[0], z_cross[0]):
            c.start()

    @pl.when(is_keeper)
    def _():
        pl.semaphore_wait(barrier, 7)
        arrived(HELD, held.at[:, top])
        for c in z_passed[:2]:
            c.start()
        arrived(HELD + 1, held.at[:, bottom])
        for c in z_passed[2:]:
            c.start()
        for device in ((t, 0), (mate, 0)):
            pl.semaphore_signal(gate, inc=1, device_id=device, device_id_type=MESH)

    z_relayed[1].wait_recv()
    z_onward[1].start()
    z_relayed[0].wait_recv()
    z_onward[0].start()
    for group in (3,):
        gathered(group)
    for group in (2,):
        gathered(group)
        centre(group)
    gathered(1)
    arrived(Z_REST, zbuf.at[0:3, 0])

    def weighted(group, total):
        return abuf[group, 0:1, :] * total[:chans] + abuf[group, 1:2, :] * total[chans:]

    def partials(group):
        whole = jnp.concatenate([columns(LEFT), columns(HEAD)], axis=1)
        return weighted(group, jnp.dot(whole, foot[group], preferred_element_type=F32))

    def lanes(q):
        return slice(q * quarter, (q + 1) * quarter)

    far = [copy(FAR + q, pout.at[q], relay.at[q], ((y1, y3)[q % 2], s)) for q in range(4)]
    to_next = [copy(SUM + q, pout.at[4 + q], rin.at[0, q], (y1, s)) for q in range(4)]
    to_last = [copy(SUM + q, pout.at[8 + q], rin.at[1, q], (y3, s)) for q in range(4)]
    partial = weighted(2, acc[2] + jnp.dot(columns(LEFT), foot[2, 0:512, :], preferred_element_type=F32))
    for q in range(4):
        pout[q] = partial[:, lanes(q)].astype(BF16)
        far[q].start()
    for group, base, copies, now in ((1, 4, to_next, 1), (3, 8, to_last, 0)):
        partial = partials(group)
        for q in (now, now + 2):
            pout[base + q] = partial[:, lanes(q)].astype(BF16)
            copies[q].start()
        for q in (1 - now, 3 - now):
            acc[group, 0:chans, lanes(q)] = partial[:, lanes(q)]
    acc[0, 0:chans] = partials(0)
    for q in range(4):
        group, base, copies = ((1, 4, to_next), (3, 8, to_last))[q % 2]
        far[q].wait_recv()
        pout[base + q] = (acc[group, 0:chans, lanes(q)] + relay[q].astype(F32)).astype(BF16)
        copies[q].start()

    ag_next = [copy(FIRST + q if q % 2 == 0 else SECOND, sbuf.at[0, q], sbuf.at[3, q], (y1, s)) for q in range(4)]
    ag_last = [copy(FIRST + q if q % 2 else SECOND, sbuf.at[0, q], sbuf.at[1, q], (y3, s)) for q in range(4)]
    ag_far = [
        copy(LAST + q // 2, sbuf.at[(3, 1)[q % 2], q], sbuf.at[2, q], ((y1, y3)[q % 2], s)) for q in range(4)
    ]
    column = lax.broadcasted_iota(jnp.int32, (1, quarter), 1)
    for q in range(4):
        arrived(SUM + q, rin.at[:, q])
        projected = acc[0, 0:chans, lanes(q)] + rin[0, q].astype(F32) + rin[1, q].astype(F32)
        live = column + q * quarter < count_ref[0, 0]
        departed = jnp.where(live, obs_t[:, lanes(q)] - projected, 0.0)
        dep_t[:, lanes(q)] = departed
        sbuf[0, q] = (departed * inv_t[:, 0:1]).astype(BF16)
        (ag_next, ag_last)[q % 2][q].start()
    for q in (0, 2):
        ag_next[q + 1].start()
        ag_last[q].start()

    dep_out[...] = jnp.transpose(dep_t[...])

    def lanes_of(ref, group, rows, quarters):
        if quarters[-1] - quarters[0] == len(quarters) - 1:
            return ref[group, rows, quarters[0] * quarter : (quarters[-1] + 1) * quarter]
        return jnp.concatenate([ref[group, rows, lanes(q)] for q in quarters], axis=1)

    def by_slot(pieces):
        parts = []
        for slot in range(2):
            row = []
            for group, quarters in pieces:
                values = jnp.concatenate([sbuf[group, q] for q in quarters], axis=1).astype(F32)
                row.append((lanes_of(abuf, group, slice(slot, slot + 1), quarters) * values).astype(BF16))
            parts.append(jnp.concatenate(row, axis=1))
        return jnp.concatenate(parts, axis=0)

    def sums(v, pieces, chunk):
        rows = slice(chunk * 256, (chunk + 1) * 256)
        return nt(v, jnp.concatenate([lanes_of(foot, group, rows, quarters) for group, quarters in pieces], axis=1))

    def spread(*pieces, fresh=False):
        v = by_slot(pieces)
        for chunk in range(4):
            if fresh:
                wide[chunk] = sums(v, pieces, chunk)
            else:
                wide[chunk] += sums(v, pieces, chunk)

    spread((0, (0, 1, 2, 3)), fresh=True)
    for q in range(4):
        (ag_next, ag_last)[q % 2][q].wait_recv()
        ag_far[q].start()
    spread((3, (0, 2)), (1, (1, 3)))
    arrived(SECOND, sbuf.at[3])
    spread((3, (1, 3)), (1, (0, 2)))
    arrived(LAST, sbuf.at[2, 0:2])
    spread((2, (0, 1)))
    arrived(LAST + 1, sbuf.at[2, 2:4])
    ends = ((LEFT, left), (RIGHT, right))
    r_own = [copy(RIMS + k, wout.at[k, 0, top], rim.at[1 - k, 0], (t, d)) for k, d in ends]
    r_other = [copy(RIMS + k, wout.at[k, 1, top], rim.at[1 - k, 1], (mate, d)) for k, d in ends]
    r_swap = [copy(SWAP + k, wout.at[k, 0, bottom], swap.at[k], (mate, s)) for k, d in ends]
    r_sum = [copy(RIMS + k, wout.at[k, 1, bottom], rim.at[1 - k, 2], (mate, d)) for k, d in ends]
    r_mate = [copy(W_MATE, wout.at[2 + k, 1], win.at[k], (mate, s)) for k in range(2)]
    @pl.when(is_zero)
    def _():
        pl.semaphore_wait(gate, 1)

    final = ((2, (2, 3)),)
    v = by_slot(final)
    for k in (RIGHT, LEFT):
        total = wide[k] + sums(v, final, k)
        wide[k] = total
        wout[k, 0] = total[:chans].astype(BF16)
        wout[k, 1, 0:64] = total[chans : chans + 64].astype(BF16)
        r_swap[k].start()

        @pl.when(core == 0)
        def _():
            r_other[k].start()

        @pl.when(core == 1)
        def _():
            r_own[k].start()

    for k in (RIGHT, LEFT):
        r_swap[k].wait_recv()
        wout[k, 1, 64:128] = (wide[k, chans + 64 : 2 * chans] + swap[k].astype(F32)).astype(BF16)
        r_sum[k].start()

    @pl.when(core == 0)
    def _():
        for k in (RIGHT, LEFT):
            r_own[k].start()

    @pl.when(core == 1)
    def _():
        for k in (RIGHT, LEFT):
            r_other[k].start()

    for k in range(2):
        total = wide[HEAD + k] + sums(v, final, HEAD + k)
        wide[HEAD + k] = total
        wout[2 + k, 1] = total[chans:].astype(BF16)
        r_mate[k].start()
    arrived(W_MATE, win)
    for h in (1, 0):
        arrived(RIMS + 1 - h, rim.at[h])
        rims = jnp.concatenate([rim[h, 0].astype(F32) + rim[h, 1].astype(F32), rim[h, 2].astype(F32)], axis=0)
        whole = wide[HEAD + h, 0:chans] + win[h].astype(F32) + rims
        adj_out[:, 0, h * 256 : (h + 1) * 256] = jnp.dot(jac_ref[...], whole.astype(BF16), preferred_element_type=F32)
    def left_here(ref, out):
        copy(META, ref, ref, (mate, s), out).wait_send()

    left_here(foot.at[0:3, 0:496], 0)

    @pl.when(is_zero)
    def _():
        left_here(held.at[0], 1)

    @pl.when(jnp.logical_not(is_zero))
    def _():
        left_here(foot.at[0:3, 0:32], 1)

    @pl.when(is_keeper)
    def _():
        left_here(foot.at[0:3, 0:64], 2)


def write(dep_in, adj_in, dep_out, adj_out, done):
    copies = [pltpu.make_async_copy(dep_in, dep_out, done.at[0]), pltpu.make_async_copy(adj_in, adj_out, done.at[1])]
    for c in copies:
        c.start()
    for c in copies:
        c.wait()


def body(state, obs_start, foot_weight, obs_slot, obs_frac, live_count, obs_values, jacobian, inv_var):
    n_space = lax.axis_size("space")
    levels = jacobian.shape[0]
    anywhere = pl.BlockSpec(memory_space=pl.ANY)
    vmem = pl.BlockSpec(memory_space=pltpu.VMEM)
    i32 = jnp.int32
    departures, adjoint = pl.pallas_call(
        functools.partial(kernel, n_space, 512 * n_space, 3 if n_space > 4 else 2),
        out_shape=(
            pltpu.VMEM((512, 128), F32),
            pltpu.VMEM((levels, 1, 512), F32),
        ),
        in_specs=[anywhere] * 5 + [pl.BlockSpec(memory_space=pltpu.SMEM)] + [anywhere] * 3,
        out_specs=(vmem, vmem),
        scratch_shapes=[
            pltpu.VMEM((levels, 512), BF16),
            pltpu.VMEM((1, 512), i32),
            pltpu.VMEM((8, 512), BF16),
            pltpu.VMEM((1, 512), i32),
            pltpu.VMEM((1, 512), F32),
            pltpu.VMEM((512, 128), F32),
            pltpu.VMEM((levels, 128), BF16),
            pltpu.VMEM((1, 128), F32),
            pltpu.VMEM((4, 1, 512), F32),
            pltpu.VMEM((3, 4, 1, 512), F32),
            pltpu.VMEM((3, 8, 512), BF16),
            pltpu.VMEM((2, 128, 256), BF16),
            pltpu.VMEM((4, 1024, 512), BF16),
            pltpu.VMEM((4, 2, 128, 256), BF16),
            pltpu.VMEM((4, 256, 512), F32),
            pltpu.VMEM((4, 2, 512), F32),
            pltpu.VMEM((12, 128, 128), BF16),
            pltpu.VMEM((4, 128, 128), BF16),
            pltpu.VMEM((2, 4, 128, 128), BF16),
            pltpu.VMEM((4, 4, 128, 128), BF16),
            pltpu.VMEM((4, 256, 256), F32),
            pltpu.VMEM((4, 2, 128, 256), BF16),
            pltpu.VMEM((2, 128, 256), BF16),
            pltpu.VMEM((2, 3, 64, 256), BF16),
            pltpu.VMEM((2, 64, 256), BF16),
            pltpu.VMEM((128, 512), F32),
            pltpu.VMEM((128, 128), F32),
            pltpu.VMEM((128, 512), F32),
            pltpu.SemaphoreType.DMA((8,)),
            pltpu.SemaphoreType.DMA((3,)),
            pltpu.SemaphoreType.DMA((ARRIVALS,)),
            pltpu.SemaphoreType.REGULAR,
        ],
        compiler_params=pltpu.CompilerParams(collective_id=0, has_side_effects=True),
        name="window",
    )(
        jnp.transpose(state[0]),
        obs_start[None],
        jnp.transpose(foot_weight),
        obs_slot[None],
        obs_frac[None],
        live_count,
        obs_values,
        jacobian,
        inv_var[None],
    )
    departures, adjoint = pl.pallas_call(
        write,
        out_shape=(jax.ShapeDtypeStruct(departures.shape, F32), jax.ShapeDtypeStruct(adjoint.shape, F32)),
        in_specs=[vmem] * 2,
        out_specs=(anywhere, anywhere),
        scratch_shapes=[pltpu.SemaphoreType.DMA((2,))],
        name="write",
    )(pltpu.with_memory_space_constraint(departures, pltpu.VMEM), pltpu.with_memory_space_constraint(adjoint, pltpu.VMEM))
    return departures, jnp.transpose(adjoint, (1, 2, 0))


def solution(mesh):
    return jax.shard_map(
        body,
        mesh=mesh,
        in_specs=(
            P("tm", "space", None),
            P(("tm", "space")),
            P(("tm", "space"), None),
            P(("tm", "space")),
            P(("tm", "space")),
            P("tm", "space"),
            P(("tm", "space"), None),
            P(),
            P(),
        ),
        out_specs=(P(("tm", "space"), None), P("tm", "space", None)),
        check_vma=False,
    )
```
